512 devices in a mesh: seq: 128 (over z_lo, y, x), tp: 4 (over z_hi, core).
Axes of the slice: x: 4, y: 4, z: 16 (z_hi: 2, z_lo: 8; z = z_hi * 8 + z_lo), core: 2. Of those that a mesh axis runs over, the one named last changes fastest.
Arguments:
- inputs: bfloat16 [32768, 5120], P('seq', 'tp'), may hold values from -6 to 6
- gate_input: bfloat16 [32768, 5120], P('seq', 'tp'), may hold values from -6 to 6
- b_source: bfloat16 [32768, 128], P('seq'), may hold values from -6 to 6
- c_source: bfloat16 [32768, 128], P('seq'), may hold values from -6 to 6
- step_raw: float32 [32768, 80], P('seq', 'tp'), may hold values from -4 to 4
- step_bias: float32 [80], P('tp'), may hold values from -3 to 0
- decay_rate: float32 [80], P('tp'), may hold values from 6.1035157e-06 to 0.05
- conv_weight: float32 [4, 256], replicated, may hold values from -3 to 3
- conv_bias: float32 [256], replicated, may hold values from -3 to 3
- norm_gain: float32 [5120], P('tp'), may hold values from 0.5 to 1.5
- doc_lengths: int32 [8], replicated, may hold values from 1 to 16384, 32768 in all
Outputs:
- output: bfloat16 [32768, 5120], P('seq', 'tp')
The draws below stay inside these ranges and needn't reach their ends.
Inputs may be any that keep to these rules, and one draw needn't show every extreme that they name: doc_lengths sums to 32768; every length is at least 1 and the largest is exactly 16384.
All inputs are finite; a program needn't handle non-finite values.
Results may differ from the reference program's by a relative error of at most 0.0015.
Values may be sent and summed in bfloat16 or wider, within the bound.
No kernel may reach another device: no remote copies, remote signals or barrier semaphores. Data moves between devices by JAX's collectives and lax.ppermute only.
A program may use at most 192 MiB of HBM per device.

```python
import math
import jax
import jax.numpy as jnp
import numpy as np
from jax import lax

H = 80
HEAD_DIM = 64
STATE = 128
CONV = 4
BLOCK = 256
DOCS = 8
SEQ = 32768
DOC_MOST = 16384


def steps_of(key, dims, shards, low, top_value):
    factor_of = 1.0
    for dim, shards_of in shards:
        steps = jax.random.uniform(jax.random.fold_in(jax.random.fold_in(key, 6), dim), (shards_of,), jnp.float32, low / len(shards), top_value / len(shards))
        factor_of = factor_of * jnp.repeat(jnp.exp(steps), dims[dim] // shards_of).reshape((-1,) + (1,) * (len(dims) - 1 - dim))
    return factor_of


def profile(number_of, total, bound, skew):
    loads = [(1 << 20) // math.isqrt(grade ** skew) + 1 for grade in range(2, number_of + 1)]
    surplus, holding = total - bound - (number_of - 1), [1] * (number_of - 1)
    while surplus > 0:
        candidates = [i for i in range(number_of - 1) if holding[i] < bound]
        pool, left = sum([loads[i] for i in candidates]), surplus
        for i in candidates:
            more = min(bound - holding[i], max(1, left * loads[i] // pool), surplus)
            holding[i] = holding[i] + more
            surplus = surplus - more
    return np.array([bound] + holding)


def ragged_sizes(rng, number_of, total, most, slope):
    if number_of == 2:
        one = jax.random.randint(rng, (), max(1, total - most), min(most, total - 1) + 1)
        return jnp.stack([one, total - one])
    lengths = jnp.asarray(profile(number_of, total, most, slope), jnp.int32)
    couples = (number_of - 1) // 2
    giver, sink = lengths[1:1 + 2 * couples:2], lengths[2:2 + 2 * couples:2]
    slack = jnp.minimum(giver - 1, most - sink)
    passed = jax.random.randint(jax.random.fold_in(rng, 1), (couples,), 0, 1 << 20) % (slack + 1)
    lengths = lengths.at[1:1 + 2 * couples:2].set(giver - passed).at[2:2 + 2 * couples:2].set(sink + passed)
    return lengths[jax.random.permutation(jax.random.fold_in(rng, 2), number_of)]


def normal_values(stream_key, extent, spread, reach, cuts=(), held_as=jnp.bfloat16):
    drawn = spread * jax.random.normal(stream_key, extent, jnp.float32)
    if cuts:
        drawn = drawn * steps_of(stream_key, extent, cuts, -0.22, 0.18)
    return jnp.clip(drawn, -reach, reach).astype(held_as)


def setup_inputs(seed: int = 0) -> dict:
    key_of = jax.random.split(jax.random.key(seed), 12)
    inputs = normal_values(key_of[0], (SEQ, H * HEAD_DIM), 1.0, 6.0, ((0, 128), (1, 4)))
    gate_input = normal_values(key_of[1], (SEQ, H * HEAD_DIM), 1.0, 6.0, ((0, 128), (1, 4)))
    b_source = normal_values(key_of[2], (SEQ, STATE), 1.0, 6.0, ((0, 128),))
    c_source = normal_values(key_of[3], (SEQ, STATE), 1.0, 6.0, ((0, 128),))
    step_raw = normal_values(key_of[4], (SEQ, H), 0.5, 4.0, ((0, 128), (1, 4)), jnp.float32)
    step_bias = jnp.clip(-3.0 + 3.0 * jax.random.uniform(key_of[5], (H,), jnp.float32) ** steps_of(key_of[5], (H,), ((0, 4),), -0.2, 0.2), -3.0, 0.0)
    decay_rate = jnp.clip(jnp.exp(math.log(0.05) - 9.010913 * jax.random.uniform(key_of[6], (H,), jnp.float32) ** steps_of(key_of[6], (H,), ((0, 4),), -0.2, 0.2)), 6.10351571594947e-06, 0.05)
    conv_weight = normal_values(key_of[7], (CONV, 2 * STATE), CONV ** -0.5, 3.0, (), jnp.float32)
    conv_bias = normal_values(key_of[8], (2 * STATE,), 0.5, 3.0, (), jnp.float32)
    norm_gain = jnp.clip(1.0 + 0.1 * jax.random.normal(key_of[9], (H * HEAD_DIM,), jnp.float32), 0.5, 1.5)
    doc_lengths = ragged_sizes(key_of[10], DOCS, SEQ, DOC_MOST, 2).astype(jnp.int32)
    return {"inputs": inputs, "gate_input": gate_input, "b_source": b_source, "c_source": c_source, "step_raw": step_raw, "step_bias": step_bias, "decay_rate": decay_rate, "conv_weight": conv_weight, "conv_bias": conv_bias, "norm_gain": norm_gain, "doc_lengths": doc_lengths}


epsilon = 1e-05

def locate(position, doc_lengths):
    starts = (jnp.cumsum(doc_lengths) - doc_lengths).astype(jnp.int32)
    chosen = jnp.where(starts[None, :] <= position[:, None], starts[None, :], 0)
    return lax.optimization_barrier(jnp.max(chosen, axis=1)).astype(jnp.int32)

def convolve(padded, weight, conv_bias, position, doc_start):
    kernel_taps = weight.shape[0]
    tokens = position.shape[0]
    widened = padded.astype(jnp.float32)
    summed = jnp.broadcast_to(conv_bias[None, :], (tokens, conv_bias.shape[0]))
    for offset in range(kernel_taps):
        backward = kernel_taps - 1 - offset
        inside = (position - backward >= doc_start)[:, None]
        summed = summed + jnp.where(inside, weight[offset][None, :] * widened[offset:offset + tokens], 0.0)
    return jax.nn.silu(summed).astype(jnp.bfloat16)

def state_terms(pieces):
    block_inputs, b_block, step_size, cumulated, doc_start, position = pieces
    same_doc = doc_start == doc_start[-1]
    weighting = jnp.where(same_doc[:, None], jnp.exp(cumulated[-1][None, :] - cumulated) * step_size, 0.0)
    weighted = (block_inputs.astype(jnp.float32) * weighting[:, :, None]).astype(jnp.bfloat16)
    weighted = lax.optimization_barrier(weighted).astype(jnp.float32)
    end_state = jnp.einsum('qhp,qn->hpn', weighted, b_block.astype(jnp.float32), precision=lax.Precision.HIGHEST)
    end_factor = jnp.where(doc_start[-1] < position[0], jnp.exp(cumulated[-1]), 0.0)
    return (end_state, end_factor)

def diagonal_terms(pieces):
    block_inputs, b_block, c_block, step_size, cumulated, doc_start = pieces
    row_count = doc_start.shape[0]
    products = jnp.dot(c_block, b_block.T, preferred_element_type=jnp.float32)
    order_ids = jnp.arange(row_count)
    causal = (order_ids[None, :] <= order_ids[:, None]) & (doc_start[None, :] == doc_start[:, None])
    decay_gap = cumulated.T[:, :, None] - cumulated.T[:, None, :]
    scores = jnp.where(causal[None], products[None] * jnp.exp(decay_gap) * step_size.T[:, None, :], 0.0)
    scores = lax.optimization_barrier(scores.astype(jnp.bfloat16)).astype(jnp.float32)
    return jnp.einsum('hts,shp->thp', scores, block_inputs.astype(jnp.float32), precision=lax.Precision.HIGHEST)

def emit_rows(state_in, pieces):
    end_state, end_factor, c_block, out_decay = pieces
    rounded = lax.optimization_barrier(state_in.astype(jnp.bfloat16)).astype(jnp.float32)
    from_state = jnp.einsum('qn,hpn->qhp', c_block.astype(jnp.float32), rounded, precision=lax.Precision.HIGHEST)
    from_state = from_state * out_decay[:, :, None]
    return (end_factor[:, None, None] * state_in + end_state, from_state)

def reference(inputs, gate_input, b_source, c_source, step_raw, step_bias, decay_rate, conv_weight, conv_bias, norm_gain, doc_lengths):
    position = jnp.arange(SEQ, dtype=jnp.int32)
    doc_start = locate(position, doc_lengths)
    keep_rows = CONV - 1
    blank = jnp.zeros((keep_rows, STATE), jnp.bfloat16)
    b_conv = convolve(jnp.concatenate([blank, b_source], 0), conv_weight[:, :STATE], conv_bias[:STATE], position, doc_start)
    c_conv = convolve(jnp.concatenate([blank, c_source], 0), conv_weight[:, STATE:], conv_bias[STATE:], position, doc_start)
    step_size = jax.nn.softplus(step_raw + step_bias[None, :])
    log_decay = -step_size * decay_rate[None, :]
    block_count = SEQ // BLOCK
    shaped_inputs = inputs.reshape(block_count, BLOCK, H, HEAD_DIM)
    b_blocks = b_conv.reshape(block_count, BLOCK, STATE)
    c_blocks = c_conv.reshape(block_count, BLOCK, STATE)
    step_blocks = step_size.reshape(block_count, BLOCK, H)
    cumulated = jnp.cumsum(log_decay.reshape(block_count, BLOCK, H), axis=1)
    start_blocks = doc_start.reshape(block_count, BLOCK)
    position_blocks = position.reshape(block_count, BLOCK)
    out_decay = jnp.where((start_blocks < position_blocks[:, :1])[:, :, None], jnp.exp(cumulated), 0.0)

    def advance(state_in, pieces):
        block_inputs, b_block, c_block, step_block, cum_block, start_block, position_block, decay_block = pieces
        end_state, end_factor = state_terms((block_inputs, b_block, step_block, cum_block, start_block, position_block))
        diagonal = diagonal_terms((block_inputs, b_block, c_block, step_block, cum_block, start_block))
        next_state, from_state = emit_rows(state_in, (end_state, end_factor, c_block, decay_block))
        return (next_state, diagonal + from_state)
    initial = jnp.zeros((H, HEAD_DIM, STATE), jnp.float32)
    final_state, mixed = lax.scan(advance, initial, (shaped_inputs, b_blocks, c_blocks, step_blocks, cumulated, start_blocks, position_blocks, out_decay))
    mixed = mixed.reshape(SEQ, H * HEAD_DIM)
    gated = mixed * jax.nn.silu(gate_input.astype(jnp.float32))
    mean_square = lax.optimization_barrier(jnp.sum(gated * gated, axis=1)) / (H * HEAD_DIM)
    return (gated * lax.rsqrt(mean_square + epsilon)[:, None] * norm_gain[None, :]).astype(jnp.bfloat16)
```

```python
import functools

import jax
import jax.numpy as jnp
from jax import lax
from jax.experimental import pallas as pl
from jax.experimental.pallas import tpu as pltpu
from jax.sharding import Mesh
from jax.sharding import PartitionSpec as P

SEQ = ("za", "zb", "y", "x")
GROUP = ("zb", "y", "x")
OUTER = "za"
LANES = 128
epsilon = 1e-05
HIGHEST = lax.Precision.HIGHEST
VMEM = pl.BlockSpec(memory_space=pltpu.VMEM)
SMEM = pl.BlockSpec(memory_space=pltpu.SMEM)


def call(kernel, outs, *args, scalars=0, scratch=(), flops=1_000_000):
    multiple = isinstance(outs, (list, tuple))
    return pl.pallas_call(
        kernel,
        out_shape=list(outs) if multiple else outs,
        in_specs=[SMEM] * scalars + [VMEM] * (len(args) - scalars),
        out_specs=[VMEM] * len(outs) if multiple else VMEM,
        scratch_shapes=list(scratch),
        compiler_params=pltpu.CompilerParams(vmem_limit_bytes=24 * 1024 * 1024),
        cost_estimate=pl.CostEstimate(flops=flops, bytes_accessed=1_000_000, transcendentals=0),
    )(*args)


def out(shape, dtype=jnp.float32):
    return jax.ShapeDtypeStruct(shape, dtype)


def latest_start(position, doc_ref):
    start, chosen = jnp.int32(0), jnp.zeros_like(position)
    for i in range(doc_ref.shape[0]):
        chosen = jnp.maximum(chosen, jnp.where(start <= position, start, 0))
        start = start + doc_ref[i]
    return chosen


def tile_of_heads(columns, tile, width):
    per, rows = LANES // width, columns.shape[0]
    lane = lax.broadcasted_iota(jnp.int32, (rows, LANES), 1)
    spread = jnp.broadcast_to(columns[:, tile * per : tile * per + 1], (rows, LANES))
    for k in range(1, per):
        h = tile * per + k
        spread = jnp.where(
            lane < k * width, spread, jnp.broadcast_to(columns[:, h : h + 1], (rows, LANES))
        )
    return spread


def convolve(source_ref, halo, weight, bias, base, doc_ref, padded_ref):
    tokens = source_ref.shape[0]
    padded_ref[0:8, :] = halo.astype(jnp.float32)
    padded_ref[8:, :] = source_ref[...].astype(jnp.float32)
    position = base + lax.broadcasted_iota(jnp.int32, source_ref.shape, 0)
    doc_start = latest_start(position, doc_ref)
    summed = jnp.broadcast_to(bias, source_ref.shape)
    taps = weight.shape[0]
    for k in range(taps):
        back = taps - 1 - k
        term = weight[k : k + 1, :] * padded_ref[8 - back : 8 - back + tokens, :]
        summed = summed + jnp.where(position - back >= doc_start, term, 0.0)
    return (summed * jax.nn.sigmoid(summed)).astype(jnp.bfloat16)


def prepare_kernel(
    base_ref, doc_ref, x_ref, raw_ref, bias_ref, rate_ref, weighted_ref, cum_ref, step_ref, factor_ref
):
    base = base_ref[0]
    tokens, heads = raw_ref.shape
    width = x_ref.shape[1] // heads
    step = jax.nn.softplus(raw_ref[...] + bias_ref[...])
    log_decay = -step * rate_ref[...]
    rows = lax.broadcasted_iota(jnp.int32, (tokens, tokens), 0)
    cols = lax.broadcasted_iota(jnp.int32, (tokens, tokens), 1)
    cum = jnp.dot(
        jnp.where(cols <= rows, 1.0, 0.0), log_decay, precision=HIGHEST,
        preferred_element_type=jnp.float32,
    )
    cum_ref[...] = jnp.zeros_like(cum_ref)
    step_ref[...] = jnp.zeros_like(step_ref)
    factor_ref[...] = jnp.zeros_like(factor_ref)
    cum_ref[:, 0:heads] = cum
    step_ref[:, 0:heads] = step
    end_start = latest_start(base + tokens - 1, doc_ref)
    last = cum[tokens - 1 : tokens, :]
    position = base + lax.broadcasted_iota(jnp.int32, (tokens, heads), 0)
    weighting = jnp.where(position >= end_start, jnp.exp(last - cum) * step, 0.0)
    factor_ref[:, 0:heads] = jnp.where(end_start < base, jnp.exp(last), 0.0)
    for j in range(x_ref.shape[1] // LANES):
        tile = slice(j * LANES, (j + 1) * LANES)
        weighted_ref[:, tile] = (
            x_ref[:, tile].astype(jnp.float32) * tile_of_heads(weighting, j, width)
        ).astype(jnp.bfloat16)


def states_kernel(
    base_ref, doc_ref, b_ref, halo_ref, weight_ref, bias_ref, weighted_ref, factor_ref,
    pieces_ref, b_conv_ref, padded_ref,
):
    state, features = b_ref.shape[1], weighted_ref.shape[1]
    members, rows, _ = pieces_ref.shape
    b_conv = convolve(
        b_ref, halo_ref[:, 0:state], weight_ref[:, 0:state], bias_ref[:, 0:state],
        base_ref[0], doc_ref, padded_ref,
    )
    b_conv_ref[...] = b_conv
    b_rows = b_conv.astype(jnp.float32).T.astype(jnp.bfloat16)
    for j in range(features // 256):
        tile = slice(j * 256, (j + 1) * 256)
        end_state = jnp.dot(b_rows, weighted_ref[:, tile], preferred_element_type=jnp.float32)
        for m in range(members):
            pieces_ref[m, :, tile] = end_state[m * rows : (m + 1) * rows, :]
    spread = jnp.broadcast_to(factor_ref[...], (rows, LANES))
    for m in range(members):
        pieces_ref[m, :, features:] = spread


def prefix_kernel(heads, pieces_ref, before_ref, factors_ref, totals_ref, single_ref, wide_ref):
    members, rows, padded = pieces_ref.shape
    features = padded - LANES
    width = features // heads
    for m in range(members):
        single_ref[m : m + 1, :] = pieces_ref[m, 0:1, features:]
    single = single_ref[...]
    for j in range(features // LANES):
        wide_ref[:, j * LANES : (j + 1) * LANES] = tile_of_heads(single, j, width)
    product = jnp.ones((1, LANES), jnp.float32)
    for m in range(members):
        factors_ref[m : m + 1, :] = product
        product = product * single_ref[m : m + 1, :]
    total = jnp.zeros((rows, features), jnp.float32)
    for m in range(members):
        before_ref[m] = total
        total = wide_ref[m : m + 1, :] * total + pieces_ref[m, :, 0:features]
    for d in range(totals_ref.shape[0]):
        totals_ref[d, :, 0:features] = total
        totals_ref[d, :, features:] = jnp.broadcast_to(product, (rows, LANES))


def states_in_kernel(heads, place_ref, totals_ref, before_ref, factors_ref, state_ref, wide_ref):
    members, rows, features = before_ref.shape
    width = features // heads
    place = place_ref[0]
    entering = jnp.zeros((rows, features), jnp.float32)
    for g in range(totals_ref.shape[0] - 1):
        factor = jnp.concatenate(
            [
                tile_of_heads(totals_ref[g, 0:1, features:], j, width)
                for j in range(features // LANES)
            ],
            axis=1,
        )
        passed = factor * entering + totals_ref[g, :, 0:features]
        entering = jnp.where(g < place, passed, entering)
    factors = factors_ref[...]
    for j in range(features // LANES):
        wide_ref[:, j * LANES : (j + 1) * LANES] = tile_of_heads(factors, j, width)
    for m in range(members):
        state_ref[m] = (wide_ref[m : m + 1, :] * entering + before_ref[m]).astype(jnp.bfloat16)


def diagonal_kernel(
    base_ref, doc_ref, c_ref, halo_ref, weight_ref, bias_ref, b_conv_ref, cum_ref, step_ref,
    x_ref, gate_ref, c_conv_ref, gated_ref, scale_ref, padded_ref, products_ref,
):
    base = base_ref[0]
    tokens, state = c_ref.shape
    features = x_ref.shape[1]
    half = tokens // 2
    c_conv = convolve(
        c_ref, halo_ref[:, state:], weight_ref[:, state:], bias_ref[:, state:], base, doc_ref,
        padded_ref,
    )
    c_conv_ref[...] = c_conv
    products = lax.dot_general(
        c_conv, b_conv_ref[...], (((1,), (1,)), ((), ())), preferred_element_type=jnp.float32
    )
    row = lax.broadcasted_iota(jnp.int32, (tokens, tokens), 0)
    col = lax.broadcasted_iota(jnp.int32, (tokens, tokens), 1)
    doc_start = latest_start(base + row, doc_ref)
    products_ref[...] = jnp.where((col <= row) & (base + col >= doc_start), products, 0.0)
    cum, cum_rows, step_rows = cum_ref[...], cum_ref[...].T, step_ref[...].T
    width = features // HEADS_OF(features)
    position = base + lax.broadcasted_iota(jnp.int32, (tokens, LANES), 0)
    carried = jnp.where(doc_start[:, 0:LANES] < base, jnp.exp(cum), 0.0)
    lane = lax.broadcasted_iota(jnp.int32, (tokens, LANES), 1)
    del position
    per = LANES // width
    for j in range(features // LANES):
        tile = slice(j * LANES, (j + 1) * LANES)
        diagonal = None
        for k in range(per):
            h = j * per + k
            column = jnp.broadcast_to(cum[:, h : h + 1], (tokens, LANES))
            cum_row, step_row = cum_rows[h : h + 1, :], step_rows[h : h + 1, :]
            upper = (
                products_ref[0:half, 0:half] * jnp.exp(column[0:half] - cum_row[:, 0:half])
            ) * step_row[:, 0:half]
            lower_left = (
                products_ref[half:, 0:half] * jnp.exp(column[half:] - cum_row[:, 0:half])
            ) * step_row[:, 0:half]
            lower_right = (
                products_ref[half:, half:] * jnp.exp(column[half:] - cum_row[:, half:])
            ) * step_row[:, half:]
            lower = jnp.concatenate([lower_left, lower_right], axis=1).astype(jnp.bfloat16)
            part = jnp.concatenate(
                [
                    jnp.dot(upper.astype(jnp.bfloat16), x_ref[0:half, tile],
                            preferred_element_type=jnp.float32),
                    jnp.dot(lower, x_ref[:, tile], preferred_element_type=jnp.float32),
                ],
                axis=0,
            )
            diagonal = part if diagonal is None else jnp.where(lane < k * width, diagonal, part)
        gate = gate_ref[:, tile].astype(jnp.float32)
        gate = gate * jax.nn.sigmoid(gate)
        gated_ref[:, tile] = diagonal * gate
        scale_ref[:, tile] = tile_of_heads(carried, j, width) * gate


def HEADS_OF(features):
    return features // 64


def gate_kernel(state_ref, c_conv_ref, diagonal_ref, scale_ref, gated_ref, squares_ref, rows_ref):
    members, rows, features = state_ref.shape
    for m in range(members):
        rows_ref[m * rows : (m + 1) * rows, :] = state_ref[m].astype(jnp.float32)
    c_conv = c_conv_ref[...]
    squares = jnp.zeros((c_conv.shape[0], LANES), jnp.float32)
    for j in range(features // LANES):
        tile = slice(j * LANES, (j + 1) * LANES)
        carried = jnp.dot(
            c_conv, rows_ref[:, tile].astype(jnp.bfloat16), preferred_element_type=jnp.float32
        )
        gated = diagonal_ref[:, tile] + scale_ref[:, tile] * carried
        gated_ref[:, tile] = gated
        squares = squares + gated * gated
    squares_ref[...] = lax.dot_general(
        jnp.ones((8, LANES), jnp.float32), squares, (((1,), (1,)), ((), ())),
        precision=HIGHEST, preferred_element_type=jnp.float32,
    )[0:1]


def normalize_kernel(features_all, squares_ref, gated_ref, gain_ref, out_ref):
    count = squares_ref.shape[0]
    total = squares_ref[0]
    for k in range(1, count):
        total = total + squares_ref[k]
    first = lax.broadcasted_iota(jnp.int32, (8, total.shape[1]), 0) == 0
    column = lax.dot_general(
        jnp.where(first, jnp.broadcast_to(total, first.shape), 0.0),
        jnp.ones((8, LANES), jnp.float32), (((0,), (0,)), ((), ())),
        precision=HIGHEST, preferred_element_type=jnp.float32,
    )
    scale = lax.rsqrt(column / features_all + epsilon)
    for j in range(gated_ref.shape[1] // LANES):
        tile = slice(j * LANES, (j + 1) * LANES)
        out_ref[:, tile] = (gated_ref[:, tile] * scale * gain_ref[:, tile]).astype(jnp.bfloat16)


def body(
    inputs, gate_input, b_source, c_source, step_raw, step_bias, decay_rate, conv_weight,
    conv_bias, norm_gain, doc_lengths,
):
    tokens, features = inputs.shape
    heads = step_raw.shape[1]
    state = b_source.shape[1]
    members = 1
    for axis in GROUP:
        members *= lax.axis_size(axis)
    outer = lax.axis_size(OUTER)
    rows = state // members
    shards = members * outer
    base = (lax.axis_index(SEQ) * tokens).astype(jnp.int32).reshape(1)
    place = lax.axis_index(OUTER).astype(jnp.int32).reshape(1)

    tails = jnp.concatenate([b_source[tokens - 8 :], c_source[tokens - 8 :]], axis=1)
    halo = lax.ppermute(tails, SEQ, [(i, i + 1) for i in range(shards - 1)])

    weighted, cum, step, factor = call(
        prepare_kernel,
        [out((tokens, features), jnp.bfloat16), out((tokens, LANES)), out((tokens, LANES)), out((1, LANES))],
        base, doc_lengths, inputs, step_raw, step_bias[None, :], decay_rate[None, :], scalars=2,
    )
    pieces, b_conv = call(
        states_kernel,
        [out((members, rows, features + LANES)), out((tokens, state), jnp.bfloat16)],
        base, doc_lengths, b_source, halo, conv_weight, conv_bias[None, :], weighted, factor,
        scalars=2, scratch=[pltpu.VMEM((tokens + 8, state), jnp.float32)],
    )
    pieces = lax.all_to_all(pieces, GROUP, 0, 0)
    c_conv, diagonal, scale = call(
        diagonal_kernel,
        [out((tokens, state), jnp.bfloat16), out((tokens, features)), out((tokens, features))],
        base, doc_lengths, c_source, halo, conv_weight, conv_bias[None, :], b_conv, cum, step,
        inputs, gate_input, scalars=2,
        scratch=[
            pltpu.VMEM((tokens + 8, state), jnp.float32),
            pltpu.VMEM((tokens, tokens), jnp.float32),
        ],
    )
    before, factors, totals = call(
        functools.partial(prefix_kernel, heads),
        [out((members, rows, features)), out((members, LANES)), out((outer, rows, features + LANES))],
        pieces,
        scratch=[pltpu.VMEM((members, LANES), jnp.float32), pltpu.VMEM((members, features), jnp.float32)],
    )
    totals = lax.all_to_all(totals, OUTER, 0, 0)
    states_in = call(
        functools.partial(states_in_kernel, heads),
        out((members, rows, features), jnp.bfloat16),
        place, totals, before, factors, scalars=1,
        scratch=[pltpu.VMEM((members, features), jnp.float32)],
    )
    states_in = lax.all_to_all(states_in, GROUP, 0, 0)
    gated, squares = call(
        gate_kernel,
        [out((tokens, features)), out((1, tokens))],
        states_in, c_conv, diagonal, scale,
        scratch=[pltpu.VMEM((state, features), jnp.float32)],
    )
    squares = lax.all_gather(squares, "tp")
    return call(
        functools.partial(normalize_kernel, features * lax.axis_size("tp")),
        out((tokens, features), jnp.bfloat16),
        squares, gated, norm_gain[None, :],
    )


def solution(mesh):
    finer = Mesh(
        mesh.devices.reshape(4, 2, 4, 4, mesh.shape["tp"]), ("za", "zb", "y", "x", "tp")
    )
    in_specs = (
        P(SEQ, "tp"), P(SEQ, "tp"), P(SEQ, None), P(SEQ, None), P(SEQ, "tp"), P("tp"), P("tp"),
        P(), P(), P("tp"), P(),
    )
    return jax.shard_map(
        body, mesh=finer, in_specs=in_specs, out_specs=P(SEQ, "tp"), check_vma=False
    )
```

```python
import functools

import jax
import jax.numpy as jnp
from jax import lax
from jax.experimental import pallas as pl
from jax.experimental.pallas import tpu as pltpu
from jax.sharding import Mesh
from jax.sharding import PartitionSpec as P

SEQ = ("za", "zb", "y", "x")
GROUP = ("zb", "y", "x")
OUTER = "za"
LANES = 128
epsilon = 1e-05
HIGHEST = lax.Precision.HIGHEST
VMEM = pl.BlockSpec(memory_space=pltpu.VMEM)
HBM = pl.BlockSpec(memory_space=pltpu.HBM)


def call(kernel, outs, *args, hbm=0, after=(), scratch=(), flops=1_000_000):
    if after:
        inner, skip = kernel, len(after)
        kernel = lambda *refs: inner(*refs[:len(args)], *refs[len(args) + skip:])
    multiple = isinstance(outs, (list, tuple))
    return pl.pallas_call(
        kernel,
        out_shape=list(outs) if multiple else outs,
        in_specs=[HBM] * hbm + [VMEM] * (len(args) - hbm) + [VMEM] * len(after),
        out_specs=[VMEM] * len(outs) if multiple else VMEM,
        scratch_shapes=list(scratch),
        compiler_params=pltpu.CompilerParams(vmem_limit_bytes=24 * 1024 * 1024),
        cost_estimate=pl.CostEstimate(flops=flops, bytes_accessed=1_000_000, transcendentals=0),
    )(*(pltpu.with_memory_space_constraint(a, pltpu.HBM) for a in args[:hbm]), *args[hbm:], *after)


def out(shape, dtype=jnp.float32):
    return pltpu.VMEM(shape, dtype)


def tile_of_heads(columns, tile, width, first=0):
    per, rows = LANES // width, columns.shape[0]
    lane = lax.broadcasted_iota(jnp.int32, (rows, LANES), 1)
    h = first + tile * per
    spread = jnp.broadcast_to(columns[:, h : h + 1], (rows, LANES))
    for k in range(1, per):
        other = jnp.broadcast_to(columns[:, h + k : h + k + 1], (rows, LANES))
        spread = jnp.where(lane < k * width, spread, other)
    return spread


def load_kernel(b_ref, c_ref, *refs):
    count = (len(refs) - 2) // 2
    sources, tails_ref, targets, sems = refs[:count], refs[count], refs[count + 1 : -1], refs[-1]
    tokens, state = b_ref.shape
    copies = [
        pltpu.make_async_copy(
            r.at[pl.ds(tokens - 8, 8), :], tails_ref.at[:, pl.ds(k * state, state)], sems.at[k]
        )
        for k, r in enumerate((b_ref, c_ref))
    ]
    for k, (source, target) in enumerate(zip(sources, targets)):
        copies.append(pltpu.make_async_copy(source, target, sems.at[k + 2]))
    for copy in copies:
        copy.start()
    for copy in copies:
        copy.wait()


def convolve(padded_ref, weight, bias, relative, start):
    tokens = relative.shape[0]
    taps = weight.shape[0]
    summed = jnp.broadcast_to(bias, (tokens, bias.shape[1]))
    for k in range(taps):
        back = taps - 1 - k
        term = weight[k : k + 1, :] * padded_ref[8 - back : 8 - back + tokens, :]
        summed = summed + jnp.where(relative - back >= start, term, 0.0)
    return (summed * jax.nn.sigmoid(summed)).astype(jnp.bfloat16)


def sequence_index():
    index = 0
    for axis in SEQ:
        index = index * lax.axis_size(axis) + lax.axis_index(axis)
    return index


def to_column(row):
    n = row.shape[1]
    same = lax.broadcasted_iota(jnp.int32, (n, n), 0) == lax.broadcasted_iota(jnp.int32, (n, n), 1)
    return jnp.sum(jnp.where(same, jnp.broadcast_to(row, (n, n)), 0.0), axis=1, keepdims=True)


WEIGHTS_AT = 32


def prepare_kernel(
    x_ref, raw_ref, bias_ref, rate_ref, docs_ref, b_ref, c_ref, taps_ref, taps_bias_ref,
    weighted_ref, cum_rows_ref, step_rows_ref, columns_ref, factor_ref, start_ref, b_conv_ref,
    c_conv_ref, stack_ref, padded_ref,
):
    heads, tokens = raw_ref.shape
    state = b_ref.shape[1]
    width = x_ref.shape[1] // heads
    base = sequence_index() * tokens
    relative = lax.broadcasted_iota(jnp.int32, (tokens, LANES), 0)
    start = jnp.zeros((1, 1), jnp.int32) - base
    last_position = jnp.full((1, 1), tokens - 1, jnp.int32)
    chosen = jnp.broadcast_to(start, relative.shape)
    end_start = start
    for i in range(1, docs_ref.shape[1]):
        start = start + docs_ref[0:1, i - 1 : i]
        chosen = jnp.where(start <= relative, start, chosen)
        end_start = jnp.where(start <= last_position, start, end_start)
    start_ref[...] = chosen

    step = jax.nn.softplus(raw_ref[...] + to_column(bias_ref[...]))
    log_decay = -step * to_column(rate_ref[...])
    rows = lax.broadcasted_iota(jnp.int32, (tokens, tokens), 0)
    cols = lax.broadcasted_iota(jnp.int32, (tokens, tokens), 1)
    cum = jnp.dot(
        log_decay, jnp.where(rows <= cols, 1.0, 0.0), precision=HIGHEST,
        preferred_element_type=jnp.float32,
    )
    cum_rows_ref[...] = cum
    step_rows_ref[...] = step
    position = lax.broadcasted_iota(jnp.int32, (heads, tokens), 1)
    weighting = jnp.where(
        position >= end_start, jnp.exp(cum[:, tokens - 1 : tokens] - cum) * step, 0.0
    )
    stack_ref[...] = jnp.zeros_like(stack_ref)
    stack_ref[0:heads, :] = cum
    stack_ref[WEIGHTS_AT : WEIGHTS_AT + heads, :] = weighting
    columns = stack_ref[...].T
    columns_ref[...] = columns
    factor_ref[...] = jnp.where(end_start < 0, jnp.exp(columns[tokens - 1 : tokens, :]), 0.0)
    for j in range(x_ref.shape[1] // LANES):
        tile = slice(j * LANES, (j + 1) * LANES)
        weighted_ref[:, tile] = (
            x_ref[:, tile].astype(jnp.float32) * tile_of_heads(columns, j, width, WEIGHTS_AT)
        ).astype(jnp.bfloat16)
    padded_ref[0:8, :] = jnp.zeros((8, state), jnp.float32)
    for k, (source_ref, target_ref) in enumerate(((b_ref, b_conv_ref), (c_ref, c_conv_ref))):
        side = slice(k * state, (k + 1) * state)
        padded_ref[8:, :] = source_ref[...].astype(jnp.float32)
        result = convolve(padded_ref, taps_ref[:, side], taps_bias_ref[:, side], relative, chosen)
        target_ref[...] = result.astype(target_ref.dtype)


def first_rows(source_ref, halo, weight, bias, start_ref, padded_ref):
    padded_ref[0:8, :] = halo.astype(jnp.float32)
    padded_ref[8:, :] = source_ref[0:8, :].astype(jnp.float32)
    relative = lax.broadcasted_iota(jnp.int32, (8, LANES), 0)
    return convolve(padded_ref, weight, bias, relative, start_ref[0:8, :])


def states_kernel(
    b_ref, halo_ref, taps_ref, taps_bias_ref, start_ref, b_early_ref, weighted_ref, factor_ref,
    pieces_ref, b_conv_ref, padded_ref,
):
    state, features = b_ref.shape[1], weighted_ref.shape[1]
    members, rows, _ = pieces_ref.shape
    first = first_rows(
        b_ref, halo_ref[:, 0:state], taps_ref[:, 0:state], taps_bias_ref[:, 0:state], start_ref,
        padded_ref,
    )
    b_conv = jnp.concatenate([first.astype(jnp.float32), b_early_ref[8:, :]], axis=0)
    b_conv_ref[...] = b_conv.astype(jnp.bfloat16)
    b_rows = b_conv.T.astype(jnp.bfloat16)
    for j in range(features // 256):
        tile = slice(j * 256, (j + 1) * 256)
        end_state = jnp.dot(b_rows, weighted_ref[:, tile], preferred_element_type=jnp.float32)
        for m in range(members):
            pieces_ref[m, :, tile] = end_state[m * rows : (m + 1) * rows, :]
    spread = jnp.broadcast_to(factor_ref[...], (rows, LANES))
    for m in range(members):
        pieces_ref[m, :, features:] = spread


def prefix_kernel(heads, pieces_ref, before_ref, factors_ref, total_ref, single_ref, wide_ref):
    members, rows, padded = pieces_ref.shape
    features = padded - LANES
    width = features // heads
    for m in range(members):
        single_ref[m : m + 1, :] = pieces_ref[m, 0:1, features:]
    single = single_ref[...]
    for j in range(features // LANES):
        wide_ref[:, j * LANES : (j + 1) * LANES] = tile_of_heads(single, j, width)
    product = jnp.ones((1, LANES), jnp.float32)
    for m in range(members):
        factors_ref[m : m + 1, :] = product
        product = product * single_ref[m : m + 1, :]
    total = jnp.zeros((rows, features), jnp.float32)
    for m in range(members):
        before_ref[m] = total
        total = wide_ref[m : m + 1, :] * total + pieces_ref[m, :, 0:features]
    total_ref[:, 0:features] = total
    total_ref[:, features:] = jnp.broadcast_to(product, (rows, LANES))


def wide_factor(pair_ref, features, width):
    factor = pair_ref[0:1, features:]
    return jnp.concatenate(
        [tile_of_heads(factor, j, width) for j in range(features // LANES)], axis=1
    )


def join_kernel(heads, own_ref, behind_ref, joined_ref):
    features = own_ref.shape[1] - LANES
    factor = wide_factor(own_ref, features, features // heads)
    joined_ref[:, 0:features] = factor * behind_ref[:, 0:features] + own_ref[:, 0:features]
    joined_ref[:, features:] = own_ref[:, features:] * behind_ref[:, features:]


def states_in_kernel(heads, near_ref, far_ref, before_ref, factors_ref, state_ref, wide_ref):
    members, rows, features = before_ref.shape
    width = features // heads
    factor = wide_factor(near_ref, features, width)
    entering = factor * far_ref[:, 0:features] + near_ref[:, 0:features]
    factors = factors_ref[...]
    for j in range(features // LANES):
        wide_ref[:, j * LANES : (j + 1) * LANES] = tile_of_heads(factors, j, width)
    for m in range(members):
        state_ref[m] = (wide_ref[m : m + 1, :] * entering + before_ref[m]).astype(jnp.bfloat16)


def diagonal_kernel(
    first_head, c_ref, halo_ref, taps_ref, taps_bias_ref, start_ref, c_early_ref, b_conv_ref,
    columns_ref, cum_rows_ref, step_rows_ref, x_ref, gate_ref, c_conv_ref, gated_ref, scale_ref,
    padded_ref, products_ref,
):
    tokens, state = c_ref.shape
    features, heads = x_ref.shape[1], cum_rows_ref.shape[0]
    width, half = features // heads, tokens // 2
    first = first_rows(
        c_ref, halo_ref[:, state:], taps_ref[:, state:], taps_bias_ref[:, state:], start_ref,
        padded_ref,
    )
    c_conv = jnp.concatenate(
        [first.astype(jnp.float32), c_early_ref[8:, :]], axis=0
    ).astype(jnp.bfloat16)
    c_conv_ref[...] = c_conv
    products = lax.dot_general(
        c_conv, b_conv_ref[...], (((1,), (1,)), ((), ())), preferred_element_type=jnp.float32
    )
    row = lax.broadcasted_iota(jnp.int32, (tokens, tokens), 0)
    col = lax.broadcasted_iota(jnp.int32, (tokens, tokens), 1)
    start = start_ref[...]
    starts = jnp.concatenate([start] * (tokens // LANES), axis=1)
    products_ref[...] = jnp.where((col <= row) & (col >= starts), products, 0.0)
    columns = columns_ref[...]
    carried = jnp.where(start < 0, jnp.exp(columns), 0.0)
    lane = lax.broadcasted_iota(jnp.int32, (tokens, LANES), 1)
    per = LANES // width
    for i in range(gated_ref.shape[1] // LANES):
        j = first_head // per + i
        tile = slice(j * LANES, (j + 1) * LANES)
        here = slice(i * LANES, (i + 1) * LANES)
        diagonal = None
        for k in range(per):
            h = j * per + k
            column = jnp.broadcast_to(columns[:, h : h + 1], (tokens, LANES))
            cum_row, step_row = cum_rows_ref[h : h + 1, :], step_rows_ref[h : h + 1, :]
            upper = (
                products_ref[0:half, 0:half] * jnp.exp(column[0:half] - cum_row[:, 0:half])
            ) * step_row[:, 0:half]
            lower_left = (
                products_ref[half:, 0:half] * jnp.exp(column[half:] - cum_row[:, 0:half])
            ) * step_row[:, 0:half]
            lower_right = (
                products_ref[half:, half:] * jnp.exp(column[half:] - cum_row[:, half:])
            ) * step_row[:, half:]
            lower = jnp.concatenate([lower_left, lower_right], axis=1).astype(jnp.bfloat16)
            part = jnp.concatenate(
                [
                    jnp.dot(upper.astype(jnp.bfloat16), x_ref[0:half, tile],
                            preferred_element_type=jnp.float32),
                    jnp.dot(lower, x_ref[:, tile], preferred_element_type=jnp.float32),
                ],
                axis=0,
            )
            diagonal = part if diagonal is None else jnp.where(lane < k * width, diagonal, part)
        gate = gate_ref[:, tile].astype(jnp.float32)
        gate = gate * jax.nn.sigmoid(gate)
        gated_ref[:, here] = diagonal * gate
        scale_ref[:, here] = tile_of_heads(carried, j, width) * gate


def gate_kernel(
    state_ref, c_conv_ref, diagonal_a_ref, scale_a_ref, diagonal_b_ref, scale_b_ref, gated_ref,
    squares_ref, rows_ref,
):
    members, rows, features = state_ref.shape
    for m in range(members):
        rows_ref[m * rows : (m + 1) * rows, :] = state_ref[m].astype(jnp.float32)
    c_conv = c_conv_ref[...]
    squares = jnp.zeros((c_conv.shape[0], LANES), jnp.float32)
    parts = diagonal_a_ref.shape[1] // LANES
    for j in range(features // LANES):
        tile = slice(j * LANES, (j + 1) * LANES)
        diagonal_ref, scale_ref = (
            (diagonal_a_ref, scale_a_ref) if j < parts else (diagonal_b_ref, scale_b_ref)
        )
        here = slice((j % parts) * LANES, (j % parts + 1) * LANES)
        carried = jnp.dot(
            c_conv, rows_ref[:, tile].astype(jnp.bfloat16), preferred_element_type=jnp.float32
        )
        gated = diagonal_ref[:, here] + scale_ref[:, here] * carried
        gated_ref[:, tile] = gated
        squares = squares + gated * gated
    squares_ref[...] = lax.dot_general(
        jnp.ones((8, LANES), jnp.float32), squares, (((1,), (1,)), ((), ())),
        precision=HIGHEST, preferred_element_type=jnp.float32,
    )[0:1]


def normalize_kernel(features_all, squares_ref, gated_ref, gain_ref, out_ref):
    count = squares_ref.shape[0]
    total = squares_ref[0]
    for k in range(1, count):
        total = total + squares_ref[k]
    first = lax.broadcasted_iota(jnp.int32, (8, total.shape[1]), 0) == 0
    column = lax.dot_general(
        jnp.where(first, jnp.broadcast_to(total, first.shape), 0.0),
        jnp.ones((8, LANES), jnp.float32), (((0,), (0,)), ((), ())),
        precision=HIGHEST, preferred_element_type=jnp.float32,
    )
    scale = lax.rsqrt(column / features_all + epsilon)
    for j in range(gated_ref.shape[1] // LANES):
        tile = slice(j * LANES, (j + 1) * LANES)
        out_ref[:, tile] = (gated_ref[:, tile] * scale * gain_ref[:, tile]).astype(jnp.bfloat16)


def body(
    inputs, gate_input, b_source, c_source, step_raw, step_bias, decay_rate, conv_weight,
    conv_bias, norm_gain, doc_lengths,
):
    tokens, features = inputs.shape
    heads = step_raw.shape[1]
    state = b_source.shape[1]
    members = 1
    for axis in GROUP:
        members *= lax.axis_size(axis)
    outer = lax.axis_size(OUTER)
    rows = state // members
    shards = members * outer
    ahead = lambda n, k: [(i, i + k) for i in range(n - k)]

    bf16 = jnp.bfloat16
    operands = [
        inputs, step_raw.T, step_bias[None, :], decay_rate[None, :], doc_lengths[None, :],
        b_source, c_source, conv_weight, conv_bias[None, :], norm_gain[None, :],
    ]
    tails, *loaded = call(
        load_kernel,
        [out((8, 2 * state), bf16)] + [out(o.shape, o.dtype) for o in operands],
        b_source, c_source, *operands,
        hbm=2 + len(operands),
        scratch=[pltpu.SemaphoreType.DMA((2 + len(operands),))],
    )
    x, raw, bias, rate, docs, b, c, taps, taps_bias, gain = loaded
    halo = lax.ppermute(tails, SEQ, ahead(shards, 1))
    weighted, cum_rows, step_rows, columns, factor, start, b_early, c_early = call(
        prepare_kernel,
        [
            out((tokens, features), bf16), out((heads, tokens)), out((heads, tokens)),
            out((tokens, LANES)), out((1, LANES)), out((tokens, LANES), jnp.int32),
            out((tokens, state)), out((tokens, state)),
        ],
        x, raw, bias, rate, docs, b, c, taps, taps_bias,
        scratch=[
            pltpu.VMEM((LANES, tokens), jnp.float32),
            pltpu.VMEM((tokens + 8, state), jnp.float32),
        ],
    )
    pieces, b_conv = call(
        states_kernel,
        [out((members, rows, features + LANES)), out((tokens, state), bf16)],
        b, halo, taps, taps_bias, start, b_early, weighted, factor,
        scratch=[pltpu.VMEM((16, state), jnp.float32)],
    )
    pieces = lax.all_to_all(pieces, GROUP, 0, 0)
    before, factors, total = call(
        functools.partial(prefix_kernel, heads),
        [out((members, rows, features)), out((members, LANES)), out((rows, features + LANES))],
        pieces,
        scratch=[
            pltpu.VMEM((members, LANES), jnp.float32),
            pltpu.VMEM((members, features), jnp.float32),
        ],
    )

    def diagonal_part(first_head):
        return call(
            functools.partial(diagonal_kernel, first_head),
            [out((tokens, state), bf16), out((tokens, features // 2)), out((tokens, features // 2))],
            c, halo, taps, taps_bias, start, c_early, b_conv, columns, cum_rows, step_rows, x,
            gate_input, flops=20_000_000_000,
            scratch=[
                pltpu.VMEM((16, state), jnp.float32),
                pltpu.VMEM((tokens, tokens), jnp.float32),
            ],
        )

    near = lax.ppermute(total, OUTER, ahead(outer, 1))
    c_conv, diagonal_a, scale_a = diagonal_part(0)
    joined = call(functools.partial(join_kernel, heads), out(total.shape), total, near, after=(c_conv,))
    far = lax.ppermute(joined, OUTER, ahead(outer, 2))
    _, diagonal_b, scale_b = diagonal_part(heads // 2)
    states_in = call(
        functools.partial(states_in_kernel, heads),
        out((members, rows, features), bf16),
        near, far, before, factors, after=(diagonal_b, scale_b),
        scratch=[pltpu.VMEM((members, features), jnp.float32)],
    )
    states_in = lax.all_to_all(states_in, GROUP, 0, 0)
    gated, squares = call(
        gate_kernel,
        [out((tokens, features)), out((1, tokens))],
        states_in, c_conv, diagonal_a, scale_a, diagonal_b, scale_b,
        scratch=[pltpu.VMEM((state, features), jnp.float32)],
    )
    squares = lax.all_gather(squares, "tp")
    return call(
        functools.partial(normalize_kernel, features * lax.axis_size("tp")),
        jax.ShapeDtypeStruct((tokens, features), bf16),
        squares, gated, gain,
    )


def solution(mesh):
    finer = Mesh(
        mesh.devices.reshape(4, 2, 4, 4, mesh.shape["tp"]), ("za", "zb", "y", "x", "tp")
    )
    in_specs = (
        P(SEQ, "tp"), P(SEQ, "tp"), P(SEQ, None), P(SEQ, None), P(SEQ, "tp"), P("tp"), P("tp"),
        P(), P(), P("tp"), P(),
    )
    return jax.shard_map(
        body, mesh=finer, in_specs=in_specs, out_specs=P(SEQ, "tp"), check_vma=False
    )
```

```python
import functools

import jax
import jax.numpy as jnp
from jax import lax
from jax.experimental import pallas as pl
from jax.experimental.pallas import tpu as pltpu
from jax.sharding import Mesh
from jax.sharding import PartitionSpec as P

SEQ = ("za", "zb", "y", "x")
GROUP = ("zb", "y", "x")
OUTER = "za"
LANES = 128
epsilon = 1e-05
HIGHEST = lax.Precision.HIGHEST
VMEM = pl.BlockSpec(memory_space=pltpu.VMEM)
HBM = pl.BlockSpec(memory_space=pltpu.HBM)


def call(kernel, outs, *args, hbm=0, after=(), scratch=(), flops=1_000_000):
    if after:
        inner, skip = kernel, len(after)
        kernel = lambda *refs: inner(*refs[:len(args)], *refs[len(args) + skip:])
    multiple = isinstance(outs, (list, tuple))
    return pl.pallas_call(
        kernel,
        out_shape=list(outs) if multiple else outs,
        in_specs=[HBM] * hbm + [VMEM] * (len(args) - hbm) + [VMEM] * len(after),
        out_specs=[VMEM] * len(outs) if multiple else VMEM,
        scratch_shapes=list(scratch),
        compiler_params=pltpu.CompilerParams(vmem_limit_bytes=24 * 1024 * 1024),
        cost_estimate=pl.CostEstimate(flops=flops, bytes_accessed=1_000_000, transcendentals=0),
    )(*(pltpu.with_memory_space_constraint(a, pltpu.HBM) for a in args[:hbm]), *args[hbm:], *after)


def out(shape, dtype=jnp.float32):
    return pltpu.VMEM(shape, dtype)


def tile_of_heads(columns, tile, width, first=0):
    per, rows = LANES // width, columns.shape[0]
    lane = lax.broadcasted_iota(jnp.int32, (rows, LANES), 1)
    h = first + tile * per
    spread = jnp.broadcast_to(columns[:, h : h + 1], (rows, LANES))
    for k in range(1, per):
        other = jnp.broadcast_to(columns[:, h + k : h + k + 1], (rows, LANES))
        spread = jnp.where(lane < k * width, spread, other)
    return spread


def tails_kernel(b_ref, c_ref, tails_ref, sems):
    tokens, state = b_ref.shape
    copies = [
        pltpu.make_async_copy(
            r.at[pl.ds(tokens - 8, 8), :], tails_ref.at[:, pl.ds(k * state, state)], sems.at[k]
        )
        for k, r in enumerate((b_ref, c_ref))
    ]
    for copy in copies:
        copy.start()
    for copy in copies:
        copy.wait()


def convolve(padded_ref, weight, bias, relative, start):
    tokens = relative.shape[0]
    taps = weight.shape[0]
    summed = jnp.broadcast_to(bias, (tokens, bias.shape[1]))
    for k in range(taps):
        back = taps - 1 - k
        term = weight[k : k + 1, :] * padded_ref[8 - back : 8 - back + tokens, :]
        summed = summed + jnp.where(relative - back >= start, term, 0.0)
    return (summed * jax.nn.sigmoid(summed)).astype(jnp.bfloat16)


def sequence_index():
    index = 0
    for axis in SEQ:
        index = index * lax.axis_size(axis) + lax.axis_index(axis)
    return index


def to_column(row):
    n = row.shape[1]
    same = lax.broadcasted_iota(jnp.int32, (n, n), 0) == lax.broadcasted_iota(jnp.int32, (n, n), 1)
    return jnp.sum(jnp.where(same, jnp.broadcast_to(row, (n, n)), 0.0), axis=1, keepdims=True)


WEIGHTS_AT = 32


def prepare_kernel(*refs):
    count, early = 10, 4
    sources, kept, results = refs[:count], refs[count : 2 * count - early], refs[2 * count - early :]
    (
        weighted_ref, cum_rows_ref, step_rows_ref, columns_ref, factor_ref, start_ref, b_conv_ref,
        c_conv_ref, stack_ref, padded_ref, sems, docs_ref, raw_ref, bias_ref, rate_ref,
    ) = results
    targets = (docs_ref, raw_ref, bias_ref, rate_ref, *kept)
    x_ref, b_ref, c_ref, taps_ref, taps_bias_ref, _ = kept
    copies = [
        pltpu.make_async_copy(source, target, sems.at[k])
        for k, (source, target) in enumerate(zip(sources, targets))
    ]
    for copy in copies:
        copy.start()
    for copy in copies[:early]:
        copy.wait()
    heads, tokens = raw_ref.shape
    state = b_ref.shape[1]
    width = x_ref.shape[1] // heads
    base = sequence_index() * tokens
    relative = lax.broadcasted_iota(jnp.int32, (tokens, LANES), 0)
    start = jnp.zeros((1, 1), jnp.int32) - base
    last_position = jnp.full((1, 1), tokens - 1, jnp.int32)
    chosen = jnp.broadcast_to(start, relative.shape)
    end_start = start
    for i in range(1, docs_ref.shape[1]):
        start = start + docs_ref[0:1, i - 1 : i]
        chosen = jnp.where(start <= relative, start, chosen)
        end_start = jnp.where(start <= last_position, start, end_start)
    start_ref[...] = chosen

    step = jax.nn.softplus(raw_ref[...] + to_column(bias_ref[...]))
    log_decay = -step * to_column(rate_ref[...])
    rows = lax.broadcasted_iota(jnp.int32, (tokens, tokens), 0)
    cols = lax.broadcasted_iota(jnp.int32, (tokens, tokens), 1)
    cum = jnp.dot(
        log_decay, jnp.where(rows <= cols, 1.0, 0.0), precision=HIGHEST,
        preferred_element_type=jnp.float32,
    )
    cum_rows_ref[...] = cum
    step_rows_ref[...] = step
    position = lax.broadcasted_iota(jnp.int32, (heads, tokens), 1)
    weighting = jnp.where(
        position >= end_start, jnp.exp(cum[:, tokens - 1 : tokens] - cum) * step, 0.0
    )
    stack_ref[...] = jnp.zeros_like(stack_ref)
    stack_ref[0:heads, :] = cum
    stack_ref[WEIGHTS_AT : WEIGHTS_AT + heads, :] = weighting
    columns = stack_ref[...].T
    columns_ref[...] = columns
    factor_ref[...] = jnp.where(end_start < 0, jnp.exp(columns[tokens - 1 : tokens, :]), 0.0)
    for copy in copies[early:]:
        copy.wait()
    for j in range(x_ref.shape[1] // LANES):
        tile = slice(j * LANES, (j + 1) * LANES)
        weighted_ref[:, tile] = (
            x_ref[:, tile].astype(jnp.float32) * tile_of_heads(columns, j, width, WEIGHTS_AT)
        ).astype(jnp.bfloat16)
    padded_ref[0:8, :] = jnp.zeros((8, state), jnp.float32)
    for k, (source_ref, target_ref) in enumerate(((b_ref, b_conv_ref), (c_ref, c_conv_ref))):
        side = slice(k * state, (k + 1) * state)
        padded_ref[8:, :] = source_ref[...].astype(jnp.float32)
        result = convolve(padded_ref, taps_ref[:, side], taps_bias_ref[:, side], relative, chosen)
        target_ref[...] = result.astype(target_ref.dtype)


def first_rows(source_ref, halo, weight, bias, start_ref, padded_ref):
    padded_ref[0:8, :] = halo.astype(jnp.float32)
    padded_ref[8:, :] = source_ref[0:8, :].astype(jnp.float32)
    relative = lax.broadcasted_iota(jnp.int32, (8, LANES), 0)
    return convolve(padded_ref, weight, bias, relative, start_ref[0:8, :])


def states_kernel(
    b_ref, halo_ref, taps_ref, taps_bias_ref, start_ref, b_early_ref, weighted_ref, factor_ref,
    pieces_ref, b_conv_ref, padded_ref,
):
    state, features = b_ref.shape[1], weighted_ref.shape[1]
    members, rows, _ = pieces_ref.shape
    first = first_rows(
        b_ref, halo_ref[:, 0:state], taps_ref[:, 0:state], taps_bias_ref[:, 0:state], start_ref,
        padded_ref,
    )
    b_conv = jnp.concatenate([first.astype(jnp.float32), b_early_ref[8:, :]], axis=0)
    b_conv_ref[...] = b_conv.astype(jnp.bfloat16)
    b_rows = b_conv.T.astype(jnp.bfloat16)
    for j in range(features // 256):
        tile = slice(j * 256, (j + 1) * 256)
        end_state = jnp.dot(b_rows, weighted_ref[:, tile], preferred_element_type=jnp.float32)
        for m in range(members):
            pieces_ref[m, :, tile] = end_state[m * rows : (m + 1) * rows, :]
    spread = jnp.broadcast_to(factor_ref[...], (rows, LANES))
    for m in range(members):
        pieces_ref[m, :, features:] = spread


def prefix_kernel(heads, pieces_ref, before_ref, factors_ref, total_ref, single_ref, wide_ref):
    members, rows, padded = pieces_ref.shape
    features = padded - LANES
    width = features // heads
    for m in range(members):
        single_ref[m : m + 1, :] = pieces_ref[m, 0:1, features:]
    single = single_ref[...]
    for j in range(features // LANES):
        wide_ref[:, j * LANES : (j + 1) * LANES] = tile_of_heads(single, j, width)
    product = jnp.ones((1, LANES), jnp.float32)
    for m in range(members):
        factors_ref[m : m + 1, :] = product
        product = product * single_ref[m : m + 1, :]
    total = jnp.zeros((rows, features), jnp.float32)
    for m in range(members):
        before_ref[m] = total
        total = wide_ref[m : m + 1, :] * total + pieces_ref[m, :, 0:features]
    total_ref[:, 0:features] = total
    total_ref[:, features:] = jnp.broadcast_to(product, (rows, LANES))


def wide_factor(pair_ref, features, width):
    factor = pair_ref[0:1, features:]
    return jnp.concatenate(
        [tile_of_heads(factor, j, width) for j in range(features // LANES)], axis=1
    )


def join_kernel(heads, own_ref, behind_ref, joined_ref):
    features = own_ref.shape[1] - LANES
    factor = wide_factor(own_ref, features, features // heads)
    joined_ref[:, 0:features] = factor * behind_ref[:, 0:features] + own_ref[:, 0:features]
    joined_ref[:, features:] = own_ref[:, features:] * behind_ref[:, features:]


def states_in_kernel(heads, near_ref, far_a_ref, far_b_ref, before_ref, factors_ref, state_ref, wide_ref):
    members, rows, features = before_ref.shape
    width = features // heads
    factor = wide_factor(near_ref, features, width)
    far = far_a_ref[:, 0:features] + far_b_ref[:, 0:features]
    entering = factor * far + near_ref[:, 0:features]
    factors = factors_ref[...]
    for j in range(features // LANES):
        wide_ref[:, j * LANES : (j + 1) * LANES] = tile_of_heads(factors, j, width)
    for m in range(members):
        state_ref[m] = (wide_ref[m : m + 1, :] * entering + before_ref[m]).astype(jnp.bfloat16)


def products_of(
    c_ref, halo_ref, taps_ref, taps_bias_ref, start_ref, c_early_ref, b_conv_ref, c_conv_ref,
    products_ref, padded_ref,
):
    tokens, state = c_ref.shape
    first = first_rows(
        c_ref, halo_ref[:, state:], taps_ref[:, state:], taps_bias_ref[:, state:], start_ref,
        padded_ref,
    )
    c_conv = jnp.concatenate(
        [first.astype(jnp.float32), c_early_ref[8:, :]], axis=0
    ).astype(jnp.bfloat16)
    c_conv_ref[...] = c_conv
    products = lax.dot_general(
        c_conv, b_conv_ref[...], (((1,), (1,)), ((), ())), preferred_element_type=jnp.float32
    )
    row = lax.broadcasted_iota(jnp.int32, (tokens, tokens), 0)
    col = lax.broadcasted_iota(jnp.int32, (tokens, tokens), 1)
    starts = jnp.concatenate([start_ref[...]] * (tokens // LANES), axis=1)
    products_ref[...] = jnp.where((col <= row) & (col >= starts), products, 0.0)


def diagonal_of(
    first_head, start_ref, columns_ref, cum_rows_ref, step_rows_ref, x_ref, gate_ref, products_ref,
    gated_ref, scale_ref,
):
    tokens, features = x_ref.shape
    width, half = features // cum_rows_ref.shape[0], tokens // 2
    columns = columns_ref[...]
    carried = jnp.where(start_ref[...] < 0, jnp.exp(columns), 0.0)
    lane = lax.broadcasted_iota(jnp.int32, (tokens, LANES), 1)
    per = LANES // width
    for i in range(gated_ref.shape[1] // LANES):
        j = first_head // per + i
        tile = slice(j * LANES, (j + 1) * LANES)
        here = slice(i * LANES, (i + 1) * LANES)
        diagonal = None
        for k in range(per):
            h = j * per + k
            column = jnp.broadcast_to(columns[:, h : h + 1], (tokens, LANES))
            cum_row, step_row = cum_rows_ref[h : h + 1, :], step_rows_ref[h : h + 1, :]
            upper = (
                products_ref[0:half, 0:half] * jnp.exp(column[0:half] - cum_row[:, 0:half])
            ) * step_row[:, 0:half]
            lower_left = (
                products_ref[half:, 0:half] * jnp.exp(column[half:] - cum_row[:, 0:half])
            ) * step_row[:, 0:half]
            lower_right = (
                products_ref[half:, half:] * jnp.exp(column[half:] - cum_row[:, half:])
            ) * step_row[:, half:]
            lower = jnp.concatenate([lower_left, lower_right], axis=1).astype(jnp.bfloat16)
            part = jnp.concatenate(
                [
                    jnp.dot(upper.astype(jnp.bfloat16), x_ref[0:half, tile],
                            preferred_element_type=jnp.float32),
                    jnp.dot(lower, x_ref[:, tile], preferred_element_type=jnp.float32),
                ],
                axis=0,
            )
            diagonal = part if diagonal is None else jnp.where(lane < k * width, diagonal, part)
        gate = gate_ref[:, tile].astype(jnp.float32)
        gate = gate * jax.nn.sigmoid(gate)
        gated_ref[:, here] = diagonal * gate
        scale_ref[:, here] = tile_of_heads(carried, j, width) * gate


def early_diagonal_kernel(*refs):
    (*sources, columns_ref, cum_rows_ref, step_rows_ref, x_ref, gate_ref) = refs[:12]
    c_conv_ref, products_ref, gated_ref, scale_ref, padded_ref = refs[12:]
    products_of(*sources, c_conv_ref, products_ref, padded_ref)
    diagonal_of(
        0, sources[4], columns_ref, cum_rows_ref, step_rows_ref, x_ref, gate_ref, products_ref,
        gated_ref, scale_ref,
    )


def gate_kernel(
    state_ref, c_conv_ref, diagonal_a_ref, scale_a_ref, diagonal_b_ref, scale_b_ref, gated_ref,
    squares_ref, rows_ref,
):
    members, rows, features = state_ref.shape
    for m in range(members):
        rows_ref[m * rows : (m + 1) * rows, :] = state_ref[m].astype(jnp.float32)
    c_conv = c_conv_ref[...]
    squares = jnp.zeros((c_conv.shape[0], LANES), jnp.float32)
    parts = diagonal_a_ref.shape[1] // LANES
    for j in range(features // LANES):
        tile = slice(j * LANES, (j + 1) * LANES)
        diagonal_ref, scale_ref = (
            (diagonal_a_ref, scale_a_ref) if j < parts else (diagonal_b_ref, scale_b_ref)
        )
        here = slice((j % parts) * LANES, (j % parts + 1) * LANES)
        carried = jnp.dot(
            c_conv, rows_ref[:, tile].astype(jnp.bfloat16), preferred_element_type=jnp.float32
        )
        gated = diagonal_ref[:, here] + scale_ref[:, here] * carried
        gated_ref[:, tile] = gated
        squares = squares + gated * gated
    squares_ref[...] = lax.dot_general(
        jnp.ones((8, LANES), jnp.float32), squares, (((1,), (1,)), ((), ())),
        precision=HIGHEST, preferred_element_type=jnp.float32,
    )[0:1]


def normalize_kernel(features_all, squares_ref, gated_ref, gain_ref, out_ref):
    count = squares_ref.shape[0]
    total = squares_ref[0]
    for k in range(1, count):
        total = total + squares_ref[k]
    first = lax.broadcasted_iota(jnp.int32, (8, total.shape[1]), 0) == 0
    column = lax.dot_general(
        jnp.where(first, jnp.broadcast_to(total, first.shape), 0.0),
        jnp.ones((8, LANES), jnp.float32), (((0,), (0,)), ((), ())),
        precision=HIGHEST, preferred_element_type=jnp.float32,
    )
    scale = lax.rsqrt(column / features_all + epsilon)
    for j in range(gated_ref.shape[1] // LANES):
        tile = slice(j * LANES, (j + 1) * LANES)
        gain = gain_ref[j : j + 1, :]
        out_ref[:, tile] = (gated_ref[:, tile] * scale * gain).astype(jnp.bfloat16)


def body(
    inputs, gate_input, b_source, c_source, step_raw, step_bias, decay_rate, conv_weight,
    conv_bias, norm_gain, doc_lengths,
):
    tokens, features = inputs.shape
    heads = step_raw.shape[1]
    state = b_source.shape[1]
    members = 1
    for axis in GROUP:
        members *= lax.axis_size(axis)
    outer = lax.axis_size(OUTER)
    rows = state // members
    shards = members * outer
    ahead = lambda n, k: [(i, i + k) for i in range(n - k)]

    bf16 = jnp.bfloat16
    tails = call(
        tails_kernel, out((8, 2 * state), bf16), b_source, c_source,
        hbm=2, scratch=[pltpu.SemaphoreType.DMA((2,))],
    )
    halo = lax.ppermute(tails, SEQ, ahead(shards, 1))
    operands = [
        doc_lengths[None, :], step_raw.T, step_bias[None, :], decay_rate[None, :], inputs,
        b_source, c_source, conv_weight, conv_bias[None, :],
        norm_gain.reshape(features // LANES, LANES),
    ]
    results = call(
        prepare_kernel,
        [out(o.shape, o.dtype) for o in operands[4:]]
        + [
            out((tokens, features), bf16), out((heads, tokens)), out((heads, tokens)),
            out((tokens, LANES)), out((1, LANES)), out((tokens, LANES), jnp.int32),
            out((tokens, state)), out((tokens, state)),
        ],
        *operands,
        hbm=len(operands), after=(tails,),
        scratch=[
            pltpu.VMEM((LANES, tokens), jnp.float32),
            pltpu.VMEM((tokens + 8, state), jnp.float32),
            pltpu.SemaphoreType.DMA((len(operands),)),
            *(pltpu.VMEM(o.shape, o.dtype) for o in operands[:4]),
        ],
    )
    x, b, c, taps, taps_bias, gain = results[0:6]
    weighted, cum_rows, step_rows, columns, factor, start, b_early, c_early = results[6:]
    pieces, b_conv = call(
        states_kernel,
        [out((members, rows, features + LANES)), out((tokens, state), bf16)],
        b, halo, taps, taps_bias, start, b_early, weighted, factor,
        scratch=[pltpu.VMEM((16, state), jnp.float32)],
    )
    pieces = lax.all_to_all(pieces, GROUP, 0, 0)
    before, factors, total = call(
        functools.partial(prefix_kernel, heads),
        [out((members, rows, features)), out((members, LANES)), out((rows, features + LANES))],
        pieces,
        scratch=[
            pltpu.VMEM((members, LANES), jnp.float32),
            pltpu.VMEM((members, features), jnp.float32),
        ],
    )

    near = lax.ppermute(total, OUTER, ahead(outer, 1))
    part = out((tokens, features // 2))
    c_conv, products, diagonal_a, scale_a = call(
        early_diagonal_kernel,
        [out((tokens, state), bf16), out((tokens, tokens)), part, part],
        c, halo, taps, taps_bias, start, c_early, b_conv, columns, cum_rows, step_rows, x,
        gate_input,
        scratch=[pltpu.VMEM((16, state), jnp.float32)],
    )
    joined = call(functools.partial(join_kernel, heads), out(total.shape), total, near, after=(c_conv,))
    far_a = lax.ppermute(joined, OUTER, [(1, 3)])
    far_b = lax.ppermute(near, OUTER, [(1, 2)])
    diagonal_b, scale_b = call(
        functools.partial(diagonal_of, heads // 2), [part, part],
        start, columns, cum_rows, step_rows, x, gate_input, products,
        flops=20_000_000_000,
    )
    states_in = call(
        functools.partial(states_in_kernel, heads),
        out((members, rows, features), bf16),
        near, far_a, far_b, before, factors, after=(diagonal_b, scale_b),
        scratch=[pltpu.VMEM((members, features), jnp.float32)],
    )
    states_in = lax.all_to_all(states_in, GROUP, 0, 0)
    gated, squares = call(
        gate_kernel,
        [out((tokens, features)), out((1, tokens))],
        states_in, c_conv, diagonal_a, scale_a, diagonal_b, scale_b,
        scratch=[pltpu.VMEM((state, features), jnp.float32)],
    )
    squares = lax.all_gather(squares, "tp")
    return call(
        functools.partial(normalize_kernel, features * lax.axis_size("tp")),
        jax.ShapeDtypeStruct((tokens, features), bf16),
        squares, gated, gain,
    )


def solution(mesh):
    finer = Mesh(
        mesh.devices.reshape(4, 2, 4, 4, mesh.shape["tp"]), ("za", "zb", "y", "x", "tp")
    )
    in_specs = (
        P(SEQ, "tp"), P(SEQ, "tp"), P(SEQ, None), P(SEQ, None), P(SEQ, "tp"), P("tp"), P("tp"),
        P(), P(), P("tp"), P(),
    )
    return jax.shard_map(
        body, mesh=finer, in_specs=in_specs, out_specs=P(SEQ, "tp"), check_vma=False
    )
```

```python
import functools

import jax
import jax.numpy as jnp
from jax import lax
from jax.experimental import pallas as pl
from jax.experimental.pallas import tpu as pltpu
from jax.sharding import Mesh
from jax.sharding import PartitionSpec as P

SEQ = ("za", "zb", "y", "x")
GROUP = ("zb", "y", "x")
OUTER = "za"
LANES = 128
epsilon = 1e-05
HIGHEST = lax.Precision.HIGHEST
VMEM = pl.BlockSpec(memory_space=pltpu.VMEM)
HBM = pl.BlockSpec(memory_space=pltpu.HBM)


def call(kernel, outs, *args, hbm=0, after=(), scratch=(), flops=1_000_000):
    if after:
        inner, skip = kernel, len(after)
        kernel = lambda *refs: inner(*refs[:len(args)], *refs[len(args) + skip:])
    multiple = isinstance(outs, (list, tuple))
    return pl.pallas_call(
        kernel,
        out_shape=list(outs) if multiple else outs,
        in_specs=[HBM] * hbm + [VMEM] * (len(args) - hbm) + [VMEM] * len(after),
        out_specs=[VMEM] * len(outs) if multiple else VMEM,
        scratch_shapes=list(scratch),
        compiler_params=pltpu.CompilerParams(vmem_limit_bytes=24 * 1024 * 1024),
        cost_estimate=pl.CostEstimate(flops=flops, bytes_accessed=1_000_000, transcendentals=0),
    )(*(pltpu.with_memory_space_constraint(a, pltpu.HBM) for a in args[:hbm]), *args[hbm:], *after)


def out(shape, dtype=jnp.float32):
    return pltpu.VMEM(shape, dtype)


def tile_of_heads(columns, tile, width, first=0):
    per, rows = LANES // width, columns.shape[0]
    lane = lax.broadcasted_iota(jnp.int32, (rows, LANES), 1)
    h = first + tile * per
    spread = jnp.broadcast_to(columns[:, h : h + 1], (rows, LANES))
    for k in range(1, per):
        other = jnp.broadcast_to(columns[:, h + k : h + k + 1], (rows, LANES))
        spread = jnp.where(lane < k * width, spread, other)
    return spread


def tails_kernel(b_ref, c_ref, tails_ref, sems):
    tokens, state = b_ref.shape
    copies = [
        pltpu.make_async_copy(
            r.at[pl.ds(tokens - 8, 8), :], tails_ref.at[:, pl.ds(k * state, state)], sems.at[k]
        )
        for k, r in enumerate((b_ref, c_ref))
    ]
    for copy in copies:
        copy.start()
    for copy in copies:
        copy.wait()


def convolve(padded_ref, weight, bias, relative, start):
    tokens = relative.shape[0]
    taps = weight.shape[0]
    summed = jnp.broadcast_to(bias, (tokens, bias.shape[1]))
    for k in range(taps):
        back = taps - 1 - k
        term = weight[k : k + 1, :] * padded_ref[8 - back : 8 - back + tokens, :]
        summed = summed + jnp.where(relative - back >= start, term, 0.0)
    return (summed * jax.nn.sigmoid(summed)).astype(jnp.bfloat16)


def sequence_index():
    index = 0
    for axis in SEQ:
        index = index * lax.axis_size(axis) + lax.axis_index(axis)
    return index


def to_column(row):
    n = row.shape[1]
    same = lax.broadcasted_iota(jnp.int32, (n, n), 0) == lax.broadcasted_iota(jnp.int32, (n, n), 1)
    return jnp.sum(jnp.where(same, jnp.broadcast_to(row, (n, n)), 0.0), axis=1, keepdims=True)


WEIGHTS_AT = 32


def prepare_kernel(*refs):
    count, early = 10, 4
    sources, kept, results = refs[:count], refs[count : 2 * count - early], refs[2 * count - early :]
    (
        weighted_ref, cum_rows_ref, step_rows_ref, columns_ref, factor_ref, start_ref, b_conv_ref,
        c_conv_ref, stack_ref, padded_ref, sems, docs_ref, raw_ref, bias_ref, rate_ref,
    ) = results
    targets = (docs_ref, raw_ref, bias_ref, rate_ref, *kept)
    x_ref, b_ref, c_ref, taps_ref, taps_bias_ref, _ = kept
    copies = [
        pltpu.make_async_copy(source, target, sems.at[k])
        for k, (source, target) in enumerate(zip(sources, targets))
    ]
    for copy in copies:
        copy.start()
    for copy in copies[:early]:
        copy.wait()
    heads, tokens = raw_ref.shape
    state = b_ref.shape[1]
    width = x_ref.shape[1] // heads
    base = sequence_index() * tokens
    relative = lax.broadcasted_iota(jnp.int32, (tokens, LANES), 0)
    start = jnp.zeros((1, 1), jnp.int32) - base
    last_position = jnp.full((1, 1), tokens - 1, jnp.int32)
    chosen = jnp.broadcast_to(start, relative.shape)
    end_start = start
    for i in range(1, docs_ref.shape[1]):
        start = start + docs_ref[0:1, i - 1 : i]
        chosen = jnp.where(start <= relative, start, chosen)
        end_start = jnp.where(start <= last_position, start, end_start)
    start_ref[...] = chosen

    step = jax.nn.softplus(raw_ref[...] + to_column(bias_ref[...]))
    log_decay = -step * to_column(rate_ref[...])
    rows = lax.broadcasted_iota(jnp.int32, (tokens, tokens), 0)
    cols = lax.broadcasted_iota(jnp.int32, (tokens, tokens), 1)
    cum = jnp.dot(
        log_decay, jnp.where(rows <= cols, 1.0, 0.0), precision=HIGHEST,
        preferred_element_type=jnp.float32,
    )
    cum_rows_ref[...] = cum
    step_rows_ref[...] = step
    position = lax.broadcasted_iota(jnp.int32, (heads, tokens), 1)
    weighting = jnp.where(
        position >= end_start, jnp.exp(cum[:, tokens - 1 : tokens] - cum) * step, 0.0
    )
    stack_ref[...] = jnp.zeros_like(stack_ref)
    stack_ref[0:heads, :] = cum
    stack_ref[WEIGHTS_AT : WEIGHTS_AT + heads, :] = weighting
    columns = stack_ref[...].T
    columns_ref[...] = columns
    factor_ref[...] = jnp.where(end_start < 0, jnp.exp(columns[tokens - 1 : tokens, :]), 0.0)
    for copy in copies[early:]:
        copy.wait()
    for j in range(x_ref.shape[1] // LANES):
        tile = slice(j * LANES, (j + 1) * LANES)
        weighted_ref[:, tile] = (
            x_ref[:, tile].astype(jnp.float32) * tile_of_heads(columns, j, width, WEIGHTS_AT)
        ).astype(jnp.bfloat16)
    padded_ref[0:8, :] = jnp.zeros((8, state), jnp.float32)
    for k, (source_ref, target_ref) in enumerate(((b_ref, b_conv_ref), (c_ref, c_conv_ref))):
        side = slice(k * state, (k + 1) * state)
        padded_ref[8:, :] = source_ref[...].astype(jnp.float32)
        result = convolve(padded_ref, taps_ref[:, side], taps_bias_ref[:, side], relative, chosen)
        target_ref[...] = result.astype(target_ref.dtype)


def first_rows(source_ref, halo, weight, bias, start_ref, padded_ref):
    padded_ref[0:8, :] = halo.astype(jnp.float32)
    padded_ref[8:, :] = source_ref[0:8, :].astype(jnp.float32)
    relative = lax.broadcasted_iota(jnp.int32, (8, LANES), 0)
    return convolve(padded_ref, weight, bias, relative, start_ref[0:8, :])


def states_kernel(
    b_ref, halo_ref, taps_ref, taps_bias_ref, start_ref, b_early_ref, weighted_ref, factor_ref,
    pieces_ref, b_conv_ref, padded_ref,
):
    state, features = b_ref.shape[1], weighted_ref.shape[1]
    members, rows, _ = pieces_ref.shape
    first = first_rows(
        b_ref, halo_ref[:, 0:state], taps_ref[:, 0:state], taps_bias_ref[:, 0:state], start_ref,
        padded_ref,
    )
    b_conv = jnp.concatenate([first.astype(jnp.float32), b_early_ref[8:, :]], axis=0)
    b_conv_ref[...] = b_conv.astype(jnp.bfloat16)
    b_rows = b_conv.T.astype(jnp.bfloat16)
    for j in range(features // 256):
        tile = slice(j * 256, (j + 1) * 256)
        end_state = jnp.dot(b_rows, weighted_ref[:, tile], preferred_element_type=jnp.float32)
        for m in range(members):
            pieces_ref[m, :, tile] = end_state[m * rows : (m + 1) * rows, :]
    spread = jnp.broadcast_to(factor_ref[...], (rows, LANES))
    for m in range(members):
        pieces_ref[m, :, features:] = spread


def prefix_kernel(heads, pieces_ref, before_ref, factors_ref, total_ref, single_ref, wide_ref):
    members, rows, padded = pieces_ref.shape
    features = padded - LANES
    width = features // heads
    for m in range(members):
        single_ref[m : m + 1, :] = pieces_ref[m, 0:1, features:]
    single = single_ref[...]
    for j in range(features // LANES):
        wide_ref[:, j * LANES : (j + 1) * LANES] = tile_of_heads(single, j, width)
    product = jnp.ones((1, LANES), jnp.float32)
    for m in range(members):
        factors_ref[m : m + 1, :] = product
        product = product * single_ref[m : m + 1, :]
    total = jnp.zeros((rows, features), jnp.float32)
    for m in range(members):
        before_ref[m] = total
        total = wide_ref[m : m + 1, :] * total + pieces_ref[m, :, 0:features]
    total_ref[:, 0:features] = total
    total_ref[:, features:] = jnp.broadcast_to(product, (rows, LANES))


def wide_factor(pair_ref, features, width):
    factor = pair_ref[0:1, features:]
    return jnp.concatenate(
        [tile_of_heads(factor, j, width) for j in range(features // LANES)], axis=1
    )


def join_kernel(heads, own_ref, behind_ref, joined_ref):
    features = own_ref.shape[1] - LANES
    factor = wide_factor(own_ref, features, features // heads)
    joined_ref[:, 0:features] = factor * behind_ref[:, 0:features] + own_ref[:, 0:features]
    joined_ref[:, features:] = own_ref[:, features:] * behind_ref[:, features:]


def states_in_kernel(
    heads, first_ref, second_ref, far_a_ref, far_b_ref, before_ref, factors_ref, state_ref, wide_ref
):
    members, rows, features = before_ref.shape
    width = features // heads
    factor = wide_factor(second_ref, features, width)
    far = far_a_ref[:, 0:features] + far_b_ref[:, 0:features]
    near = first_ref[:, 0:features] + second_ref[:, 0:features]
    entering = factor * far + near
    factors = factors_ref[...]
    for j in range(features // LANES):
        wide_ref[:, j * LANES : (j + 1) * LANES] = tile_of_heads(factors, j, width)
    for m in range(members):
        state_ref[m] = (wide_ref[m : m + 1, :] * entering + before_ref[m]).astype(jnp.bfloat16)


def products_of(
    c_ref, halo_ref, taps_ref, taps_bias_ref, start_ref, c_early_ref, b_conv_ref, c_conv_ref,
    products_ref, padded_ref,
):
    tokens, state = c_ref.shape
    first = first_rows(
        c_ref, halo_ref[:, state:], taps_ref[:, state:], taps_bias_ref[:, state:], start_ref,
        padded_ref,
    )
    c_conv = jnp.concatenate(
        [first.astype(jnp.float32), c_early_ref[8:, :]], axis=0
    ).astype(jnp.bfloat16)
    c_conv_ref[...] = c_conv
    products = lax.dot_general(
        c_conv, b_conv_ref[...], (((1,), (1,)), ((), ())), preferred_element_type=jnp.float32
    )
    row = lax.broadcasted_iota(jnp.int32, (tokens, tokens), 0)
    col = lax.broadcasted_iota(jnp.int32, (tokens, tokens), 1)
    starts = jnp.concatenate([start_ref[...]] * (tokens // LANES), axis=1)
    products_ref[...] = jnp.where((col <= row) & (col >= starts), products, 0.0)


def diagonal_of(
    start_ref, columns_ref, cum_rows_ref, step_rows_ref, x_ref, gate_ref, products_ref, gated_ref,
    scale_ref,
):
    tokens, features = x_ref.shape
    width, half = features // cum_rows_ref.shape[0], tokens // 2
    columns = columns_ref[...]
    carried = jnp.where(start_ref[...] < 0, jnp.exp(columns), 0.0)
    lane = lax.broadcasted_iota(jnp.int32, (tokens, LANES), 1)
    per = LANES // width
    for j in range(features // LANES):
        tile = slice(j * LANES, (j + 1) * LANES)
        diagonal = None
        for k in range(per):
            h = j * per + k
            column = jnp.broadcast_to(columns[:, h : h + 1], (tokens, LANES))
            cum_row, step_row = cum_rows_ref[h : h + 1, :], step_rows_ref[h : h + 1, :]
            upper = (
                products_ref[0:half, 0:half] * jnp.exp(column[0:half] - cum_row[:, 0:half])
            ) * step_row[:, 0:half]
            lower_left = (
                products_ref[half:, 0:half] * jnp.exp(column[half:] - cum_row[:, 0:half])
            ) * step_row[:, 0:half]
            lower_right = (
                products_ref[half:, half:] * jnp.exp(column[half:] - cum_row[:, half:])
            ) * step_row[:, half:]
            lower = jnp.concatenate([lower_left, lower_right], axis=1).astype(jnp.bfloat16)
            part = jnp.concatenate(
                [
                    jnp.dot(upper.astype(jnp.bfloat16), x_ref[0:half, tile],
                            preferred_element_type=jnp.float32),
                    jnp.dot(lower, x_ref[:, tile], preferred_element_type=jnp.float32),
                ],
                axis=0,
            )
            diagonal = part if diagonal is None else jnp.where(lane < k * width, diagonal, part)
        gate = gate_ref[:, tile].astype(jnp.float32)
        gate = gate * jax.nn.sigmoid(gate)
        gated_ref[:, tile] = diagonal * gate
        scale_ref[:, tile] = tile_of_heads(carried, j, width) * gate


def diagonal_kernel(*refs):
    (*sources, columns_ref, cum_rows_ref, step_rows_ref, x_ref, gate_ref) = refs[:12]
    c_conv_ref, gated_ref, scale_ref, products_ref, padded_ref = refs[12:]
    products_of(*sources, c_conv_ref, products_ref, padded_ref)
    diagonal_of(
        sources[4], columns_ref, cum_rows_ref, step_rows_ref, x_ref, gate_ref, products_ref,
        gated_ref, scale_ref,
    )


def gate_kernel(
    state_ref, c_conv_ref, diagonal_ref, scale_ref, gated_ref, squares_ref, rows_ref
):
    members, rows, features = state_ref.shape
    for m in range(members):
        rows_ref[m * rows : (m + 1) * rows, :] = state_ref[m].astype(jnp.float32)
    c_conv = c_conv_ref[...]
    squares = jnp.zeros((c_conv.shape[0], LANES), jnp.float32)
    for j in range(features // LANES):
        tile = slice(j * LANES, (j + 1) * LANES)
        carried = jnp.dot(
            c_conv, rows_ref[:, tile].astype(jnp.bfloat16), preferred_element_type=jnp.float32
        )
        gated = diagonal_ref[:, tile] + scale_ref[:, tile] * carried
        gated_ref[:, tile] = gated
        squares = squares + gated * gated
    squares_ref[...] = lax.dot_general(
        jnp.ones((8, LANES), jnp.float32), squares, (((1,), (1,)), ((), ())),
        precision=HIGHEST, preferred_element_type=jnp.float32,
    )[0:1]


def normalize_kernel(features_all, squares_ref, gated_ref, gain_ref, out_ref):
    count = squares_ref.shape[0]
    total = squares_ref[0]
    for k in range(1, count):
        total = total + squares_ref[k]
    first = lax.broadcasted_iota(jnp.int32, (8, total.shape[1]), 0) == 0
    column = lax.dot_general(
        jnp.where(first, jnp.broadcast_to(total, first.shape), 0.0),
        jnp.ones((8, LANES), jnp.float32), (((0,), (0,)), ((), ())),
        precision=HIGHEST, preferred_element_type=jnp.float32,
    )
    scale = lax.rsqrt(column / features_all + epsilon)
    for j in range(gated_ref.shape[1] // LANES):
        tile = slice(j * LANES, (j + 1) * LANES)
        gain = gain_ref[j : j + 1, :]
        out_ref[:, tile] = (gated_ref[:, tile] * scale * gain).astype(jnp.bfloat16)


def body(
    inputs, gate_input, b_source, c_source, step_raw, step_bias, decay_rate, conv_weight,
    conv_bias, norm_gain, doc_lengths,
):
    tokens, features = inputs.shape
    heads = step_raw.shape[1]
    state = b_source.shape[1]
    members = 1
    for axis in GROUP:
        members *= lax.axis_size(axis)
    outer = lax.axis_size(OUTER)
    rows = state // members
    shards = members * outer
    ahead = lambda n, k: [(i, i + k) for i in range(n - k)]

    bf16 = jnp.bfloat16
    tails = call(
        tails_kernel, out((8, 2 * state), bf16), b_source, c_source,
        hbm=2, scratch=[pltpu.SemaphoreType.DMA((2,))],
    )
    halo = lax.ppermute(tails, SEQ, ahead(shards, 1))
    operands = [
        doc_lengths[None, :], step_raw.T, step_bias[None, :], decay_rate[None, :], inputs,
        b_source, c_source, conv_weight, conv_bias[None, :],
        norm_gain.reshape(features // LANES, LANES),
    ]
    results = call(
        prepare_kernel,
        [out(o.shape, o.dtype) for o in operands[4:]]
        + [
            out((tokens, features), bf16), out((heads, tokens)), out((heads, tokens)),
            out((tokens, LANES)), out((1, LANES)), out((tokens, LANES), jnp.int32),
            out((tokens, state)), out((tokens, state)),
        ],
        *operands,
        hbm=len(operands), after=(tails,),
        scratch=[
            pltpu.VMEM((LANES, tokens), jnp.float32),
            pltpu.VMEM((tokens + 8, state), jnp.float32),
            pltpu.SemaphoreType.DMA((len(operands),)),
            *(pltpu.VMEM(o.shape, o.dtype) for o in operands[:4]),
        ],
    )
    x, b, c, taps, taps_bias, gain = results[0:6]
    weighted, cum_rows, step_rows, columns, factor, start, b_early, c_early = results[6:]
    pieces, b_conv = call(
        states_kernel,
        [out((members, rows, features + LANES)), out((tokens, state), bf16)],
        b, halo, taps, taps_bias, start, b_early, weighted, factor,
        scratch=[pltpu.VMEM((16, state), jnp.float32)],
    )
    pieces = lax.all_to_all(pieces, GROUP, 0, 0)
    before, factors, total = call(
        functools.partial(prefix_kernel, heads),
        [out((members, rows, features)), out((members, LANES)), out((rows, features + LANES))],
        pieces,
        scratch=[
            pltpu.VMEM((members, LANES), jnp.float32),
            pltpu.VMEM((members, features), jnp.float32),
        ],
    )

    first = lax.ppermute(total, OUTER, [(0, 1)])
    second = lax.ppermute(total, OUTER, [(1, 2), (2, 3)])
    joined = call(functools.partial(join_kernel, heads), out(total.shape), total, first)
    far_a = lax.ppermute(joined, OUTER, [(1, 3)])
    far_b = lax.ppermute(first, OUTER, [(1, 2)])
    c_conv, diagonal, scale = call(
        diagonal_kernel,
        [out((tokens, state), bf16), out((tokens, features)), out((tokens, features))],
        c, halo, taps, taps_bias, start, c_early, b_conv, columns, cum_rows, step_rows, x,
        gate_input, after=(joined,), flops=20_000_000_000,
        scratch=[
            pltpu.VMEM((tokens, tokens), jnp.float32),
            pltpu.VMEM((16, state), jnp.float32),
        ],
    )
    states_in = call(
        functools.partial(states_in_kernel, heads),
        out((members, rows, features), bf16),
        first, second, far_a, far_b, before, factors, after=(diagonal, scale),
        scratch=[pltpu.VMEM((members, features), jnp.float32)],
    )
    states_in = lax.all_to_all(states_in, GROUP, 0, 0)
    gated, squares = call(
        gate_kernel,
        [out((tokens, features)), out((1, tokens))],
        states_in, c_conv, diagonal, scale,
        scratch=[pltpu.VMEM((state, features), jnp.float32)],
    )
    squares = lax.all_gather(squares, "tp")
    return call(
        functools.partial(normalize_kernel, features * lax.axis_size("tp")),
        jax.ShapeDtypeStruct((tokens, features), bf16),
        squares, gated, gain,
    )


def solution(mesh):
    finer = Mesh(
        mesh.devices.reshape(4, 2, 4, 4, mesh.shape["tp"]), ("za", "zb", "y", "x", "tp")
    )
    in_specs = (
        P(SEQ, "tp"), P(SEQ, "tp"), P(SEQ, None), P(SEQ, None), P(SEQ, "tp"), P("tp"), P("tp"),
        P(), P(), P("tp"), P(),
    )
    return jax.shard_map(
        body, mesh=finer, in_specs=in_specs, out_specs=P(SEQ, "tp"), check_vma=False
    )
```

```python
import functools

import jax
import jax.numpy as jnp
from jax import lax
from jax.experimental import pallas as pl
from jax.experimental.pallas import tpu as pltpu
from jax.sharding import Mesh
from jax.sharding import PartitionSpec as P

SEQ = ("za", "zb", "y", "x")
GROUP = ("zb", "y", "x")
OUTER = "za"
LANES = 128
epsilon = 1e-05
HIGHEST = lax.Precision.HIGHEST
VMEM = pl.BlockSpec(memory_space=pltpu.VMEM)
HBM = pl.BlockSpec(memory_space=pltpu.HBM)


def call(
    kernel, outs, *args, hbm=0, after=(), scratch=(), flops=1_000_000, aliases=None, to_hbm=False
):
    if after:
        inner, skip = kernel, len(after)
        kernel = lambda *refs: inner(*refs[:len(args)], *refs[len(args) + skip:])
    multiple = isinstance(outs, (list, tuple))
    return pl.pallas_call(
        kernel,
        out_shape=list(outs) if multiple else outs,
        in_specs=[HBM] * hbm + [VMEM] * (len(args) - hbm) + [VMEM] * len(after),
        out_specs=[VMEM] * len(outs) if multiple else HBM if to_hbm else VMEM,
        input_output_aliases=aliases or {},
        scratch_shapes=list(scratch),
        compiler_params=pltpu.CompilerParams(vmem_limit_bytes=24 * 1024 * 1024),
        cost_estimate=pl.CostEstimate(flops=flops, bytes_accessed=1_000_000, transcendentals=0),
    )(*(pltpu.with_memory_space_constraint(a, pltpu.HBM) for a in args[:hbm]), *args[hbm:], *after)


def out(shape, dtype=jnp.float32):
    return pltpu.VMEM(shape, dtype)


def tile_of_heads(columns, tile, width, first=0):
    per, rows = LANES // width, columns.shape[0]
    lane = lax.broadcasted_iota(jnp.int32, (rows, LANES), 1)
    h = first + tile * per
    spread = jnp.broadcast_to(columns[:, h : h + 1], (rows, LANES))
    for k in range(1, per):
        other = jnp.broadcast_to(columns[:, h + k : h + k + 1], (rows, LANES))
        spread = jnp.where(lane < k * width, spread, other)
    return spread


def tails_kernel(b_ref, c_ref, *refs):
    count = (len(refs) - 2) // 2
    sources, tails_ref, targets, sems = refs[:count], refs[count], refs[count + 1 : -1], refs[-1]
    tokens, state = b_ref.shape
    copies = [
        pltpu.make_async_copy(
            r.at[pl.ds(tokens - 8, 8), :], tails_ref.at[:, pl.ds(k * state, state)], sems.at[k]
        )
        for k, r in enumerate((b_ref, c_ref))
    ]
    for k, (source, target) in enumerate(zip(sources, targets)):
        copies.append(pltpu.make_async_copy(source, target, sems.at[k + 2]))
    for copy in copies:
        copy.start()
    for copy in copies:
        copy.wait()


def convolve(padded_ref, weight, bias, relative, start):
    tokens = relative.shape[0]
    taps = weight.shape[0]
    summed = jnp.broadcast_to(bias, (tokens, bias.shape[1]))
    for k in range(taps):
        back = taps - 1 - k
        term = weight[k : k + 1, :] * padded_ref[8 - back : 8 - back + tokens, :]
        summed = summed + jnp.where(relative - back >= start, term, 0.0)
    return (summed * jax.nn.sigmoid(summed)).astype(jnp.bfloat16)


def sequence_index():
    index = 0
    for axis in SEQ:
        index = index * lax.axis_size(axis) + lax.axis_index(axis)
    return index


def to_column(row):
    n = row.shape[1]
    same = lax.broadcasted_iota(jnp.int32, (n, n), 0) == lax.broadcasted_iota(jnp.int32, (n, n), 1)
    return jnp.sum(jnp.where(same, jnp.broadcast_to(row, (n, n)), 0.0), axis=1, keepdims=True)


WEIGHTS_AT = 32


def prepare_kernel(*refs):
    count = 6
    sources, (docs_ref, raw_ref, bias_ref, rate_ref, _) = refs[:count], refs[count : count + 5]
    targets = refs[count + 5 : 2 * count + 5]
    (
        weighted_ref, cum_rows_ref, step_rows_ref, columns_ref, factor_ref, start_ref, b_conv_ref,
        c_conv_ref, stack_ref, padded_ref, sems,
    ) = refs[2 * count + 5 :]
    x_ref, b_ref, c_ref, taps_ref, taps_bias_ref, _ = targets
    copies = [
        pltpu.make_async_copy(source, target, sems.at[k])
        for k, (source, target) in enumerate(zip(sources, targets))
    ]
    for copy in copies:
        copy.start()
    heads, tokens = raw_ref.shape
    state = b_ref.shape[1]
    width = x_ref.shape[1] // heads
    base = sequence_index() * tokens
    relative = lax.broadcasted_iota(jnp.int32, (tokens, LANES), 0)
    start = jnp.zeros((1, 1), jnp.int32) - base
    last_position = jnp.full((1, 1), tokens - 1, jnp.int32)
    chosen = jnp.broadcast_to(start, relative.shape)
    end_start = start
    for i in range(1, docs_ref.shape[1]):
        start = start + docs_ref[0:1, i - 1 : i]
        chosen = jnp.where(start <= relative, start, chosen)
        end_start = jnp.where(start <= last_position, start, end_start)
    start_ref[...] = chosen

    step = jax.nn.softplus(raw_ref[...] + to_column(bias_ref[...]))
    log_decay = -step * to_column(rate_ref[...])
    rows = lax.broadcasted_iota(jnp.int32, (tokens, tokens), 0)
    cols = lax.broadcasted_iota(jnp.int32, (tokens, tokens), 1)
    cum = jnp.dot(
        log_decay, jnp.where(rows <= cols, 1.0, 0.0), precision=HIGHEST,
        preferred_element_type=jnp.float32,
    )
    cum_rows_ref[...] = cum
    step_rows_ref[...] = step
    position = lax.broadcasted_iota(jnp.int32, (heads, tokens), 1)
    weighting = jnp.where(
        position >= end_start, jnp.exp(cum[:, tokens - 1 : tokens] - cum) * step, 0.0
    )
    stack_ref[...] = jnp.zeros_like(stack_ref)
    stack_ref[0:heads, :] = cum
    stack_ref[WEIGHTS_AT : WEIGHTS_AT + heads, :] = weighting
    columns = stack_ref[...].T
    columns_ref[...] = columns
    factor_ref[...] = jnp.where(end_start < 0, jnp.exp(columns[tokens - 1 : tokens, :]), 0.0)
    for copy in copies:
        copy.wait()
    for j in range(x_ref.shape[1] // LANES):
        tile = slice(j * LANES, (j + 1) * LANES)
        weighted_ref[:, tile] = (
            x_ref[:, tile].astype(jnp.float32) * tile_of_heads(columns, j, width, WEIGHTS_AT)
        ).astype(jnp.bfloat16)
    padded_ref[0:8, :] = jnp.zeros((8, state), jnp.float32)
    for k, (source_ref, target_ref) in enumerate(((b_ref, b_conv_ref), (c_ref, c_conv_ref))):
        side = slice(k * state, (k + 1) * state)
        padded_ref[8:, :] = source_ref[...].astype(jnp.float32)
        result = convolve(padded_ref, taps_ref[:, side], taps_bias_ref[:, side], relative, chosen)
        target_ref[...] = result.astype(target_ref.dtype)


def first_rows(source_ref, halo, weight, bias, start_ref, padded_ref):
    padded_ref[0:8, :] = halo.astype(jnp.float32)
    padded_ref[8:, :] = source_ref[0:8, :].astype(jnp.float32)
    relative = lax.broadcasted_iota(jnp.int32, (8, LANES), 0)
    return convolve(padded_ref, weight, bias, relative, start_ref[0:8, :])


def states_kernel(
    b_ref, halo_ref, taps_ref, taps_bias_ref, start_ref, b_early_ref, weighted_ref, factor_ref,
    pieces_ref, b_conv_ref, padded_ref,
):
    state, features = b_ref.shape[1], weighted_ref.shape[1]
    members, rows, _ = pieces_ref.shape
    first = first_rows(
        b_ref, halo_ref[:, 0:state], taps_ref[:, 0:state], taps_bias_ref[:, 0:state], start_ref,
        padded_ref,
    )
    b_conv = jnp.concatenate([first.astype(jnp.float32), b_early_ref[8:, :]], axis=0)
    b_conv_ref[...] = b_conv.astype(jnp.bfloat16)
    b_rows = b_conv.T.astype(jnp.bfloat16)
    for j in range(features // 256):
        tile = slice(j * 256, (j + 1) * 256)
        end_state = jnp.dot(b_rows, weighted_ref[:, tile], preferred_element_type=jnp.float32)
        for m in range(members):
            pieces_ref[m, :, tile] = end_state[m * rows : (m + 1) * rows, :]
    spread = jnp.broadcast_to(factor_ref[...], (rows, LANES))
    for m in range(members):
        pieces_ref[m, :, features:] = spread


def prefix_kernel(
    heads, pieces_ref, before_ref, factors_ref, total_a_ref, total_b_ref, single_ref, wide_ref
):
    members, rows, padded = pieces_ref.shape
    features = padded - LANES
    width = features // heads
    for m in range(members):
        single_ref[m : m + 1, :] = pieces_ref[m, 0:1, features:]
    single = single_ref[...]
    for j in range(features // LANES):
        wide_ref[:, j * LANES : (j + 1) * LANES] = tile_of_heads(single, j, width)
    product = jnp.ones((1, LANES), jnp.float32)
    for m in range(members):
        factors_ref[m : m + 1, :] = product
        product = product * single_ref[m : m + 1, :]
    total = jnp.zeros((rows, features), jnp.float32)
    for m in range(members):
        before_ref[m] = total
        total = wide_ref[m : m + 1, :] * total + pieces_ref[m, :, 0:features]
    for total_ref in (total_a_ref, total_b_ref):
        total_ref[:, 0:features] = total
        total_ref[:, features:] = jnp.broadcast_to(product, (rows, LANES))


def wide_factor(pair_ref, features, width):
    factor = pair_ref[0:1, features:]
    return jnp.concatenate(
        [tile_of_heads(factor, j, width) for j in range(features // LANES)], axis=1
    )


def join_kernel(heads, own_ref, behind_ref, joined_ref):
    features = own_ref.shape[1] - LANES
    factor = wide_factor(own_ref, features, features // heads)
    joined_ref[:, 0:features] = factor * behind_ref[:, 0:features] + own_ref[:, 0:features]
    joined_ref[:, features:] = own_ref[:, features:] * behind_ref[:, features:]


def states_in_kernel(
    heads, first_ref, second_ref, far_a_ref, far_b_ref, before_ref, factors_ref, state_ref, wide_ref
):
    members, rows, features = before_ref.shape
    width = features // heads
    factor = wide_factor(second_ref, features, width)
    far = far_a_ref[:, 0:features] + far_b_ref[:, 0:features]
    near = first_ref[:, 0:features] + second_ref[:, 0:features]
    entering = factor * far + near
    factors = factors_ref[...]
    for j in range(features // LANES):
        wide_ref[:, j * LANES : (j + 1) * LANES] = tile_of_heads(factors, j, width)
    for m in range(members):
        state_ref[m] = (wide_ref[m : m + 1, :] * entering + before_ref[m]).astype(jnp.bfloat16)


def products_of(
    c_ref, halo_ref, taps_ref, taps_bias_ref, start_ref, c_early_ref, b_conv_ref, c_conv_ref,
    products_ref, padded_ref,
):
    tokens, state = c_ref.shape
    first = first_rows(
        c_ref, halo_ref[:, state:], taps_ref[:, state:], taps_bias_ref[:, state:], start_ref,
        padded_ref,
    )
    c_conv = jnp.concatenate(
        [first.astype(jnp.float32), c_early_ref[8:, :]], axis=0
    ).astype(jnp.bfloat16)
    c_conv_ref[...] = c_conv
    products = lax.dot_general(
        c_conv, b_conv_ref[...], (((1,), (1,)), ((), ())), preferred_element_type=jnp.float32
    )
    row = lax.broadcasted_iota(jnp.int32, (tokens, tokens), 0)
    col = lax.broadcasted_iota(jnp.int32, (tokens, tokens), 1)
    starts = jnp.concatenate([start_ref[...]] * (tokens // LANES), axis=1)
    products_ref[...] = jnp.where((col <= row) & (col >= starts), products, 0.0)


def diagonal_of(
    start_ref, columns_ref, cum_rows_ref, step_rows_ref, x_ref, gate_ref, products_ref, gated_ref,
    scale_ref,
):
    tokens, features = x_ref.shape
    width, half = features // cum_rows_ref.shape[0], tokens // 2
    columns = columns_ref[...]
    carried = jnp.where(start_ref[...] < 0, jnp.exp(columns), 0.0)
    lane = lax.broadcasted_iota(jnp.int32, (tokens, LANES), 1)
    per = LANES // width
    for j in range(features // LANES):
        tile = slice(j * LANES, (j + 1) * LANES)
        diagonal = None
        for k in range(per):
            h = j * per + k
            column = jnp.broadcast_to(columns[:, h : h + 1], (tokens, LANES))
            cum_row, step_row = cum_rows_ref[h : h + 1, :], step_rows_ref[h : h + 1, :]
            upper = (
                products_ref[0:half, 0:half] * jnp.exp(column[0:half] - cum_row[:, 0:half])
            ) * step_row[:, 0:half]
            lower_left = (
                products_ref[half:, 0:half] * jnp.exp(column[half:] - cum_row[:, 0:half])
            ) * step_row[:, 0:half]
            lower_right = (
                products_ref[half:, half:] * jnp.exp(column[half:] - cum_row[:, half:])
            ) * step_row[:, half:]
            lower = jnp.concatenate([lower_left, lower_right], axis=1).astype(jnp.bfloat16)
            part = jnp.concatenate(
                [
                    jnp.dot(upper.astype(jnp.bfloat16), x_ref[0:half, tile],
                            preferred_element_type=jnp.float32),
                    jnp.dot(lower, x_ref[:, tile], preferred_element_type=jnp.float32),
                ],
                axis=0,
            )
            diagonal = part if diagonal is None else jnp.where(lane < k * width, diagonal, part)
        gate = gate_ref[:, tile].astype(jnp.float32)
        gate = gate * jax.nn.sigmoid(gate)
        gated_ref[:, tile] = diagonal * gate
        scale_ref[:, tile] = tile_of_heads(carried, j, width) * gate


def diagonal_kernel(groups, *refs):
    (*sources, columns_ref, cum_rows_ref, step_rows_ref, x_ref, gate_ref) = refs[:12]
    _, c_conv_ref, gated_ref, scale_ref, products_ref, padded_ref = refs[-6:]
    place = lax.axis_index(OUTER)

    @pl.when((place >= groups[0]) & (place <= groups[-1]))
    def _():
        products_of(*sources, c_conv_ref, products_ref, padded_ref)
        diagonal_of(
            sources[4], columns_ref, cum_rows_ref, step_rows_ref, x_ref, gate_ref, products_ref,
            gated_ref, scale_ref,
        )


def gate_kernel(
    state_ref, c_conv_ref, diagonal_ref, scale_ref, gated_ref, squares_ref, rows_ref
):
    members, rows, features = state_ref.shape
    for m in range(members):
        rows_ref[m * rows : (m + 1) * rows, :] = state_ref[m].astype(jnp.float32)
    c_conv = c_conv_ref[...]
    squares = jnp.zeros((c_conv.shape[0], LANES), jnp.float32)
    for j in range(features // LANES):
        tile = slice(j * LANES, (j + 1) * LANES)
        carried = jnp.dot(
            c_conv, rows_ref[:, tile].astype(jnp.bfloat16), preferred_element_type=jnp.float32
        )
        gated = diagonal_ref[:, tile] + scale_ref[:, tile] * carried
        gated_ref[:, tile] = gated
        squares = squares + gated * gated
    squares_ref[...] = lax.dot_general(
        jnp.ones((8, LANES), jnp.float32), squares, (((1,), (1,)), ((), ())),
        precision=HIGHEST, preferred_element_type=jnp.float32,
    )[0:1]


def normalize_kernel(features_all, squares_ref, gated_ref, gain_ref, out_ref, rows_ref, sems):
    count = squares_ref.shape[0]
    tokens, features = gated_ref.shape
    total = squares_ref[0]
    for k in range(1, count):
        total = total + squares_ref[k]
    first = lax.broadcasted_iota(jnp.int32, (8, total.shape[1]), 0) == 0
    column = lax.dot_general(
        jnp.where(first, jnp.broadcast_to(total, first.shape), 0.0),
        jnp.ones((8, LANES), jnp.float32), (((0,), (0,)), ((), ())),
        precision=HIGHEST, preferred_element_type=jnp.float32,
    )
    scale = lax.rsqrt(column / features_all + epsilon)
    chunks = sems.shape[0]
    size = tokens // chunks
    copies = []
    for i in range(chunks):
        part = slice(i * size, (i + 1) * size)
        for j in range(features // LANES):
            tile = slice(j * LANES, (j + 1) * LANES)
            rows_ref[part, tile] = (
                gated_ref[part, tile] * scale[part] * gain_ref[j : j + 1, :]
            ).astype(jnp.bfloat16)
        copies.append(
            pltpu.make_async_copy(
                rows_ref.at[pl.ds(i * size, size), :], out_ref.at[pl.ds(i * size, size), :],
                sems.at[i],
            )
        )
        copies[-1].start()
    for copy in copies:
        copy.wait()


def body(
    inputs, gate_input, b_source, c_source, step_raw, step_bias, decay_rate, conv_weight,
    conv_bias, norm_gain, doc_lengths,
):
    tokens, features = inputs.shape
    heads = step_raw.shape[1]
    state = b_source.shape[1]
    members = 1
    for axis in GROUP:
        members *= lax.axis_size(axis)
    outer = lax.axis_size(OUTER)
    rows = state // members
    shards = members * outer
    ahead = lambda n, k: [(i, i + k) for i in range(n - k)]

    bf16 = jnp.bfloat16
    small = [doc_lengths[None, :], step_raw.T, step_bias[None, :], decay_rate[None, :]]
    tails, *small = call(
        tails_kernel,
        [out((8, 2 * state), bf16)] + [out(o.shape, o.dtype) for o in small],
        b_source, c_source, *small,
        hbm=2 + len(small), scratch=[pltpu.SemaphoreType.DMA((2 + len(small),))],
    )
    halo = lax.ppermute(tails, SEQ, ahead(shards, 1))
    operands = [
        inputs, b_source, c_source, conv_weight, conv_bias[None, :],
        norm_gain.reshape(features // LANES, LANES),
    ]
    results = call(
        prepare_kernel,
        [out(o.shape, o.dtype) for o in operands]
        + [
            out((tokens, features), bf16), out((heads, tokens)), out((heads, tokens)),
            out((tokens, LANES)), out((1, LANES)), out((tokens, LANES), jnp.int32),
            out((tokens, state)), out((tokens, state)),
        ],
        *operands, *small, tails,
        hbm=len(operands),
        scratch=[
            pltpu.VMEM((LANES, tokens), jnp.float32),
            pltpu.VMEM((tokens + 8, state), jnp.float32),
            pltpu.SemaphoreType.DMA((len(operands),)),
        ],
    )
    x, b, c, taps, taps_bias, gain = results[0:6]
    weighted, cum_rows, step_rows, columns, factor, start, b_early, c_early = results[6:]
    pieces, b_conv = call(
        states_kernel,
        [out((members, rows, features + LANES)), out((tokens, state), bf16)],
        b, halo, taps, taps_bias, start, b_early, weighted, factor,
        scratch=[pltpu.VMEM((16, state), jnp.float32)],
    )
    pieces = lax.all_to_all(pieces, GROUP, 0, 0)
    pair = out((rows, features + LANES))
    before, factors, total_a, total_b = call(
        functools.partial(prefix_kernel, heads),
        [out((members, rows, features)), out((members, LANES)), pair, pair],
        pieces,
        scratch=[
            pltpu.VMEM((members, LANES), jnp.float32),
            pltpu.VMEM((members, features), jnp.float32),
        ],
    )

    def diagonal_terms(groups, token, *before, late=()):
        sources = [
            c, halo, taps, taps_bias, start, c_early, b_conv, columns, cum_rows, step_rows, x,
            gate_input,
        ]
        count = len(sources)
        return call(
            functools.partial(diagonal_kernel, groups),
            [
                out(token.shape), out((tokens, state), bf16), out((tokens, features)),
                out((tokens, features)),
            ],
            *sources, token, *before, after=late, flops=20_000_000_000,
            aliases={count + k: k for k in range(1 + len(before))},
            scratch=[
                pltpu.VMEM((tokens, tokens), jnp.float32),
                pltpu.VMEM((16, state), jnp.float32),
            ],
        )

    total_a, *diagonal = diagonal_terms((0,), total_a)
    first = lax.ppermute(total_a, OUTER, [(0, 1)])
    total_b, *diagonal = diagonal_terms((1,), total_b, *diagonal)
    second = lax.ppermute(total_b, OUTER, [(1, 2), (2, 3)])
    joined = call(functools.partial(join_kernel, heads), pair, total_b, first)
    far_a = lax.ppermute(joined, OUTER, [(1, 3)])
    far_b = lax.ppermute(first, OUTER, [(1, 2)])
    factors, *diagonal = diagonal_terms((2, 3), factors, *diagonal, late=(joined,))
    c_conv, diagonal, scale = diagonal
    states_in = call(
        functools.partial(states_in_kernel, heads),
        out((members, rows, features), bf16),
        first, second, far_a, far_b, before, factors,
        scratch=[pltpu.VMEM((members, features), jnp.float32)],
    )
    states_in = lax.all_to_all(states_in, GROUP, 0, 0)
    gated, squares = call(
        gate_kernel,
        [out((tokens, features)), out((1, tokens))],
        states_in, c_conv, diagonal, scale,
        scratch=[pltpu.VMEM((state, features), jnp.float32)],
    )
    squares = lax.all_gather(squares, "tp")
    return call(
        functools.partial(normalize_kernel, features * lax.axis_size("tp")),
        jax.ShapeDtypeStruct((tokens, features), bf16),
        squares, gated, gain, to_hbm=True,
        scratch=[pltpu.VMEM((tokens, features), bf16), pltpu.SemaphoreType.DMA((4,))],
    )


def solution(mesh):
    finer = Mesh(
        mesh.devices.reshape(4, 2, 4, 4, mesh.shape["tp"]), ("za", "zb", "y", "x", "tp")
    )
    in_specs = (
        P(SEQ, "tp"), P(SEQ, "tp"), P(SEQ, None), P(SEQ, None), P(SEQ, "tp"), P("tp"), P("tp"),
        P(), P(), P("tp"), P(),
    )
    return jax.shard_map(
        body, mesh=finer, in_specs=in_specs, out_specs=P(SEQ, "tp"), check_vma=False
    )
```

```python
import functools

import jax
import jax.numpy as jnp
from jax import lax
from jax.experimental import pallas as pl
from jax.experimental.pallas import tpu as pltpu
from jax.sharding import Mesh
from jax.sharding import PartitionSpec as P

SEQ = ("za", "zb", "y", "x")
GROUP = ("zb", "y", "x")
OUTER = "za"
LANES = 128
epsilon = 1e-05
HIGHEST = lax.Precision.HIGHEST
VMEM = pl.BlockSpec(memory_space=pltpu.VMEM)
HBM = pl.BlockSpec(memory_space=pltpu.HBM)


def call(
    kernel, outs, *args, hbm=0, after=(), scratch=(), flops=1_000_000, aliases=None, to_hbm=False
):
    if after:
        inner, skip = kernel, len(after)
        kernel = lambda *refs: inner(*refs[:len(args)], *refs[len(args) + skip:])
    multiple = isinstance(outs, (list, tuple))
    return pl.pallas_call(
        kernel,
        out_shape=list(outs) if multiple else outs,
        in_specs=[HBM] * hbm + [VMEM] * (len(args) - hbm) + [VMEM] * len(after),
        out_specs=[VMEM] * len(outs) if multiple else HBM if to_hbm else VMEM,
        input_output_aliases=aliases or {},
        scratch_shapes=list(scratch),
        compiler_params=pltpu.CompilerParams(vmem_limit_bytes=24 * 1024 * 1024),
        cost_estimate=pl.CostEstimate(flops=flops, bytes_accessed=1_000_000, transcendentals=0),
    )(*(pltpu.with_memory_space_constraint(a, pltpu.HBM) for a in args[:hbm]), *args[hbm:], *after)


def out(shape, dtype=jnp.float32):
    return pltpu.VMEM(shape, dtype)


def tile_of_heads(columns, tile, width, first=0):
    per, rows = LANES // width, columns.shape[0]
    lane = lax.broadcasted_iota(jnp.int32, (rows, LANES), 1)
    h = first + tile * per
    spread = jnp.broadcast_to(columns[:, h : h + 1], (rows, LANES))
    for k in range(1, per):
        other = jnp.broadcast_to(columns[:, h + k : h + k + 1], (rows, LANES))
        spread = jnp.where(lane < k * width, spread, other)
    return spread


def tails_kernel(b_ref, c_ref, *refs):
    count = (len(refs) - 2) // 2
    sources, tails_ref, targets, sems = refs[:count], refs[count], refs[count + 1 : -1], refs[-1]
    tokens, state = b_ref.shape
    copies = [
        pltpu.make_async_copy(
            r.at[pl.ds(tokens - 8, 8), :], tails_ref.at[:, pl.ds(k * state, state)], sems.at[k]
        )
        for k, r in enumerate((b_ref, c_ref))
    ]
    for k, (source, target) in enumerate(zip(sources, targets)):
        copies.append(pltpu.make_async_copy(source, target, sems.at[k + 2]))
    for copy in copies:
        copy.start()
    for copy in copies:
        copy.wait()


def convolve(padded_ref, weight, bias, relative, start):
    tokens = relative.shape[0]
    taps = weight.shape[0]
    summed = jnp.broadcast_to(bias, (tokens, bias.shape[1]))
    for k in range(taps):
        back = taps - 1 - k
        term = weight[k : k + 1, :] * padded_ref[8 - back : 8 - back + tokens, :]
        summed = summed + jnp.where(relative - back >= start, term, 0.0)
    return (summed * jax.nn.sigmoid(summed)).astype(jnp.bfloat16)


def sequence_index():
    index = 0
    for axis in SEQ:
        index = index * lax.axis_size(axis) + lax.axis_index(axis)
    return index


def to_column(row):
    n = row.shape[1]
    same = lax.broadcasted_iota(jnp.int32, (n, n), 0) == lax.broadcasted_iota(jnp.int32, (n, n), 1)
    return jnp.sum(jnp.where(same, jnp.broadcast_to(row, (n, n)), 0.0), axis=1, keepdims=True)


WEIGHTS_AT = 32


def prepare_kernel(*refs):
    count = 6
    sources, (docs_ref, raw_ref, bias_ref, rate_ref, _) = refs[:count], refs[count : count + 5]
    targets = refs[count + 5 : 2 * count + 5]
    (
        weighted_ref, cum_rows_ref, step_rows_ref, columns_ref, factor_ref, start_ref, b_conv_ref,
        c_conv_ref, stack_ref, padded_ref, sems,
    ) = refs[2 * count + 5 :]
    x_ref, b_ref, c_ref, taps_ref, taps_bias_ref, _ = targets
    copies = [
        pltpu.make_async_copy(source, target, sems.at[k])
        for k, (source, target) in enumerate(zip(sources, targets))
    ]
    for copy in copies:
        copy.start()
    heads, tokens = raw_ref.shape
    state = b_ref.shape[1]
    width = x_ref.shape[1] // heads
    base = sequence_index() * tokens
    relative = lax.broadcasted_iota(jnp.int32, (tokens, LANES), 0)
    start = jnp.zeros((1, 1), jnp.int32) - base
    last_position = jnp.full((1, 1), tokens - 1, jnp.int32)
    chosen = jnp.broadcast_to(start, relative.shape)
    end_start = start
    for i in range(1, docs_ref.shape[1]):
        start = start + docs_ref[0:1, i - 1 : i]
        chosen = jnp.where(start <= relative, start, chosen)
        end_start = jnp.where(start <= last_position, start, end_start)
    start_ref[...] = chosen

    step = jax.nn.softplus(raw_ref[...] + to_column(bias_ref[...]))
    log_decay = -step * to_column(rate_ref[...])
    rows = lax.broadcasted_iota(jnp.int32, (tokens, tokens), 0)
    cols = lax.broadcasted_iota(jnp.int32, (tokens, tokens), 1)
    cum = jnp.dot(
        log_decay, jnp.where(rows <= cols, 1.0, 0.0), precision=HIGHEST,
        preferred_element_type=jnp.float32,
    )
    cum_rows_ref[...] = cum
    step_rows_ref[...] = step
    position = lax.broadcasted_iota(jnp.int32, (heads, tokens), 1)
    weighting = jnp.where(
        position >= end_start, jnp.exp(cum[:, tokens - 1 : tokens] - cum) * step, 0.0
    )
    stack_ref[...] = jnp.zeros_like(stack_ref)
    stack_ref[0:heads, :] = cum
    stack_ref[WEIGHTS_AT : WEIGHTS_AT + heads, :] = weighting
    columns = stack_ref[...].T
    columns_ref[...] = columns
    factor_ref[...] = jnp.where(end_start < 0, jnp.exp(columns[tokens - 1 : tokens, :]), 0.0)
    for copy in copies:
        copy.wait()
    for j in range(x_ref.shape[1] // LANES):
        tile = slice(j * LANES, (j + 1) * LANES)
        weighted_ref[:, tile] = (
            x_ref[:, tile].astype(jnp.float32) * tile_of_heads(columns, j, width, WEIGHTS_AT)
        ).astype(jnp.bfloat16)
    padded_ref[0:8, :] = jnp.zeros((8, state), jnp.float32)
    for k, (source_ref, target_ref) in enumerate(((b_ref, b_conv_ref), (c_ref, c_conv_ref))):
        side = slice(k * state, (k + 1) * state)
        padded_ref[8:, :] = source_ref[...].astype(jnp.float32)
        result = convolve(padded_ref, taps_ref[:, side], taps_bias_ref[:, side], relative, chosen)
        target_ref[...] = result.astype(target_ref.dtype)


def first_rows(source_ref, halo, weight, bias, start_ref, padded_ref):
    padded_ref[0:8, :] = halo.astype(jnp.float32)
    padded_ref[8:, :] = source_ref[0:8, :].astype(jnp.float32)
    relative = lax.broadcasted_iota(jnp.int32, (8, LANES), 0)
    return convolve(padded_ref, weight, bias, relative, start_ref[0:8, :])


def states_kernel(
    b_ref, halo_ref, taps_ref, taps_bias_ref, start_ref, b_early_ref, weighted_ref, factor_ref,
    pieces_ref, b_conv_ref, padded_ref,
):
    state, features = b_ref.shape[1], weighted_ref.shape[1]
    members, rows, _ = pieces_ref.shape
    first = first_rows(
        b_ref, halo_ref[:, 0:state], taps_ref[:, 0:state], taps_bias_ref[:, 0:state], start_ref,
        padded_ref,
    )
    b_conv = jnp.concatenate([first.astype(jnp.float32), b_early_ref[8:, :]], axis=0)
    b_conv_ref[...] = b_conv.astype(jnp.bfloat16)
    b_rows = b_conv.T.astype(jnp.bfloat16)
    for j in range(features // 256):
        tile = slice(j * 256, (j + 1) * 256)
        end_state = jnp.dot(b_rows, weighted_ref[:, tile], preferred_element_type=jnp.float32)
        for m in range(members):
            pieces_ref[m, :, tile] = end_state[m * rows : (m + 1) * rows, :]
    spread = jnp.broadcast_to(factor_ref[...], (rows, LANES))
    for m in range(members):
        pieces_ref[m, :, features:] = spread


def prefix_kernel(
    heads, pieces_ref, before_ref, factors_ref, total_a_ref, total_b_ref, single_ref, wide_ref
):
    members, rows, padded = pieces_ref.shape
    features = padded - LANES
    width = features // heads
    for m in range(members):
        single_ref[m : m + 1, :] = pieces_ref[m, 0:1, features:]
    single = single_ref[...]
    for j in range(features // LANES):
        wide_ref[:, j * LANES : (j + 1) * LANES] = tile_of_heads(single, j, width)
    product = jnp.ones((1, LANES), jnp.float32)
    for m in range(members):
        factors_ref[m : m + 1, :] = product
        product = product * single_ref[m : m + 1, :]
    total = jnp.zeros((rows, features), jnp.float32)
    for m in range(members):
        before_ref[m] = total
        total = wide_ref[m : m + 1, :] * total + pieces_ref[m, :, 0:features]
    for total_ref in (total_a_ref, total_b_ref):
        total_ref[:, 0:features] = total
        total_ref[:, features:] = jnp.broadcast_to(product, (rows, LANES))


def wide_factor(pair_ref, features, width):
    factor = pair_ref[0:1, features:]
    return jnp.concatenate(
        [tile_of_heads(factor, j, width) for j in range(features // LANES)], axis=1
    )


def join_kernel(heads, own_ref, behind_ref, joined_ref):
    features = own_ref.shape[1] - LANES
    factor = wide_factor(own_ref, features, features // heads)
    joined_ref[:, 0:features] = factor * behind_ref[:, 0:features] + own_ref[:, 0:features]
    joined_ref[:, features:] = own_ref[:, features:]


def states_in_kernel(
    heads, first_ref, second_ref, far_ref, before_ref, factors_ref, state_ref, wide_ref
):
    members, rows, features = before_ref.shape
    width = features // heads
    factor = wide_factor(second_ref, features, width)
    near = first_ref[:, 0:features] + second_ref[:, 0:features]
    entering = factor * far_ref[:, 0:features] + near
    factors = factors_ref[...]
    for j in range(features // LANES):
        wide_ref[:, j * LANES : (j + 1) * LANES] = tile_of_heads(factors, j, width)
    for m in range(members):
        state_ref[m] = (wide_ref[m : m + 1, :] * entering + before_ref[m]).astype(jnp.bfloat16)


def products_of(
    c_ref, halo_ref, taps_ref, taps_bias_ref, start_ref, c_early_ref, b_conv_ref, c_conv_ref,
    products_ref, padded_ref,
):
    tokens, state = c_ref.shape
    first = first_rows(
        c_ref, halo_ref[:, state:], taps_ref[:, state:], taps_bias_ref[:, state:], start_ref,
        padded_ref,
    )
    c_conv = jnp.concatenate(
        [first.astype(jnp.float32), c_early_ref[8:, :]], axis=0
    ).astype(jnp.bfloat16)
    c_conv_ref[...] = c_conv
    products = lax.dot_general(
        c_conv, b_conv_ref[...], (((1,), (1,)), ((), ())), preferred_element_type=jnp.float32
    )
    row = lax.broadcasted_iota(jnp.int32, (tokens, tokens), 0)
    col = lax.broadcasted_iota(jnp.int32, (tokens, tokens), 1)
    starts = jnp.concatenate([start_ref[...]] * (tokens // LANES), axis=1)
    products_ref[...] = jnp.where((col <= row) & (col >= starts), products, 0.0)


def diagonal_of(
    start_ref, columns_ref, cum_rows_ref, step_rows_ref, x_ref, gate_ref, products_ref, gated_ref,
    scale_ref,
):
    tokens, features = x_ref.shape
    width, half = features // cum_rows_ref.shape[0], tokens // 2
    columns = columns_ref[...]
    carried = jnp.where(start_ref[...] < 0, jnp.exp(columns), 0.0)
    lane = lax.broadcasted_iota(jnp.int32, (tokens, LANES), 1)
    per = LANES // width
    for j in range(features // LANES):
        tile = slice(j * LANES, (j + 1) * LANES)
        diagonal = None
        for k in range(per):
            h = j * per + k
            column = jnp.broadcast_to(columns[:, h : h + 1], (tokens, LANES))
            cum_row, step_row = cum_rows_ref[h : h + 1, :], step_rows_ref[h : h + 1, :]
            upper = (
                products_ref[0:half, 0:half] * jnp.exp(column[0:half] - cum_row[:, 0:half])
            ) * step_row[:, 0:half]
            lower_left = (
                products_ref[half:, 0:half] * jnp.exp(column[half:] - cum_row[:, 0:half])
            ) * step_row[:, 0:half]
            lower_right = (
                products_ref[half:, half:] * jnp.exp(column[half:] - cum_row[:, half:])
            ) * step_row[:, half:]
            lower = jnp.concatenate([lower_left, lower_right], axis=1).astype(jnp.bfloat16)
            part = jnp.concatenate(
                [
                    jnp.dot(upper.astype(jnp.bfloat16), x_ref[0:half, tile],
                            preferred_element_type=jnp.float32),
                    jnp.dot(lower, x_ref[:, tile], preferred_element_type=jnp.float32),
                ],
                axis=0,
            )
            diagonal = part if diagonal is None else jnp.where(lane < k * width, diagonal, part)
        gate = gate_ref[:, tile].astype(jnp.float32)
        gate = gate * jax.nn.sigmoid(gate)
        gated_ref[:, tile] = diagonal * gate
        scale_ref[:, tile] = tile_of_heads(carried, j, width) * gate


def diagonal_kernel(turn, *refs):
    (*sources, columns_ref, cum_rows_ref, step_rows_ref, x_ref, gate_ref) = refs[:12]
    _, c_conv_ref, gated_ref, scale_ref, products_ref, padded_ref = refs[-6:]
    place = lax.axis_index(OUTER)
    early = (place == 0) & (lax.axis_index("tp") < lax.axis_size("tp") // 2)
    late = place >= 2

    @pl.when((early, jnp.logical_not(early | late), late)[turn])
    def _():
        products_of(*sources, c_conv_ref, products_ref, padded_ref)
        diagonal_of(
            sources[4], columns_ref, cum_rows_ref, step_rows_ref, x_ref, gate_ref, products_ref,
            gated_ref, scale_ref,
        )


def gate_kernel(
    state_ref, c_conv_ref, diagonal_ref, scale_ref, gated_ref, squares_ref, rows_ref
):
    members, rows, features = state_ref.shape
    for m in range(members):
        rows_ref[m * rows : (m + 1) * rows, :] = state_ref[m].astype(jnp.float32)
    c_conv = c_conv_ref[...]
    squares = jnp.zeros((c_conv.shape[0], LANES), jnp.float32)
    for j in range(features // LANES):
        tile = slice(j * LANES, (j + 1) * LANES)
        carried = jnp.dot(
            c_conv, rows_ref[:, tile].astype(jnp.bfloat16), preferred_element_type=jnp.float32
        )
        gated = diagonal_ref[:, tile] + scale_ref[:, tile] * carried
        gated_ref[:, tile] = gated
        squares = squares + gated * gated
    squares_ref[...] = lax.dot_general(
        jnp.ones((8, LANES), jnp.float32), squares, (((1,), (1,)), ((), ())),
        precision=HIGHEST, preferred_element_type=jnp.float32,
    )[0:1]


def normalize_kernel(features_all, squares_ref, gated_ref, gain_ref, out_ref, rows_ref, sems):
    count = squares_ref.shape[0]
    tokens, features = gated_ref.shape
    total = squares_ref[0]
    for k in range(1, count):
        total = total + squares_ref[k]
    first = lax.broadcasted_iota(jnp.int32, (8, total.shape[1]), 0) == 0
    column = lax.dot_general(
        jnp.where(first, jnp.broadcast_to(total, first.shape), 0.0),
        jnp.ones((8, LANES), jnp.float32), (((0,), (0,)), ((), ())),
        precision=HIGHEST, preferred_element_type=jnp.float32,
    )
    scale = lax.rsqrt(column / features_all + epsilon)
    chunks = sems.shape[0]
    size = tokens // chunks
    copies = []
    for i in range(chunks):
        part = slice(i * size, (i + 1) * size)
        for j in range(features // LANES):
            tile = slice(j * LANES, (j + 1) * LANES)
            rows_ref[part, tile] = (
                gated_ref[part, tile] * scale[part] * gain_ref[j : j + 1, :]
            ).astype(jnp.bfloat16)
        copies.append(
            pltpu.make_async_copy(
                rows_ref.at[pl.ds(i * size, size), :], out_ref.at[pl.ds(i * size, size), :],
                sems.at[i],
            )
        )
        copies[-1].start()
    for copy in copies:
        copy.wait()


def body(
    inputs, gate_input, b_source, c_source, step_raw, step_bias, decay_rate, conv_weight,
    conv_bias, norm_gain, doc_lengths,
):
    tokens, features = inputs.shape
    heads = step_raw.shape[1]
    state = b_source.shape[1]
    members = 1
    for axis in GROUP:
        members *= lax.axis_size(axis)
    outer = lax.axis_size(OUTER)
    rows = state // members
    shards = members * outer
    ahead = lambda n, k: [(i, i + k) for i in range(n - k)]

    bf16 = jnp.bfloat16
    small = [doc_lengths[None, :], step_raw.T, step_bias[None, :], decay_rate[None, :]]
    tails, *small = call(
        tails_kernel,
        [out((8, 2 * state), bf16)] + [out(o.shape, o.dtype) for o in small],
        b_source, c_source, *small,
        hbm=2 + len(small), scratch=[pltpu.SemaphoreType.DMA((2 + len(small),))],
    )
    halo = lax.ppermute(tails, SEQ, ahead(shards, 1))
    operands = [
        inputs, b_source, c_source, conv_weight, conv_bias[None, :],
        norm_gain.reshape(features // LANES, LANES),
    ]
    results = call(
        prepare_kernel,
        [out(o.shape, o.dtype) for o in operands]
        + [
            out((tokens, features), bf16), out((heads, tokens)), out((heads, tokens)),
            out((tokens, LANES)), out((1, LANES)), out((tokens, LANES), jnp.int32),
            out((tokens, state)), out((tokens, state)),
        ],
        *operands, *small, tails,
        hbm=len(operands),
        scratch=[
            pltpu.VMEM((LANES, tokens), jnp.float32),
            pltpu.VMEM((tokens + 8, state), jnp.float32),
            pltpu.SemaphoreType.DMA((len(operands),)),
        ],
    )
    x, b, c, taps, taps_bias, gain = results[0:6]
    weighted, cum_rows, step_rows, columns, factor, start, b_early, c_early = results[6:]
    pieces, b_conv = call(
        states_kernel,
        [out((members, rows, features + LANES)), out((tokens, state), bf16)],
        b, halo, taps, taps_bias, start, b_early, weighted, factor,
        scratch=[pltpu.VMEM((16, state), jnp.float32)],
    )
    pieces = lax.all_to_all(pieces, GROUP, 0, 0)
    pair = out((rows, features + LANES))
    before, factors, total_a, total_b = call(
        functools.partial(prefix_kernel, heads),
        [out((members, rows, features)), out((members, LANES)), pair, pair],
        pieces,
        scratch=[
            pltpu.VMEM((members, LANES), jnp.float32),
            pltpu.VMEM((members, features), jnp.float32),
        ],
    )

    def diagonal_terms(turn, token, *before, late=()):
        sources = [
            c, halo, taps, taps_bias, start, c_early, b_conv, columns, cum_rows, step_rows, x,
            gate_input,
        ]
        count = len(sources)
        return call(
            functools.partial(diagonal_kernel, turn),
            [
                out(token.shape), out((tokens, state), bf16), out((tokens, features)),
                out((tokens, features)),
            ],
            *sources, token, *before, after=late, flops=20_000_000_000,
            aliases={count + k: k for k in range(1 + len(before))},
            scratch=[
                pltpu.VMEM((tokens, tokens), jnp.float32),
                pltpu.VMEM((16, state), jnp.float32),
            ],
        )

    total_a, *diagonal = diagonal_terms(0, total_a)
    first = lax.ppermute(total_a, OUTER, [(0, 1)])
    total_b, *diagonal = diagonal_terms(1, total_b, *diagonal)
    joined = call(functools.partial(join_kernel, heads), pair, total_b, first)
    far = lax.ppermute(joined, OUTER, [(1, 3)])
    second = lax.ppermute(joined, OUTER, [(1, 2), (2, 3)])
    factors, *diagonal = diagonal_terms(2, factors, *diagonal, late=(joined,))
    c_conv, diagonal, scale = diagonal
    states_in = call(
        functools.partial(states_in_kernel, heads),
        out((members, rows, features), bf16),
        first, second, far, before, factors,
        scratch=[pltpu.VMEM((members, features), jnp.float32)],
    )
    states_in = lax.all_to_all(states_in, GROUP, 0, 0)
    gated, squares = call(
        gate_kernel,
        [out((tokens, features)), out((1, tokens))],
        states_in, c_conv, diagonal, scale,
        scratch=[pltpu.VMEM((state, features), jnp.float32)],
    )
    squares = lax.all_gather(squares, "tp")
    return call(
        functools.partial(normalize_kernel, features * lax.axis_size("tp")),
        jax.ShapeDtypeStruct((tokens, features), bf16),
        squares, gated, gain, to_hbm=True,
        scratch=[pltpu.VMEM((tokens, features), bf16), pltpu.SemaphoreType.DMA((4,))],
    )


def solution(mesh):
    finer = Mesh(
        mesh.devices.reshape(4, 2, 4, 4, mesh.shape["tp"]), ("za", "zb", "y", "x", "tp")
    )
    in_specs = (
        P(SEQ, "tp"), P(SEQ, "tp"), P(SEQ, None), P(SEQ, None), P(SEQ, "tp"), P("tp"), P("tp"),
        P(), P(), P("tp"), P(),
    )
    return jax.shard_map(
        body, mesh=finer, in_specs=in_specs, out_specs=P(SEQ, "tp"), check_vma=False
    )
```

```python
import functools

import jax
import jax.numpy as jnp
from jax import lax
from jax.experimental import pallas as pl
from jax.experimental.pallas import tpu as pltpu
from jax.sharding import Mesh
from jax.sharding import PartitionSpec as P

SEQ = ("za", "zb", "y", "x")
GROUP = ("zb", "y", "x")
OUTER = "za"
LANES = 128
epsilon = 1e-05
HIGHEST = lax.Precision.HIGHEST
VMEM = pl.BlockSpec(memory_space=pltpu.VMEM)
HBM = pl.BlockSpec(memory_space=pltpu.HBM)


def call(
    kernel, outs, *args, hbm=0, after=(), scratch=(), flops=1_000_000, aliases=None, to_hbm=False
):
    if after:
        inner, skip = kernel, len(after)
        kernel = lambda *refs: inner(*refs[:len(args)], *refs[len(args) + skip:])
    multiple = isinstance(outs, (list, tuple))
    return pl.pallas_call(
        kernel,
        out_shape=list(outs) if multiple else outs,
        in_specs=[HBM] * hbm + [VMEM] * (len(args) - hbm) + [VMEM] * len(after),
        out_specs=[VMEM] * len(outs) if multiple else HBM if to_hbm else VMEM,
        input_output_aliases=aliases or {},
        scratch_shapes=list(scratch),
        compiler_params=pltpu.CompilerParams(vmem_limit_bytes=24 * 1024 * 1024),
        cost_estimate=pl.CostEstimate(flops=flops, bytes_accessed=1_000_000, transcendentals=0),
    )(*(pltpu.with_memory_space_constraint(a, pltpu.HBM) for a in args[:hbm]), *args[hbm:], *after)


def out(shape, dtype=jnp.float32):
    return pltpu.VMEM(shape, dtype)


def tile_of_heads(columns, tile, width, first=0):
    per, rows = LANES // width, columns.shape[0]
    lane = lax.broadcasted_iota(jnp.int32, (rows, LANES), 1)
    h = first + tile * per
    spread = jnp.broadcast_to(columns[:, h : h + 1], (rows, LANES))
    for k in range(1, per):
        other = jnp.broadcast_to(columns[:, h + k : h + k + 1], (rows, LANES))
        spread = jnp.where(lane < k * width, spread, other)
    return spread


def tails_kernel(b_ref, c_ref, *refs):
    count = (len(refs) - 2) // 2
    sources, tails_ref, targets, sems = refs[:count], refs[count], refs[count + 1 : -1], refs[-1]
    tokens, state = b_ref.shape
    copies = [
        pltpu.make_async_copy(
            r.at[pl.ds(tokens - 8, 8), :], tails_ref.at[:, pl.ds(k * state, state)], sems.at[k]
        )
        for k, r in enumerate((b_ref, c_ref))
    ]
    for k, (source, target) in enumerate(zip(sources, targets)):
        copies.append(pltpu.make_async_copy(source, target, sems.at[k + 2]))
    for copy in copies:
        copy.start()
    for copy in copies:
        copy.wait()


def convolve(padded_ref, weight, bias, relative, start):
    tokens = relative.shape[0]
    taps = weight.shape[0]
    summed = jnp.broadcast_to(bias, (tokens, bias.shape[1]))
    for k in range(taps):
        back = taps - 1 - k
        term = weight[k : k + 1, :] * padded_ref[8 - back : 8 - back + tokens, :]
        summed = summed + jnp.where(relative - back >= start, term, 0.0)
    return (summed * jax.nn.sigmoid(summed)).astype(jnp.bfloat16)


def sequence_index():
    index = 0
    for axis in SEQ:
        index = index * lax.axis_size(axis) + lax.axis_index(axis)
    return index


def to_column(row):
    n = row.shape[1]
    same = lax.broadcasted_iota(jnp.int32, (n, n), 0) == lax.broadcasted_iota(jnp.int32, (n, n), 1)
    return jnp.sum(jnp.where(same, jnp.broadcast_to(row, (n, n)), 0.0), axis=1, keepdims=True)


WEIGHTS_AT = 32


def prepare_kernel(*refs):
    count = 6
    sources, (docs_ref, raw_ref, bias_ref, rate_ref, _) = refs[:count], refs[count : count + 5]
    targets = refs[count + 5 : 2 * count + 5]
    (
        weighted_ref, cum_rows_ref, step_rows_ref, columns_ref, factor_ref, start_ref, b_conv_ref,
        stack_ref, padded_ref, sems,
    ) = refs[2 * count + 5 :]
    x_ref, b_ref, _, taps_ref, taps_bias_ref, _ = targets
    copies = [
        pltpu.make_async_copy(source, target, sems.at[k])
        for k, (source, target) in enumerate(zip(sources, targets))
    ]
    for copy in copies:
        copy.start()
    heads, tokens = raw_ref.shape
    state = b_ref.shape[1]
    width = x_ref.shape[1] // heads
    base = sequence_index() * tokens
    relative = lax.broadcasted_iota(jnp.int32, (tokens, LANES), 0)
    start = jnp.zeros((1, 1), jnp.int32) - base
    last_position = jnp.full((1, 1), tokens - 1, jnp.int32)
    chosen = jnp.broadcast_to(start, relative.shape)
    end_start = start
    for i in range(1, docs_ref.shape[1]):
        start = start + docs_ref[0:1, i - 1 : i]
        chosen = jnp.where(start <= relative, start, chosen)
        end_start = jnp.where(start <= last_position, start, end_start)
    start_ref[...] = chosen

    step = jax.nn.softplus(raw_ref[...] + to_column(bias_ref[...]))
    log_decay = -step * to_column(rate_ref[...])
    rows = lax.broadcasted_iota(jnp.int32, (tokens, tokens), 0)
    cols = lax.broadcasted_iota(jnp.int32, (tokens, tokens), 1)
    cum = jnp.dot(
        log_decay, jnp.where(rows <= cols, 1.0, 0.0), precision=HIGHEST,
        preferred_element_type=jnp.float32,
    )
    cum_rows_ref[...] = cum
    step_rows_ref[...] = step
    position = lax.broadcasted_iota(jnp.int32, (heads, tokens), 1)
    weighting = jnp.where(
        position >= end_start, jnp.exp(cum[:, tokens - 1 : tokens] - cum) * step, 0.0
    )
    stack_ref[...] = jnp.zeros_like(stack_ref)
    stack_ref[0:heads, :] = cum
    stack_ref[WEIGHTS_AT : WEIGHTS_AT + heads, :] = weighting
    columns = stack_ref[...].T
    columns_ref[...] = columns
    factor_ref[...] = jnp.where(end_start < 0, jnp.exp(columns[tokens - 1 : tokens, :]), 0.0)
    for copy in copies:
        copy.wait()
    for j in range(x_ref.shape[1] // LANES):
        tile = slice(j * LANES, (j + 1) * LANES)
        weighted_ref[:, tile] = (
            x_ref[:, tile].astype(jnp.float32) * tile_of_heads(columns, j, width, WEIGHTS_AT)
        ).astype(jnp.bfloat16)
    side = slice(0, state)
    padded_ref[0:8, :] = jnp.zeros((8, state), jnp.float32)
    padded_ref[8:, :] = b_ref[...].astype(jnp.float32)
    b_conv = convolve(padded_ref, taps_ref[:, side], taps_bias_ref[:, side], relative, chosen)
    b_conv_ref[...] = b_conv.astype(jnp.float32)


def first_rows(source_ref, halo, weight, bias, start_ref, padded_ref):
    padded_ref[0:8, :] = halo.astype(jnp.float32)
    padded_ref[8:, :] = source_ref[0:8, :].astype(jnp.float32)
    relative = lax.broadcasted_iota(jnp.int32, (8, LANES), 0)
    return convolve(padded_ref, weight, bias, relative, start_ref[0:8, :])


def states_kernel(
    b_ref, halo_ref, taps_ref, taps_bias_ref, start_ref, b_early_ref, weighted_ref, factor_ref,
    pieces_ref, b_conv_ref, padded_ref,
):
    state, features = b_ref.shape[1], weighted_ref.shape[1]
    members, rows, _ = pieces_ref.shape
    first = first_rows(
        b_ref, halo_ref[:, 0:state], taps_ref[:, 0:state], taps_bias_ref[:, 0:state], start_ref,
        padded_ref,
    )
    b_conv = jnp.concatenate([first.astype(jnp.float32), b_early_ref[8:, :]], axis=0)
    b_conv_ref[...] = b_conv.astype(jnp.bfloat16)
    b_rows = b_conv.T.astype(jnp.bfloat16)
    for j in range(features // 256):
        tile = slice(j * 256, (j + 1) * 256)
        end_state = jnp.dot(b_rows, weighted_ref[:, tile], preferred_element_type=jnp.float32)
        for m in range(members):
            pieces_ref[m, :, tile] = end_state[m * rows : (m + 1) * rows, :]
    spread = jnp.broadcast_to(factor_ref[...], (rows, LANES))
    for m in range(members):
        pieces_ref[m, :, features:] = spread


def prefix_kernel(
    heads, pieces_ref, before_ref, factors_ref, total_a_ref, total_b_ref, single_ref, wide_ref
):
    members, rows, padded = pieces_ref.shape
    features = padded - LANES
    width = features // heads
    for m in range(members):
        single_ref[m : m + 1, :] = pieces_ref[m, 0:1, features:]
    single = single_ref[...]
    for j in range(features // LANES):
        wide_ref[:, j * LANES : (j + 1) * LANES] = tile_of_heads(single, j, width)
    product = jnp.ones((1, LANES), jnp.float32)
    for m in range(members):
        factors_ref[m : m + 1, :] = product
        product = product * single_ref[m : m + 1, :]
    total = jnp.zeros((rows, features), jnp.float32)
    for m in range(members):
        before_ref[m] = total
        total = wide_ref[m : m + 1, :] * total + pieces_ref[m, :, 0:features]
    for total_ref in (total_a_ref, total_b_ref):
        total_ref[:, 0:features] = total
        total_ref[:, features:] = jnp.broadcast_to(product, (rows, LANES))


def wide_factor(pair_ref, features, width):
    factor = pair_ref[0:1, features:]
    return jnp.concatenate(
        [tile_of_heads(factor, j, width) for j in range(features // LANES)], axis=1
    )


def join_kernel(heads, own_ref, behind_ref, joined_ref):
    features = own_ref.shape[1] - LANES
    factor = wide_factor(own_ref, features, features // heads)
    joined_ref[:, 0:features] = factor * behind_ref[:, 0:features] + own_ref[:, 0:features]
    joined_ref[:, features:] = own_ref[:, features:]


def states_in_kernel(
    heads, first_ref, second_ref, far_ref, before_ref, factors_ref, state_ref, wide_ref
):
    members, rows, features = before_ref.shape
    width = features // heads
    factor = wide_factor(second_ref, features, width)
    near = first_ref[:, 0:features] + second_ref[:, 0:features]
    entering = factor * far_ref[:, 0:features] + near
    factors = factors_ref[...]
    for j in range(features // LANES):
        wide_ref[:, j * LANES : (j + 1) * LANES] = tile_of_heads(factors, j, width)
    for m in range(members):
        state_ref[m] = (wide_ref[m : m + 1, :] * entering + before_ref[m]).astype(jnp.bfloat16)


def products_of(
    c_ref, halo_ref, taps_ref, taps_bias_ref, start_ref, b_conv_ref, c_conv_ref, products_ref,
    padded_ref,
):
    tokens, state = c_ref.shape
    padded_ref[0:8, :] = halo_ref[:, state:].astype(jnp.float32)
    padded_ref[8:, :] = c_ref[...].astype(jnp.float32)
    relative = lax.broadcasted_iota(jnp.int32, (tokens, LANES), 0)
    c_conv = convolve(
        padded_ref, taps_ref[:, state:], taps_bias_ref[:, state:], relative, start_ref[...]
    )
    c_conv_ref[...] = c_conv
    products = lax.dot_general(
        c_conv, b_conv_ref[...], (((1,), (1,)), ((), ())), preferred_element_type=jnp.float32
    )
    row = lax.broadcasted_iota(jnp.int32, (tokens, tokens), 0)
    col = lax.broadcasted_iota(jnp.int32, (tokens, tokens), 1)
    starts = jnp.concatenate([start_ref[...]] * (tokens // LANES), axis=1)
    products_ref[...] = jnp.where((col <= row) & (col >= starts), products, 0.0)


def diagonal_of(
    start_ref, columns_ref, cum_rows_ref, step_rows_ref, x_ref, gate_ref, products_ref, gated_ref,
    scale_ref,
):
    tokens, features = x_ref.shape
    width, half = features // cum_rows_ref.shape[0], tokens // 2
    columns = columns_ref[...]
    carried = jnp.where(start_ref[...] < 0, jnp.exp(columns), 0.0)
    lane = lax.broadcasted_iota(jnp.int32, (tokens, LANES), 1)
    per = LANES // width
    for j in range(features // LANES):
        tile = slice(j * LANES, (j + 1) * LANES)
        diagonal = None
        for k in range(per):
            h = j * per + k
            column = jnp.broadcast_to(columns[:, h : h + 1], (tokens, LANES))
            cum_row, step_row = cum_rows_ref[h : h + 1, :], step_rows_ref[h : h + 1, :]
            upper = (
                products_ref[0:half, 0:half] * jnp.exp(column[0:half] - cum_row[:, 0:half])
            ) * step_row[:, 0:half]
            lower_left = (
                products_ref[half:, 0:half] * jnp.exp(column[half:] - cum_row[:, 0:half])
            ) * step_row[:, 0:half]
            lower_right = (
                products_ref[half:, half:] * jnp.exp(column[half:] - cum_row[:, half:])
            ) * step_row[:, half:]
            lower = jnp.concatenate([lower_left, lower_right], axis=1).astype(jnp.bfloat16)
            part = jnp.concatenate(
                [
                    jnp.dot(upper.astype(jnp.bfloat16), x_ref[0:half, tile],
                            preferred_element_type=jnp.float32),
                    jnp.dot(lower, x_ref[:, tile], preferred_element_type=jnp.float32),
                ],
                axis=0,
            )
            diagonal = part if diagonal is None else jnp.where(lane < k * width, diagonal, part)
        gate = gate_ref[:, tile].astype(jnp.float32)
        gate = gate * jax.nn.sigmoid(gate)
        gated_ref[:, tile] = diagonal * gate
        scale_ref[:, tile] = tile_of_heads(carried, j, width) * gate


def diagonal_kernel(turn, *refs):
    (*sources, columns_ref, cum_rows_ref, step_rows_ref, x_ref, gate_ref) = refs[:11]
    _, c_conv_ref, gated_ref, scale_ref, products_ref, padded_ref = refs[-6:]
    place = lax.axis_index(OUTER)
    early = (place == 0) & (lax.axis_index("tp") < lax.axis_size("tp") // 2)
    late = place >= 2

    @pl.when((early, jnp.logical_not(early | late), late)[turn])
    def _():
        products_of(*sources, c_conv_ref, products_ref, padded_ref)
        diagonal_of(
            sources[4], columns_ref, cum_rows_ref, step_rows_ref, x_ref, gate_ref, products_ref,
            gated_ref, scale_ref,
        )


def gate_kernel(state_ref, c_conv_ref, diagonal_ref, scale_ref, gated_ref, squares_ref):
    members, rows, features = state_ref.shape
    c_conv = c_conv_ref[...]
    squares = jnp.zeros((c_conv.shape[0], LANES), jnp.float32)
    for j in range(features // LANES):
        tile = slice(j * LANES, (j + 1) * LANES)
        state = state_ref[:, :, tile].astype(jnp.float32).reshape(members * rows, LANES)
        carried = jnp.dot(c_conv, state.astype(jnp.bfloat16), preferred_element_type=jnp.float32)
        gated = diagonal_ref[:, tile] + scale_ref[:, tile] * carried
        gated_ref[:, tile] = gated
        squares = squares + gated * gated
    squares_ref[...] = lax.dot_general(
        jnp.ones((8, LANES), jnp.float32), squares, (((1,), (1,)), ((), ())),
        precision=HIGHEST, preferred_element_type=jnp.float32,
    )[0:1]


def normalize_kernel(features_all, squares_ref, gated_ref, gain_ref, out_ref, rows_ref, sems):
    count = squares_ref.shape[0]
    tokens, features = gated_ref.shape
    total = squares_ref[0]
    for k in range(1, count):
        total = total + squares_ref[k]
    first = lax.broadcasted_iota(jnp.int32, (8, total.shape[1]), 0) == 0
    column = lax.dot_general(
        jnp.where(first, jnp.broadcast_to(total, first.shape), 0.0),
        jnp.ones((8, LANES), jnp.float32), (((0,), (0,)), ((), ())),
        precision=HIGHEST, preferred_element_type=jnp.float32,
    )
    scale = lax.rsqrt(column / features_all + epsilon)
    chunks = sems.shape[0]
    size = tokens // chunks
    copies = []
    for i in range(chunks):
        part = slice(i * size, (i + 1) * size)
        for j in range(features // LANES):
            tile = slice(j * LANES, (j + 1) * LANES)
            rows_ref[part, tile] = (
                gated_ref[part, tile] * scale[part] * gain_ref[j : j + 1, :]
            ).astype(jnp.bfloat16)
        copies.append(
            pltpu.make_async_copy(
                rows_ref.at[pl.ds(i * size, size), :], out_ref.at[pl.ds(i * size, size), :],
                sems.at[i],
            )
        )
        copies[-1].start()
    for copy in copies:
        copy.wait()


def body(
    inputs, gate_input, b_source, c_source, step_raw, step_bias, decay_rate, conv_weight,
    conv_bias, norm_gain, doc_lengths,
):
    tokens, features = inputs.shape
    heads = step_raw.shape[1]
    state = b_source.shape[1]
    members = 1
    for axis in GROUP:
        members *= lax.axis_size(axis)
    outer = lax.axis_size(OUTER)
    rows = state // members
    shards = members * outer
    ahead = lambda n, k: [(i, i + k) for i in range(n - k)]

    bf16 = jnp.bfloat16
    small = [doc_lengths[None, :], step_raw.T, step_bias[None, :], decay_rate[None, :]]
    tails, *small = call(
        tails_kernel,
        [out((8, 2 * state), bf16)] + [out(o.shape, o.dtype) for o in small],
        b_source, c_source, *small,
        hbm=2 + len(small), scratch=[pltpu.SemaphoreType.DMA((2 + len(small),))],
    )
    halo = lax.ppermute(tails, SEQ, ahead(shards, 1))
    operands = [
        inputs, b_source, c_source, conv_weight, conv_bias[None, :],
        norm_gain.reshape(features // LANES, LANES),
    ]
    results = call(
        prepare_kernel,
        [out(o.shape, o.dtype) for o in operands]
        + [
            out((tokens, features), bf16), out((heads, tokens)), out((heads, tokens)),
            out((tokens, LANES)), out((1, LANES)), out((tokens, LANES), jnp.int32),
            out((tokens, state)),
        ],
        *operands, *small, tails,
        hbm=len(operands),
        scratch=[
            pltpu.VMEM((LANES, tokens), jnp.float32),
            pltpu.VMEM((tokens + 8, state), jnp.float32),
            pltpu.SemaphoreType.DMA((len(operands),)),
        ],
    )
    x, b, c, taps, taps_bias, gain = results[0:6]
    weighted, cum_rows, step_rows, columns, factor, start, b_early = results[6:]
    pieces, b_conv = call(
        states_kernel,
        [out((members, rows, features + LANES)), out((tokens, state), bf16)],
        b, halo, taps, taps_bias, start, b_early, weighted, factor,
        scratch=[pltpu.VMEM((16, state), jnp.float32)],
    )
    pieces = lax.all_to_all(pieces, GROUP, 0, 0)
    pair = out((rows, features + LANES))
    before, factors, total_a, total_b = call(
        functools.partial(prefix_kernel, heads),
        [out((members, rows, features)), out((members, LANES)), pair, pair],
        pieces,
        scratch=[
            pltpu.VMEM((members, LANES), jnp.float32),
            pltpu.VMEM((members, features), jnp.float32),
        ],
    )

    def diagonal_terms(turn, token, *before, late=()):
        sources = [
            c, halo, taps, taps_bias, start, b_conv, columns, cum_rows, step_rows, x,
            gate_input,
        ]
        count = len(sources)
        return call(
            functools.partial(diagonal_kernel, turn),
            [
                out(token.shape), out((tokens, state), bf16), out((tokens, features)),
                out((tokens, features)),
            ],
            *sources, token, *before, after=late, flops=20_000_000_000,
            aliases={count + k: k for k in range(1 + len(before))},
            scratch=[
                pltpu.VMEM((tokens, tokens), jnp.float32),
                pltpu.VMEM((tokens + 8, state), jnp.float32),
            ],
        )

    total_a, *diagonal = diagonal_terms(0, total_a)
    first = lax.ppermute(total_a, OUTER, [(0, 1)])
    total_b, *diagonal = diagonal_terms(1, total_b, *diagonal)
    joined = call(functools.partial(join_kernel, heads), pair, total_b, first)
    far = lax.ppermute(joined, OUTER, [(1, 3)])
    second = lax.ppermute(joined, OUTER, [(1, 2), (2, 3)])
    factors, *diagonal = diagonal_terms(2, factors, *diagonal, late=(joined,))
    c_conv, diagonal, scale = diagonal
    states_in = call(
        functools.partial(states_in_kernel, heads),
        out((members, rows, features), bf16),
        first, second, far, before, factors,
        scratch=[pltpu.VMEM((members, features), jnp.float32)],
    )
    states_in = lax.all_to_all(states_in, GROUP, 0, 0)
    gated, squares = call(
        gate_kernel,
        [out((tokens, features)), out((1, tokens))],
        states_in, c_conv, diagonal, scale,
    )
    squares = lax.all_gather(squares, "tp")
    return call(
        functools.partial(normalize_kernel, features * lax.axis_size("tp")),
        jax.ShapeDtypeStruct((tokens, features), bf16),
        squares, gated, gain, to_hbm=True,
        scratch=[pltpu.VMEM((tokens, features), bf16), pltpu.SemaphoreType.DMA((4,))],
    )


def solution(mesh):
    finer = Mesh(
        mesh.devices.reshape(4, 2, 4, 4, mesh.shape["tp"]), ("za", "zb", "y", "x", "tp")
    )
    in_specs = (
        P(SEQ, "tp"), P(SEQ, "tp"), P(SEQ, None), P(SEQ, None), P(SEQ, "tp"), P("tp"), P("tp"),
        P(), P(), P("tp"), P(),
    )
    return jax.shard_map(
        body, mesh=finer, in_specs=in_specs, out_specs=P(SEQ, "tp"), check_vma=False
    )
```

```python
import functools

import jax
import jax.numpy as jnp
from jax import lax
from jax.experimental import pallas as pl
from jax.experimental.pallas import tpu as pltpu
from jax.sharding import Mesh
from jax.sharding import PartitionSpec as P

SEQ = ("za", "zb", "y", "x")
GROUP = ("zb", "y", "x")
OUTER = "za"
LANES = 128
epsilon = 1e-05
HIGHEST = lax.Precision.HIGHEST
VMEM = pl.BlockSpec(memory_space=pltpu.VMEM)
HBM = pl.BlockSpec(memory_space=pltpu.HBM)


def call(
    kernel, outs, *args, hbm=0, after=(), scratch=(), flops=1_000_000, aliases=None, to_hbm=False
):
    if after:
        inner, skip = kernel, len(after)
        kernel = lambda *refs: inner(*refs[:len(args)], *refs[len(args) + skip:])
    multiple = isinstance(outs, (list, tuple))
    return pl.pallas_call(
        kernel,
        out_shape=list(outs) if multiple else outs,
        in_specs=[HBM] * hbm + [VMEM] * (len(args) - hbm) + [VMEM] * len(after),
        out_specs=[VMEM] * len(outs) if multiple else HBM if to_hbm else VMEM,
        input_output_aliases=aliases or {},
        scratch_shapes=list(scratch),
        compiler_params=pltpu.CompilerParams(vmem_limit_bytes=24 * 1024 * 1024),
        cost_estimate=pl.CostEstimate(flops=flops, bytes_accessed=1_000_000, transcendentals=0),
    )(*(pltpu.with_memory_space_constraint(a, pltpu.HBM) for a in args[:hbm]), *args[hbm:], *after)


def out(shape, dtype=jnp.float32):
    return pltpu.VMEM(shape, dtype)


def tile_of_heads(columns, tile, width):
    per, rows = LANES // width, columns.shape[0]
    lane = lax.broadcasted_iota(jnp.int32, (rows, LANES), 1)
    h = tile * per
    spread = jnp.broadcast_to(columns[:, h : h + 1], (rows, LANES))
    for k in range(1, per):
        other = jnp.broadcast_to(columns[:, h + k : h + k + 1], (rows, LANES))
        spread = jnp.where(lane < k * width, spread, other)
    return spread


def tails_kernel(b_ref, c_ref, *refs):
    count = (len(refs) - 2) // 2
    sources, tails_ref, targets, sems = refs[:count], refs[count], refs[count + 1 : -1], refs[-1]
    tokens, state = b_ref.shape
    copies = [
        pltpu.make_async_copy(
            r.at[pl.ds(tokens - 8, 8), :], tails_ref.at[:, pl.ds(k * state, state)], sems.at[k]
        )
        for k, r in enumerate((b_ref, c_ref))
    ]
    for k, (source, target) in enumerate(zip(sources, targets)):
        copies.append(pltpu.make_async_copy(source, target, sems.at[k + 2]))
    for copy in copies:
        copy.start()
    for copy in copies:
        copy.wait()


def convolve(padded_ref, weight, bias, relative, start):
    tokens = relative.shape[0]
    taps = weight.shape[0]
    summed = jnp.broadcast_to(bias, (tokens, bias.shape[1]))
    for k in range(taps):
        back = taps - 1 - k
        term = weight[k : k + 1, :] * padded_ref[8 - back : 8 - back + tokens, :]
        summed = summed + jnp.where(relative - back >= start, term, 0.0)
    return (summed * jax.nn.sigmoid(summed)).astype(jnp.bfloat16)


def bf16_parts(value):
    parts = []
    for _ in range(3):
        part = value.astype(jnp.bfloat16)
        parts.append(part)
        value = value - part.astype(jnp.float32)
    return parts


def spread_matrix(first, last, width, at):
    row = lax.broadcasted_iota(jnp.int32, (LANES, last - first), 0)
    head = (first + lax.broadcasted_iota(jnp.int32, (LANES, last - first), 1)) // width
    inside = (row >= at) if at else (row < 32)
    return jnp.where(inside & ((row & 31) == head), 1.0, 0.0).astype(jnp.bfloat16)


def spread_rows(values, features, heads, wide_ref):
    count = values.shape[0]
    parts = jnp.concatenate(bf16_parts(jnp.where(
        lax.broadcasted_iota(jnp.int32, values.shape, 1) < heads, values, 0.0
    )), axis=0)
    for j in range(0, features, 256):
        wide = jnp.dot(
            parts, spread_matrix(j, j + 256, features // heads, 0),
            preferred_element_type=jnp.float32,
        )
        wide_ref[:, j : j + 256] = (
            wide[2 * count :] + wide[count : 2 * count]
        ) + wide[0:count]


def sequence_index():
    index = 0
    for axis in SEQ:
        index = index * lax.axis_size(axis) + lax.axis_index(axis)
    return index


def to_column(row):
    n = row.shape[1]
    same = lax.broadcasted_iota(jnp.int32, (n, n), 0) == lax.broadcasted_iota(jnp.int32, (n, n), 1)
    return jnp.sum(jnp.where(same, jnp.broadcast_to(row, (n, n)), 0.0), axis=1, keepdims=True)


WEIGHTS_AT = 32


def prepare_kernel(*refs):
    count = 6
    sources, (docs_ref, raw_ref, bias_ref, rate_ref, _) = refs[:count], refs[count : count + 5]
    targets = refs[count + 5 : 2 * count + 5]
    (
        weighted_ref, cum_rows_ref, step_rows_ref, columns_ref, factor_ref, start_ref, b_conv_ref,
        stack_ref, padded_ref, sems,
    ) = refs[2 * count + 5 :]
    x_ref, b_ref, _, taps_ref, taps_bias_ref, _ = targets
    copies = [
        pltpu.make_async_copy(source, target, sems.at[k])
        for k, (source, target) in enumerate(zip(sources, targets))
    ]
    for copy in copies:
        copy.start()
    heads, tokens = raw_ref.shape
    state = b_ref.shape[1]
    width = x_ref.shape[1] // heads
    base = sequence_index() * tokens
    relative = lax.broadcasted_iota(jnp.int32, (tokens, LANES), 0)
    start = jnp.zeros((1, 1), jnp.int32) - base
    last_position = jnp.full((1, 1), tokens - 1, jnp.int32)
    chosen = jnp.broadcast_to(start, relative.shape)
    end_start = start
    for i in range(1, docs_ref.shape[1]):
        start = start + docs_ref[0:1, i - 1 : i]
        chosen = jnp.where(start <= relative, start, chosen)
        end_start = jnp.where(start <= last_position, start, end_start)
    start_ref[...] = chosen

    step = jax.nn.softplus(raw_ref[...] + to_column(bias_ref[...]))
    log_decay = -step * to_column(rate_ref[...])
    rows = lax.broadcasted_iota(jnp.int32, (tokens, tokens), 0)
    cols = lax.broadcasted_iota(jnp.int32, (tokens, tokens), 1)
    upper = jnp.where(rows <= cols, 1.0, 0.0).astype(jnp.bfloat16)
    cum = sum(
        jnp.dot(part, upper, preferred_element_type=jnp.float32)
        for part in reversed(bf16_parts(log_decay))
    )
    cum_rows_ref[...] = cum
    step_rows_ref[...] = step
    position = lax.broadcasted_iota(jnp.int32, (heads, tokens), 1)
    weighting = jnp.where(
        position >= end_start, jnp.exp(cum[:, tokens - 1 : tokens] - cum) * step, 0.0
    )
    stack_ref[...] = jnp.zeros_like(stack_ref)
    stack_ref[0:heads, :] = cum
    for k, part in enumerate(bf16_parts(weighting)):
        at = WEIGHTS_AT * (k + 1)
        stack_ref[at : at + heads, :] = part.astype(jnp.float32)
    columns = stack_ref[...].T
    columns_ref[...] = columns
    factor_ref[...] = jnp.where(end_start < 0, jnp.exp(columns[tokens - 1 : tokens, :]), 0.0)
    for copy in copies:
        copy.wait()
    weights = columns.astype(jnp.bfloat16)
    for j in range(0, x_ref.shape[1], 256):
        tile = slice(j, j + 256)
        spread = jnp.dot(
            weights, spread_matrix(j, j + 256, width, WEIGHTS_AT),
            preferred_element_type=jnp.float32,
        )
        weighted_ref[:, tile] = (x_ref[:, tile].astype(jnp.float32) * spread).astype(jnp.bfloat16)
    side = slice(0, state)
    padded_ref[0:8, :] = jnp.zeros((8, state), jnp.float32)
    padded_ref[8:, :] = b_ref[...].astype(jnp.float32)
    b_conv = convolve(padded_ref, taps_ref[:, side], taps_bias_ref[:, side], relative, chosen)
    b_conv_ref[...] = b_conv.astype(jnp.float32)


def first_rows(source_ref, halo, weight, bias, start_ref, padded_ref):
    padded_ref[0:8, :] = halo.astype(jnp.float32)
    padded_ref[8:, :] = source_ref[0:8, :].astype(jnp.float32)
    relative = lax.broadcasted_iota(jnp.int32, (8, LANES), 0)
    return convolve(padded_ref, weight, bias, relative, start_ref[0:8, :])


def states_kernel(
    b_ref, halo_ref, taps_ref, taps_bias_ref, start_ref, b_early_ref, weighted_ref, factor_ref,
    pieces_ref, b_conv_ref, padded_ref,
):
    state, features = b_ref.shape[1], weighted_ref.shape[1]
    members, rows, _ = pieces_ref.shape
    first = first_rows(
        b_ref, halo_ref[:, 0:state], taps_ref[:, 0:state], taps_bias_ref[:, 0:state], start_ref,
        padded_ref,
    )
    b_conv = jnp.concatenate([first.astype(jnp.float32), b_early_ref[8:, :]], axis=0)
    b_conv_ref[...] = b_conv.astype(jnp.bfloat16)
    b_rows = b_conv.T.astype(jnp.bfloat16)
    for j in range(features // 256):
        tile = slice(j * 256, (j + 1) * 256)
        end_state = jnp.dot(b_rows, weighted_ref[:, tile], preferred_element_type=jnp.float32)
        for m in range(members):
            pieces_ref[m, :, tile] = end_state[m * rows : (m + 1) * rows, :]
    spread = jnp.broadcast_to(factor_ref[...], (rows, LANES))
    for m in range(members):
        pieces_ref[m, :, features:] = spread


def prefix_kernel(
    heads, pieces_ref, before_ref, factors_ref, total_a_ref, total_b_ref, single_ref, wide_ref
):
    members, rows, padded = pieces_ref.shape
    features = padded - LANES
    for m in range(members):
        single_ref[m : m + 1, :] = pieces_ref[m, 0:1, features:]
    spread_rows(single_ref[...], features, heads, wide_ref)
    product = jnp.ones((1, LANES), jnp.float32)
    for m in range(members):
        factors_ref[m : m + 1, :] = product
        product = product * single_ref[m : m + 1, :]
    total = jnp.zeros((rows, features), jnp.float32)
    for m in range(members):
        before_ref[m] = total
        total = wide_ref[m : m + 1, :] * total + pieces_ref[m, :, 0:features]
    for total_ref in (total_a_ref, total_b_ref):
        total_ref[:, 0:features] = total
        total_ref[:, features:] = jnp.broadcast_to(product, (rows, LANES))


def wide_factor(pair_ref, features, width):
    factor = pair_ref[0:1, features:]
    return jnp.concatenate(
        [tile_of_heads(factor, j, width) for j in range(features // LANES)], axis=1
    )


def join_kernel(heads, own_ref, behind_ref, joined_ref):
    features = own_ref.shape[1] - LANES
    factor = wide_factor(own_ref, features, features // heads)
    joined_ref[:, 0:features] = factor * behind_ref[:, 0:features] + own_ref[:, 0:features]
    joined_ref[:, features:] = own_ref[:, features:]


def states_in_kernel(
    heads, first_ref, second_ref, far_ref, before_ref, wide_ref, state_ref
):
    members, rows, features = before_ref.shape
    width = features // heads
    factor = wide_factor(second_ref, features, width)
    near = first_ref[:, 0:features] + second_ref[:, 0:features]
    entering = factor * far_ref[:, 0:features] + near
    for m in range(members):
        state_ref[m] = (wide_ref[m : m + 1, :] * entering + before_ref[m]).astype(jnp.bfloat16)


def products_of(
    c_ref, halo_ref, taps_ref, taps_bias_ref, start_ref, b_conv_ref, c_conv_ref, products_ref,
    padded_ref,
):
    tokens, state = c_ref.shape
    padded_ref[0:8, :] = halo_ref[:, state:].astype(jnp.float32)
    padded_ref[8:, :] = c_ref[...].astype(jnp.float32)
    relative = lax.broadcasted_iota(jnp.int32, (tokens, LANES), 0)
    c_conv = convolve(
        padded_ref, taps_ref[:, state:], taps_bias_ref[:, state:], relative, start_ref[...]
    )
    c_conv_ref[...] = c_conv
    products = lax.dot_general(
        c_conv, b_conv_ref[...], (((1,), (1,)), ((), ())), preferred_element_type=jnp.float32
    )
    row = lax.broadcasted_iota(jnp.int32, (tokens, tokens), 0)
    col = lax.broadcasted_iota(jnp.int32, (tokens, tokens), 1)
    starts = jnp.concatenate([start_ref[...]] * (tokens // LANES), axis=1)
    products_ref[...] = jnp.where((col <= row) & (col >= starts), products, 0.0)


def diagonal_of(
    start_ref, columns_ref, cum_rows_ref, step_rows_ref, x_ref, gate_ref, products_ref, gated_ref,
    scale_ref,
):
    tokens, features = x_ref.shape
    width, half = features // cum_rows_ref.shape[0], tokens // 2
    columns = columns_ref[...]
    carried = jnp.where(start_ref[...] < 0, jnp.exp(columns), 0.0)
    lane = lax.broadcasted_iota(jnp.int32, (tokens, LANES), 1)
    per = LANES // width
    for j in range(features // LANES):
        tile = slice(j * LANES, (j + 1) * LANES)
        diagonal = None
        for k in range(per):
            h = j * per + k
            column = jnp.broadcast_to(columns[:, h : h + 1], (tokens, LANES))
            cum_row, step_row = cum_rows_ref[h : h + 1, :], step_rows_ref[h : h + 1, :]
            upper = (
                products_ref[0:half, 0:half] * jnp.exp(column[0:half] - cum_row[:, 0:half])
            ) * step_row[:, 0:half]
            lower_left = (
                products_ref[half:, 0:half] * jnp.exp(column[half:] - cum_row[:, 0:half])
            ) * step_row[:, 0:half]
            lower_right = (
                products_ref[half:, half:] * jnp.exp(column[half:] - cum_row[:, half:])
            ) * step_row[:, half:]
            lower = jnp.concatenate([lower_left, lower_right], axis=1).astype(jnp.bfloat16)
            part = jnp.concatenate(
                [
                    jnp.dot(upper.astype(jnp.bfloat16), x_ref[0:half, tile],
                            preferred_element_type=jnp.float32),
                    jnp.dot(lower, x_ref[:, tile], preferred_element_type=jnp.float32),
                ],
                axis=0,
            )
            diagonal = part if diagonal is None else jnp.where(lane < k * width, diagonal, part)
        gate = gate_ref[:, tile].astype(jnp.float32)
        gate = gate * jax.nn.sigmoid(gate)
        gated_ref[:, tile] = diagonal * gate
        scale_ref[:, tile] = tile_of_heads(carried, j, width) * gate


def diagonal_kernel(turn, *refs):
    (*sources, columns_ref, cum_rows_ref, step_rows_ref, x_ref, gate_ref, factors_ref) = refs[:12]
    wide_ref, c_conv_ref, gated_ref, scale_ref, products_ref, padded_ref = refs[-6:]
    place = lax.axis_index(OUTER)
    early = (place == 0) & (lax.axis_index("tp") < lax.axis_size("tp") // 2)
    late = place >= 2

    @pl.when((early, jnp.logical_not(early | late), late)[turn])
    def _():
        spread_rows(factors_ref[...], x_ref.shape[1], cum_rows_ref.shape[0], wide_ref)
        products_of(*sources, c_conv_ref, products_ref, padded_ref)
        diagonal_of(
            sources[4], columns_ref, cum_rows_ref, step_rows_ref, x_ref, gate_ref, products_ref,
            gated_ref, scale_ref,
        )


def gate_kernel(state_ref, c_conv_ref, diagonal_ref, scale_ref, gated_ref, squares_ref):
    members, rows, features = state_ref.shape
    c_conv = c_conv_ref[...]
    squares = jnp.zeros((c_conv.shape[0], LANES), jnp.float32)
    for j in range(features // LANES):
        tile = slice(j * LANES, (j + 1) * LANES)
        state = state_ref[:, :, tile].astype(jnp.float32).reshape(members * rows, LANES)
        carried = jnp.dot(c_conv, state.astype(jnp.bfloat16), preferred_element_type=jnp.float32)
        gated = diagonal_ref[:, tile] + scale_ref[:, tile] * carried
        gated_ref[:, tile] = gated
        squares = squares + gated * gated
    ones = jnp.ones((8, LANES), jnp.bfloat16)
    squares_ref[...] = sum(
        lax.dot_general(ones, part, (((1,), (1,)), ((), ())), preferred_element_type=jnp.float32)
        for part in reversed(bf16_parts(squares))
    )[0:1]


def normalize_kernel(features_all, squares_ref, gated_ref, gain_ref, out_ref, rows_ref, sems):
    count = squares_ref.shape[0]
    tokens, features = gated_ref.shape
    total = squares_ref[0]
    for k in range(1, count):
        total = total + squares_ref[k]
    scale = lax.rsqrt(total / features_all + epsilon)
    scale = jnp.broadcast_to(scale, (LANES, tokens)).T
    chunks = sems.shape[0]
    size = tokens // chunks
    copies = []
    for i in range(chunks):
        part = slice(i * size, (i + 1) * size)
        for j in range(features // LANES):
            tile = slice(j * LANES, (j + 1) * LANES)
            rows_ref[part, tile] = (
                gated_ref[part, tile] * scale[part] * gain_ref[j : j + 1, :]
            ).astype(jnp.bfloat16)
        copies.append(
            pltpu.make_async_copy(
                rows_ref.at[pl.ds(i * size, size), :], out_ref.at[pl.ds(i * size, size), :],
                sems.at[i],
            )
        )
        copies[-1].start()
    for copy in copies:
        copy.wait()


def body(
    inputs, gate_input, b_source, c_source, step_raw, step_bias, decay_rate, conv_weight,
    conv_bias, norm_gain, doc_lengths,
):
    tokens, features = inputs.shape
    heads = step_raw.shape[1]
    state = b_source.shape[1]
    members = 1
    for axis in GROUP:
        members *= lax.axis_size(axis)
    outer = lax.axis_size(OUTER)
    rows = state // members
    shards = members * outer
    ahead = lambda n, k: [(i, i + k) for i in range(n - k)]

    bf16 = jnp.bfloat16
    small = [doc_lengths[None, :], step_raw.T, step_bias[None, :], decay_rate[None, :]]
    tails, *small = call(
        tails_kernel,
        [out((8, 2 * state), bf16)] + [out(o.shape, o.dtype) for o in small],
        b_source, c_source, *small,
        hbm=2 + len(small), scratch=[pltpu.SemaphoreType.DMA((2 + len(small),))],
    )
    halo = lax.ppermute(tails, SEQ, ahead(shards, 1))
    operands = [
        inputs, b_source, c_source, conv_weight, conv_bias[None, :],
        norm_gain.reshape(features // LANES, LANES),
    ]
    results = call(
        prepare_kernel,
        [out(o.shape, o.dtype) for o in operands]
        + [
            out((tokens, features), bf16), out((heads, tokens)), out((heads, tokens)),
            out((tokens, LANES)), out((1, LANES)), out((tokens, LANES), jnp.int32),
            out((tokens, state)),
        ],
        *operands, *small, tails,
        hbm=len(operands),
        scratch=[
            pltpu.VMEM((LANES, tokens), jnp.float32),
            pltpu.VMEM((tokens + 8, state), jnp.float32),
            pltpu.SemaphoreType.DMA((len(operands),)),
        ],
    )
    x, b, c, taps, taps_bias, gain = results[0:6]
    weighted, cum_rows, step_rows, columns, factor, start, b_early = results[6:]
    pieces, b_conv = call(
        states_kernel,
        [out((members, rows, features + LANES)), out((tokens, state), bf16)],
        b, halo, taps, taps_bias, start, b_early, weighted, factor,
        scratch=[pltpu.VMEM((16, state), jnp.float32)],
    )
    pieces = lax.all_to_all(pieces, GROUP, 0, 0)
    pair = out((rows, features + LANES))
    before, factors, total_a, total_b = call(
        functools.partial(prefix_kernel, heads),
        [out((members, rows, features)), out((members, LANES)), pair, pair],
        pieces,
        scratch=[
            pltpu.VMEM((members, LANES), jnp.float32),
            pltpu.VMEM((members, features), jnp.float32),
        ],
    )

    def diagonal_terms(turn, token, *before, late=()):
        sources = [
            c, halo, taps, taps_bias, start, b_conv, columns, cum_rows, step_rows, x, gate_input,
            factors,
        ]
        token = [] if token is None else [token]
        count = len(sources)
        results = call(
            functools.partial(diagonal_kernel, turn),
            [out(t.shape) for t in token] + [
                out((members, features)), out((tokens, state), bf16), out((tokens, features)),
                out((tokens, features)),
            ],
            *sources, *token, *before, after=late, flops=20_000_000_000,
            aliases={count + k: k for k in range(len(token) + len(before))},
            scratch=[
                pltpu.VMEM((tokens, tokens), jnp.float32),
                pltpu.VMEM((tokens + 8, state), jnp.float32),
            ],
        )
        return results

    total_a, *diagonal = diagonal_terms(0, total_a)
    first = lax.ppermute(total_a, OUTER, [(0, 1)])
    total_b, *diagonal = diagonal_terms(1, total_b, *diagonal)
    joined = call(functools.partial(join_kernel, heads), pair, total_b, first)
    far = lax.ppermute(joined, OUTER, [(1, 3)])
    second = lax.ppermute(joined, OUTER, [(1, 2), (2, 3)])
    wide, c_conv, diagonal, scale = diagonal_terms(2, None, *diagonal, late=(joined,))
    states_in = call(
        functools.partial(states_in_kernel, heads),
        out((members, rows, features), bf16),
        first, second, far, before, wide,
    )
    states_in = lax.all_to_all(states_in, GROUP, 0, 0)
    gated, squares = call(
        gate_kernel,
        [out((tokens, features)), out((1, tokens))],
        states_in, c_conv, diagonal, scale,
    )
    squares = lax.all_gather(squares, "tp")
    return call(
        functools.partial(normalize_kernel, features * lax.axis_size("tp")),
        jax.ShapeDtypeStruct((tokens, features), bf16),
        squares, gated, gain, to_hbm=True,
        scratch=[pltpu.VMEM((tokens, features), bf16), pltpu.SemaphoreType.DMA((4,))],
    )


def solution(mesh):
    finer = Mesh(
        mesh.devices.reshape(4, 2, 4, 4, mesh.shape["tp"]), ("za", "zb", "y", "x", "tp")
    )
    in_specs = (
        P(SEQ, "tp"), P(SEQ, "tp"), P(SEQ, None), P(SEQ, None), P(SEQ, "tp"), P("tp"), P("tp"),
        P(), P(), P("tp"), P(),
    )
    return jax.shard_map(
        body, mesh=finer, in_specs=in_specs, out_specs=P(SEQ, "tp"), check_vma=False
    )
```

```python
import functools

import jax
import jax.numpy as jnp
from jax import lax
from jax.experimental import pallas as pl
from jax.experimental.pallas import tpu as pltpu
from jax.sharding import Mesh
from jax.sharding import PartitionSpec as P

SEQ = ("za", "zb", "y", "x")
GROUP = ("zb", "y", "x")
OUTER = "za"
LANES = 128
epsilon = 1e-05
VMEM = pl.BlockSpec(memory_space=pltpu.VMEM)
HBM = pl.BlockSpec(memory_space=pltpu.HBM)


def call(
    kernel, outs, *args, hbm=0, after=(), scratch=(), flops=1_000_000, aliases=None, to_hbm=False
):
    if after:
        inner, skip = kernel, len(after)
        kernel = lambda *refs: inner(*refs[:len(args)], *refs[len(args) + skip:])
    multiple = isinstance(outs, (list, tuple))
    return pl.pallas_call(
        kernel,
        out_shape=list(outs) if multiple else outs,
        in_specs=[HBM] * hbm + [VMEM] * (len(args) - hbm) + [VMEM] * len(after),
        out_specs=[VMEM] * len(outs) if multiple else HBM if to_hbm else VMEM,
        input_output_aliases=aliases or {},
        scratch_shapes=list(scratch),
        compiler_params=pltpu.CompilerParams(vmem_limit_bytes=24 * 1024 * 1024),
        cost_estimate=pl.CostEstimate(flops=flops, bytes_accessed=1_000_000, transcendentals=0),
    )(*(pltpu.with_memory_space_constraint(a, pltpu.HBM) for a in args[:hbm]), *args[hbm:], *after)


def out(shape, dtype=jnp.float32):
    return pltpu.VMEM(shape, dtype)


def tile_of_heads(columns, tile, width):
    per, rows = LANES // width, columns.shape[0]
    lane = lax.broadcasted_iota(jnp.int32, (rows, LANES), 1)
    h = tile * per
    spread = jnp.broadcast_to(columns[:, h : h + 1], (rows, LANES))
    for k in range(1, per):
        other = jnp.broadcast_to(columns[:, h + k : h + k + 1], (rows, LANES))
        spread = jnp.where(lane < k * width, spread, other)
    return spread


def tails_kernel(b_ref, c_ref, *refs):
    count = (len(refs) - 2) // 2
    sources, tails_ref, targets, sems = refs[:count], refs[count], refs[count + 1 : -1], refs[-1]
    tokens, state = b_ref.shape
    copies = [
        pltpu.make_async_copy(
            r.at[pl.ds(tokens - 8, 8), :], tails_ref.at[:, pl.ds(k * state, state)], sems.at[k]
        )
        for k, r in enumerate((b_ref, c_ref))
    ]
    for k, (source, target) in enumerate(zip(sources, targets)):
        copies.append(pltpu.make_async_copy(source, target, sems.at[k + 2]))
    for copy in copies:
        copy.start()
    for copy in copies:
        copy.wait()


def convolve(padded_ref, weight, bias, relative, start):
    tokens = relative.shape[0]
    taps = weight.shape[0]
    summed = jnp.broadcast_to(bias, (tokens, bias.shape[1]))
    for k in range(taps):
        back = taps - 1 - k
        term = weight[k : k + 1, :] * padded_ref[8 - back : 8 - back + tokens, :]
        summed = summed + jnp.where(relative - back >= start, term, 0.0)
    return (summed * jax.nn.sigmoid(summed)).astype(jnp.bfloat16)


def bf16_parts(value):
    parts = []
    for _ in range(3):
        part = value.astype(jnp.bfloat16)
        parts.append(part)
        value = value - part.astype(jnp.float32)
    return parts


def spread_matrix(first, last, width, at):
    row = lax.broadcasted_iota(jnp.int32, (LANES, last - first), 0)
    head = (first + lax.broadcasted_iota(jnp.int32, (LANES, last - first), 1)) // width
    inside = (row >= at) if at else (row < 32)
    return jnp.where(inside & ((row & 31) == head), 1.0, 0.0).astype(jnp.bfloat16)


def spread_rows(values, features, heads, wide_ref):
    count = values.shape[0]
    parts = jnp.concatenate(bf16_parts(jnp.where(
        lax.broadcasted_iota(jnp.int32, values.shape, 1) < heads, values, 0.0
    )), axis=0)
    for j in range(0, features, 256):
        wide = jnp.dot(
            parts, spread_matrix(j, j + 256, features // heads, 0),
            preferred_element_type=jnp.float32,
        )
        wide_ref[:, j : j + 256] = (
            wide[2 * count :] + wide[count : 2 * count]
        ) + wide[0:count]


def sequence_index():
    index = 0
    for axis in SEQ:
        index = index * lax.axis_size(axis) + lax.axis_index(axis)
    return index


def to_column(row):
    n = row.shape[1]
    same = lax.broadcasted_iota(jnp.int32, (n, n), 0) == lax.broadcasted_iota(jnp.int32, (n, n), 1)
    return jnp.sum(jnp.where(same, jnp.broadcast_to(row, (n, n)), 0.0), axis=1, keepdims=True)


WEIGHTS_AT = 32


def prepare_kernel(*refs):
    count = 6
    sources, (docs_ref, raw_ref, bias_ref, rate_ref, _) = refs[:count], refs[count : count + 5]
    targets = refs[count + 5 : 2 * count + 5]
    (
        weighted_ref, cum_rows_ref, step_rows_ref, columns_ref, factor_ref, start_ref, b_conv_ref,
        stack_ref, padded_ref, sems,
    ) = refs[2 * count + 5 :]
    x_ref, b_ref, _, taps_ref, taps_bias_ref, _ = targets
    copies = [
        pltpu.make_async_copy(source, target, sems.at[k])
        for k, (source, target) in enumerate(zip(sources, targets))
    ]
    for copy in copies:
        copy.start()
    heads, tokens = raw_ref.shape
    state = b_ref.shape[1]
    width = x_ref.shape[1] // heads
    base = sequence_index() * tokens
    relative = lax.broadcasted_iota(jnp.int32, (tokens, LANES), 0)
    start = jnp.zeros((1, 1), jnp.int32) - base
    last_position = jnp.full((1, 1), tokens - 1, jnp.int32)
    chosen = jnp.broadcast_to(start, relative.shape)
    end_start = start
    for i in range(1, docs_ref.shape[1]):
        start = start + docs_ref[0:1, i - 1 : i]
        chosen = jnp.where(start <= relative, start, chosen)
        end_start = jnp.where(start <= last_position, start, end_start)
    start_ref[...] = chosen

    step = jax.nn.softplus(raw_ref[...] + to_column(bias_ref[...]))
    log_decay = -step * to_column(rate_ref[...])
    rows = lax.broadcasted_iota(jnp.int32, (tokens, tokens), 0)
    cols = lax.broadcasted_iota(jnp.int32, (tokens, tokens), 1)
    upper = jnp.where(rows <= cols, 1.0, 0.0).astype(jnp.bfloat16)
    cum = sum(
        jnp.dot(part, upper, preferred_element_type=jnp.float32)
        for part in reversed(bf16_parts(log_decay))
    )
    cum_rows_ref[...] = cum
    step_rows_ref[...] = step
    position = lax.broadcasted_iota(jnp.int32, (heads, tokens), 1)
    weighting = jnp.where(
        position >= end_start, jnp.exp(cum[:, tokens - 1 : tokens] - cum) * step, 0.0
    )
    stack_ref[...] = jnp.zeros_like(stack_ref)
    stack_ref[0:heads, :] = cum
    for k, part in enumerate(bf16_parts(weighting)):
        at = WEIGHTS_AT * (k + 1)
        stack_ref[at : at + heads, :] = part.astype(jnp.float32)
    columns = stack_ref[...].T
    columns_ref[...] = columns
    factor_ref[...] = jnp.where(end_start < 0, jnp.exp(columns[tokens - 1 : tokens, :]), 0.0)
    for copy in copies:
        copy.wait()
    weights = columns.astype(jnp.bfloat16)
    for j in range(0, x_ref.shape[1], 256):
        tile = slice(j, j + 256)
        spread = jnp.dot(
            weights, spread_matrix(j, j + 256, width, WEIGHTS_AT),
            preferred_element_type=jnp.float32,
        )
        weighted_ref[:, tile] = (x_ref[:, tile].astype(jnp.float32) * spread).astype(jnp.bfloat16)
    side = slice(0, state)
    padded_ref[0:8, :] = jnp.zeros((8, state), jnp.float32)
    padded_ref[8:, :] = b_ref[...].astype(jnp.float32)
    b_conv = convolve(padded_ref, taps_ref[:, side], taps_bias_ref[:, side], relative, chosen)
    b_conv_ref[...] = b_conv.astype(jnp.float32)


def first_rows(source_ref, halo, weight, bias, start_ref, padded_ref):
    padded_ref[0:8, :] = halo.astype(jnp.float32)
    padded_ref[8:, :] = source_ref[0:8, :].astype(jnp.float32)
    relative = lax.broadcasted_iota(jnp.int32, (8, LANES), 0)
    return convolve(padded_ref, weight, bias, relative, start_ref[0:8, :])


def states_kernel(
    b_ref, halo_ref, taps_ref, taps_bias_ref, start_ref, b_early_ref, weighted_ref, factor_ref,
    pieces_ref, b_conv_ref, padded_ref,
):
    state, features = b_ref.shape[1], weighted_ref.shape[1]
    members, rows, _ = pieces_ref.shape
    first = first_rows(
        b_ref, halo_ref[:, 0:state], taps_ref[:, 0:state], taps_bias_ref[:, 0:state], start_ref,
        padded_ref,
    )
    b_conv = jnp.concatenate([first.astype(jnp.float32), b_early_ref[8:, :]], axis=0)
    b_conv_ref[...] = b_conv.astype(jnp.bfloat16)
    b_rows = b_conv.T.astype(jnp.bfloat16)
    for j in range(features // 256):
        tile = slice(j * 256, (j + 1) * 256)
        end_state = jnp.dot(b_rows, weighted_ref[:, tile], preferred_element_type=jnp.float32)
        for m in range(members):
            pieces_ref[m, :, tile] = end_state[m * rows : (m + 1) * rows, :]
    spread = jnp.broadcast_to(factor_ref[...], (rows, LANES))
    for m in range(members):
        pieces_ref[m, :, features:] = spread


def prefix_kernel(
    heads, pieces_ref, before_ref, factors_ref, total_a_ref, total_b_ref, total_c_ref, single_ref,
    wide_ref,
):
    members, rows, padded = pieces_ref.shape
    features = padded - LANES
    for m in range(members):
        single_ref[m : m + 1, :] = pieces_ref[m, 0:1, features:]
    spread_rows(single_ref[...], features, heads, wide_ref)
    product = jnp.ones((1, LANES), jnp.float32)
    for m in range(members):
        factors_ref[m : m + 1, :] = product
        product = product * single_ref[m : m + 1, :]
    total = jnp.zeros((rows, features), jnp.float32)
    for m in range(members):
        before_ref[m] = total
        total = wide_ref[m : m + 1, :] * total + pieces_ref[m, :, 0:features]
    for total_ref in (total_a_ref, total_b_ref, total_c_ref):
        total_ref[:, 0:features] = total
        total_ref[:, features:] = jnp.broadcast_to(product, (rows, LANES))


def wide_factor(pair_ref, features, width):
    factor = pair_ref[0:1, features:]
    return jnp.concatenate(
        [tile_of_heads(factor, j, width) for j in range(features // LANES)], axis=1
    )


def states_in_kernel(heads, *refs):
    *near_refs, far_ref, before_ref, wide_ref, state_ref, near_ref = refs
    members, _, features = before_ref.shape
    near_ref[...] = sum(ref[...] for ref in near_refs)
    factor = wide_factor(near_ref, features, features // heads)
    entering = factor * far_ref[:, 0:features] + near_ref[:, 0:features]
    for m in range(members):
        state_ref[m] = (wide_ref[m : m + 1, :] * entering + before_ref[m]).astype(jnp.bfloat16)


def products_of(
    c_ref, halo_ref, taps_ref, taps_bias_ref, start_ref, b_conv_ref, c_conv_ref, products_ref,
    padded_ref,
):
    tokens, state = c_ref.shape
    padded_ref[0:8, :] = halo_ref[:, state:].astype(jnp.float32)
    padded_ref[8:, :] = c_ref[...].astype(jnp.float32)
    relative = lax.broadcasted_iota(jnp.int32, (tokens, LANES), 0)
    c_conv = convolve(
        padded_ref, taps_ref[:, state:], taps_bias_ref[:, state:], relative, start_ref[...]
    )
    c_conv_ref[...] = c_conv
    products = lax.dot_general(
        c_conv, b_conv_ref[...], (((1,), (1,)), ((), ())), preferred_element_type=jnp.float32
    )
    row = lax.broadcasted_iota(jnp.int32, (tokens, tokens), 0)
    col = lax.broadcasted_iota(jnp.int32, (tokens, tokens), 1)
    starts = jnp.concatenate([start_ref[...]] * (tokens // LANES), axis=1)
    products_ref[...] = jnp.where((col <= row) & (col >= starts), products, 0.0)


def diagonal_of(
    start_ref, columns_ref, cum_rows_ref, step_rows_ref, x_ref, gate_ref, products_ref, gated_ref,
    scale_ref,
):
    tokens, features = x_ref.shape
    width, half = features // cum_rows_ref.shape[0], tokens // 2
    columns = columns_ref[...]
    carried = jnp.where(start_ref[...] < 0, jnp.exp(columns), 0.0)
    lane = lax.broadcasted_iota(jnp.int32, (tokens, LANES), 1)
    per = LANES // width
    for j in range(features // LANES):
        tile = slice(j * LANES, (j + 1) * LANES)
        diagonal = None
        for k in range(per):
            h = j * per + k
            column = jnp.broadcast_to(columns[:, h : h + 1], (tokens, LANES))
            cum_row, step_row = cum_rows_ref[h : h + 1, :], step_rows_ref[h : h + 1, :]
            upper = (
                products_ref[0:half, 0:half] * jnp.exp(column[0:half] - cum_row[:, 0:half])
            ) * step_row[:, 0:half]
            lower_left = (
                products_ref[half:, 0:half] * jnp.exp(column[half:] - cum_row[:, 0:half])
            ) * step_row[:, 0:half]
            lower_right = (
                products_ref[half:, half:] * jnp.exp(column[half:] - cum_row[:, half:])
            ) * step_row[:, half:]
            lower = jnp.concatenate([lower_left, lower_right], axis=1).astype(jnp.bfloat16)
            part = jnp.concatenate(
                [
                    jnp.dot(upper.astype(jnp.bfloat16), x_ref[0:half, tile],
                            preferred_element_type=jnp.float32),
                    jnp.dot(lower, x_ref[:, tile], preferred_element_type=jnp.float32),
                ],
                axis=0,
            )
            diagonal = part if diagonal is None else jnp.where(lane < k * width, diagonal, part)
        gate = gate_ref[:, tile].astype(jnp.float32)
        gate = gate * jax.nn.sigmoid(gate)
        gated_ref[:, tile] = diagonal * gate
        scale_ref[:, tile] = tile_of_heads(carried, j, width) * gate


def diagonal_kernel(turn, *refs):
    (*sources, columns_ref, cum_rows_ref, step_rows_ref, x_ref, gate_ref, factors_ref) = refs[:12]
    wide_ref, c_conv_ref, gated_ref, scale_ref, products_ref, padded_ref = refs[-6:]
    place = lax.axis_index(OUTER)
    early = (place == 0) & (lax.axis_index("tp") < lax.axis_size("tp") // 2)
    late = place >= 2

    @pl.when((early, jnp.logical_not(early | late), late)[turn])
    def _():
        spread_rows(factors_ref[...], x_ref.shape[1], cum_rows_ref.shape[0], wide_ref)
        products_of(*sources, c_conv_ref, products_ref, padded_ref)
        diagonal_of(
            sources[4], columns_ref, cum_rows_ref, step_rows_ref, x_ref, gate_ref, products_ref,
            gated_ref, scale_ref,
        )


def gate_kernel(state_ref, c_conv_ref, diagonal_ref, scale_ref, gated_ref, squares_ref):
    members, rows, features = state_ref.shape
    c_conv = c_conv_ref[...]
    squares = jnp.zeros((c_conv.shape[0], LANES), jnp.float32)
    for j in range(features // LANES):
        tile = slice(j * LANES, (j + 1) * LANES)
        state = state_ref[:, :, tile].astype(jnp.float32).reshape(members * rows, LANES)
        carried = jnp.dot(c_conv, state.astype(jnp.bfloat16), preferred_element_type=jnp.float32)
        gated = diagonal_ref[:, tile] + scale_ref[:, tile] * carried
        gated_ref[:, tile] = gated
        squares = squares + gated * gated
    ones = jnp.ones((8, LANES), jnp.bfloat16)
    squares_ref[...] = sum(
        lax.dot_general(ones, part, (((1,), (1,)), ((), ())), preferred_element_type=jnp.float32)
        for part in reversed(bf16_parts(squares))
    )[0:1]


def normalize_kernel(features_all, squares_ref, gated_ref, gain_ref, out_ref, rows_ref, sems):
    count = squares_ref.shape[0]
    tokens, features = gated_ref.shape
    total = squares_ref[0]
    for k in range(1, count):
        total = total + squares_ref[k]
    scale = lax.rsqrt(total / features_all + epsilon)
    scale = jnp.broadcast_to(scale, (LANES, tokens)).T
    chunks = sems.shape[0]
    size = tokens // chunks
    copies = []
    for i in range(chunks):
        part = slice(i * size, (i + 1) * size)
        for j in range(features // LANES):
            tile = slice(j * LANES, (j + 1) * LANES)
            rows_ref[part, tile] = (
                gated_ref[part, tile] * scale[part] * gain_ref[j : j + 1, :]
            ).astype(jnp.bfloat16)
        copies.append(
            pltpu.make_async_copy(
                rows_ref.at[pl.ds(i * size, size), :], out_ref.at[pl.ds(i * size, size), :],
                sems.at[i],
            )
        )
        copies[-1].start()
    for copy in copies:
        copy.wait()


def body(
    inputs, gate_input, b_source, c_source, step_raw, step_bias, decay_rate, conv_weight,
    conv_bias, norm_gain, doc_lengths,
):
    tokens, features = inputs.shape
    heads = step_raw.shape[1]
    state = b_source.shape[1]
    members = 1
    for axis in GROUP:
        members *= lax.axis_size(axis)
    outer = lax.axis_size(OUTER)
    rows = state // members
    shards = members * outer
    ahead = lambda n, k: [(i, i + k) for i in range(n - k)]

    bf16 = jnp.bfloat16
    small = [doc_lengths[None, :], step_raw.T, step_bias[None, :], decay_rate[None, :]]
    tails, *small = call(
        tails_kernel,
        [out((8, 2 * state), bf16)] + [out(o.shape, o.dtype) for o in small],
        b_source, c_source, *small,
        hbm=2 + len(small), scratch=[pltpu.SemaphoreType.DMA((2 + len(small),))],
    )
    halo = lax.ppermute(tails, SEQ, ahead(shards, 1))
    operands = [
        inputs, b_source, c_source, conv_weight, conv_bias[None, :],
        norm_gain.reshape(features // LANES, LANES),
    ]
    results = call(
        prepare_kernel,
        [out(o.shape, o.dtype) for o in operands]
        + [
            out((tokens, features), bf16), out((heads, tokens)), out((heads, tokens)),
            out((tokens, LANES)), out((1, LANES)), out((tokens, LANES), jnp.int32),
            out((tokens, state)),
        ],
        *operands, *small, tails,
        hbm=len(operands),
        scratch=[
            pltpu.VMEM((LANES, tokens), jnp.float32),
            pltpu.VMEM((tokens + 8, state), jnp.float32),
            pltpu.SemaphoreType.DMA((len(operands),)),
        ],
    )
    x, b, c, taps, taps_bias, gain = results[0:6]
    weighted, cum_rows, step_rows, columns, factor, start, b_early = results[6:]
    pieces, b_conv = call(
        states_kernel,
        [out((members, rows, features + LANES)), out((tokens, state), bf16)],
        b, halo, taps, taps_bias, start, b_early, weighted, factor,
        scratch=[pltpu.VMEM((16, state), jnp.float32)],
    )
    pieces = lax.all_to_all(pieces, GROUP, 0, 0)
    pair = out((rows, features + LANES))
    before, factors, total_a, total_b, total_c = call(
        functools.partial(prefix_kernel, heads),
        [out((members, rows, features)), out((members, LANES)), pair, pair, pair],
        pieces,
        scratch=[
            pltpu.VMEM((members, LANES), jnp.float32),
            pltpu.VMEM((members, features), jnp.float32),
        ],
    )

    def diagonal_terms(turn, token, *before):
        sources = [
            c, halo, taps, taps_bias, start, b_conv, columns, cum_rows, step_rows, x, gate_input,
            factors,
        ]
        token = [] if token is None else [token]
        count = len(sources)
        return call(
            functools.partial(diagonal_kernel, turn),
            [out(t.shape) for t in token] + [
                out((members, features)), out((tokens, state), bf16), out((tokens, features)),
                out((tokens, features)),
            ],
            *sources, *token, *before, flops=20_000_000_000,
            aliases={count + k: k for k in range(len(token) + len(before))},
            scratch=[
                pltpu.VMEM((tokens, tokens), jnp.float32),
                pltpu.VMEM((tokens + 8, state), jnp.float32),
            ],
        )

    def send(total, *pairs):
        return lax.ppermute(total, OUTER, pairs)

    total_a, *diagonal = diagonal_terms(0, total_a)
    near_a = send(total_a, (0, 1))
    near_b = send(total_b, (1, 2))
    total_c, *diagonal = diagonal_terms(1, total_c, *diagonal)
    far = send(total_c, (0, 2), (1, 3))
    near_d = send(total_c, (2, 3))
    wide, c_conv, diagonal, scale = diagonal_terms(2, None, *diagonal)
    states_in = call(
        functools.partial(states_in_kernel, heads),
        out((members, rows, features), bf16),
        near_a, near_b, near_d, far, before, wide,
        scratch=[pltpu.VMEM(pair.shape, jnp.float32)],
    )
    states_in = lax.all_to_all(states_in, GROUP, 0, 0)
    gated, squares = call(
        gate_kernel,
        [out((tokens, features)), out((1, tokens))],
        states_in, c_conv, diagonal, scale,
    )
    squares = lax.all_gather(squares, "tp")
    return call(
        functools.partial(normalize_kernel, features * lax.axis_size("tp")),
        jax.ShapeDtypeStruct((tokens, features), bf16),
        squares, gated, gain, to_hbm=True,
        scratch=[pltpu.VMEM((tokens, features), bf16), pltpu.SemaphoreType.DMA((4,))],
    )


def solution(mesh):
    finer = Mesh(
        mesh.devices.reshape(4, 2, 4, 4, mesh.shape["tp"]), ("za", "zb", "y", "x", "tp")
    )
    in_specs = (
        P(SEQ, "tp"), P(SEQ, "tp"), P(SEQ, None), P(SEQ, None), P(SEQ, "tp"), P("tp"), P("tp"),
        P(), P(), P("tp"), P(),
    )
    return jax.shard_map(
        body, mesh=finer, in_specs=in_specs, out_specs=P(SEQ, "tp"), check_vma=False
    )
```

```python
import functools

import jax
import jax.numpy as jnp
from jax import lax
from jax.experimental import pallas as pl
from jax.experimental.pallas import tpu as pltpu
from jax.sharding import Mesh
from jax.sharding import PartitionSpec as P

SEQ = ("za", "zb", "y", "x")
GROUP = ("zb", "y", "x")
OUTER = "za"
LANES = 128
epsilon = 1e-05
VMEM = pl.BlockSpec(memory_space=pltpu.VMEM)
HBM = pl.BlockSpec(memory_space=pltpu.HBM)


def call(
    kernel, outs, *args, hbm=0, after=(), scratch=(), flops=1_000_000, aliases=None, to_hbm=False
):
    if after:
        inner, skip = kernel, len(after)
        kernel = lambda *refs: inner(*refs[:len(args)], *refs[len(args) + skip:])
    multiple = isinstance(outs, (list, tuple))
    return pl.pallas_call(
        kernel,
        out_shape=list(outs) if multiple else outs,
        in_specs=[HBM] * hbm + [VMEM] * (len(args) - hbm) + [VMEM] * len(after),
        out_specs=[VMEM] * len(outs) if multiple else HBM if to_hbm else VMEM,
        input_output_aliases=aliases or {},
        scratch_shapes=list(scratch),
        compiler_params=pltpu.CompilerParams(vmem_limit_bytes=24 * 1024 * 1024),
        cost_estimate=pl.CostEstimate(flops=flops, bytes_accessed=1_000_000, transcendentals=0),
    )(*(pltpu.with_memory_space_constraint(a, pltpu.HBM) for a in args[:hbm]), *args[hbm:], *after)


def out(shape, dtype=jnp.float32):
    return pltpu.VMEM(shape, dtype)


def tile_of_heads(columns, tile, width):
    per, rows = LANES // width, columns.shape[0]
    lane = lax.broadcasted_iota(jnp.int32, (rows, LANES), 1)
    h = tile * per
    spread = jnp.broadcast_to(columns[:, h : h + 1], (rows, LANES))
    for k in range(1, per):
        other = jnp.broadcast_to(columns[:, h + k : h + k + 1], (rows, LANES))
        spread = jnp.where(lane < k * width, spread, other)
    return spread


def tails_kernel(b_ref, c_ref, *refs):
    count = (len(refs) - 2) // 2
    sources, tails_ref, targets, sems = refs[:count], refs[count], refs[count + 1 : -1], refs[-1]
    tokens, state = b_ref.shape
    copies = [
        pltpu.make_async_copy(
            r.at[pl.ds(tokens - 8, 8), :], tails_ref.at[:, pl.ds(k * state, state)], sems.at[k]
        )
        for k, r in enumerate((b_ref, c_ref))
    ]
    for k, (source, target) in enumerate(zip(sources, targets)):
        copies.append(pltpu.make_async_copy(source, target, sems.at[k + 2]))
    for copy in copies:
        copy.start()
    for copy in copies:
        copy.wait()


def convolve(padded_ref, weight, bias, relative, start):
    tokens = relative.shape[0]
    taps = weight.shape[0]
    summed = jnp.broadcast_to(bias, (tokens, bias.shape[1]))
    for k in range(taps):
        back = taps - 1 - k
        term = weight[k : k + 1, :] * padded_ref[8 - back : 8 - back + tokens, :]
        summed = summed + jnp.where(relative - back >= start, term, 0.0)
    return (summed * jax.nn.sigmoid(summed)).astype(jnp.bfloat16)


def bf16_parts(value):
    parts = []
    for _ in range(3):
        part = value.astype(jnp.bfloat16)
        parts.append(part)
        value = value - part.astype(jnp.float32)
    return parts


def spread_matrix(first, last, width, at):
    row = lax.broadcasted_iota(jnp.int32, (LANES, last - first), 0)
    head = (first + lax.broadcasted_iota(jnp.int32, (LANES, last - first), 1)) // width
    inside = (row >= at) if at else (row < 32)
    return jnp.where(inside & ((row & 31) == head), 1.0, 0.0).astype(jnp.bfloat16)


def spread_rows(values, features, heads, wide_ref):
    count = values.shape[0]
    parts = jnp.concatenate(bf16_parts(jnp.where(
        lax.broadcasted_iota(jnp.int32, values.shape, 1) < heads, values, 0.0
    )), axis=0)
    for j in range(0, features, 256):
        wide = jnp.dot(
            parts, spread_matrix(j, j + 256, features // heads, 0),
            preferred_element_type=jnp.float32,
        )
        wide_ref[:, j : j + 256] = (
            wide[2 * count :] + wide[count : 2 * count]
        ) + wide[0:count]


def sequence_index():
    index = 0
    for axis in SEQ:
        index = index * lax.axis_size(axis) + lax.axis_index(axis)
    return index


def to_column(row):
    n = row.shape[1]
    same = lax.broadcasted_iota(jnp.int32, (n, n), 0) == lax.broadcasted_iota(jnp.int32, (n, n), 1)
    return jnp.sum(jnp.where(same, jnp.broadcast_to(row, (n, n)), 0.0), axis=1, keepdims=True)


WEIGHTS_AT = 32


def prepare_kernel(*refs):
    count = 6
    sources, (docs_ref, raw_ref, bias_ref, rate_ref, _) = refs[:count], refs[count : count + 5]
    targets = refs[count + 5 : 2 * count + 5]
    (
        weighted_ref, cum_rows_ref, step_rows_ref, columns_ref, factor_ref, start_ref, b_conv_ref,
        stack_ref, padded_ref, sems,
    ) = refs[2 * count + 5 :]
    x_ref, b_ref, _, taps_ref, taps_bias_ref, _ = targets
    copies = [
        pltpu.make_async_copy(source, target, sems.at[k])
        for k, (source, target) in enumerate(zip(sources, targets))
    ]
    for copy in copies:
        copy.start()
    heads, tokens = raw_ref.shape
    state = b_ref.shape[1]
    width = x_ref.shape[1] // heads
    base = sequence_index() * tokens
    relative = lax.broadcasted_iota(jnp.int32, (tokens, LANES), 0)
    start = jnp.zeros((1, 1), jnp.int32) - base
    last_position = jnp.full((1, 1), tokens - 1, jnp.int32)
    chosen = jnp.broadcast_to(start, relative.shape)
    end_start = start
    for i in range(1, docs_ref.shape[1]):
        start = start + docs_ref[0:1, i - 1 : i]
        chosen = jnp.where(start <= relative, start, chosen)
        end_start = jnp.where(start <= last_position, start, end_start)
    start_ref[...] = chosen

    step = jax.nn.softplus(raw_ref[...] + to_column(bias_ref[...]))
    log_decay = -step * to_column(rate_ref[...])
    rows = lax.broadcasted_iota(jnp.int32, (tokens, tokens), 0)
    cols = lax.broadcasted_iota(jnp.int32, (tokens, tokens), 1)
    upper = jnp.where(rows <= cols, 1.0, 0.0).astype(jnp.bfloat16)
    cum = sum(
        jnp.dot(part, upper, preferred_element_type=jnp.float32)
        for part in reversed(bf16_parts(log_decay))
    )
    cum_rows_ref[...] = cum
    step_rows_ref[...] = step
    position = lax.broadcasted_iota(jnp.int32, (heads, tokens), 1)
    weighting = jnp.where(
        position >= end_start, jnp.exp(cum[:, tokens - 1 : tokens] - cum) * step, 0.0
    )
    stack_ref[...] = jnp.zeros_like(stack_ref)
    stack_ref[0:heads, :] = cum
    for k, part in enumerate(bf16_parts(weighting)):
        at = WEIGHTS_AT * (k + 1)
        stack_ref[at : at + heads, :] = part.astype(jnp.float32)
    columns = stack_ref[...].T
    columns_ref[...] = columns
    factor_ref[...] = jnp.where(end_start < 0, jnp.exp(columns[tokens - 1 : tokens, :]), 0.0)
    for copy in copies:
        copy.wait()
    weights = columns.astype(jnp.bfloat16)
    for j in range(0, x_ref.shape[1], 256):
        tile = slice(j, j + 256)
        spread = jnp.dot(
            weights, spread_matrix(j, j + 256, width, WEIGHTS_AT),
            preferred_element_type=jnp.float32,
        )
        weighted_ref[:, tile] = (x_ref[:, tile].astype(jnp.float32) * spread).astype(jnp.bfloat16)
    side = slice(0, state)
    padded_ref[0:8, :] = jnp.zeros((8, state), jnp.float32)
    padded_ref[8:, :] = b_ref[...].astype(jnp.float32)
    b_conv = convolve(padded_ref, taps_ref[:, side], taps_bias_ref[:, side], relative, chosen)
    b_conv_ref[...] = b_conv.astype(jnp.float32)


def first_rows(source_ref, halo, weight, bias, start_ref, padded_ref):
    padded_ref[0:8, :] = halo.astype(jnp.float32)
    padded_ref[8:, :] = source_ref[0:8, :].astype(jnp.float32)
    relative = lax.broadcasted_iota(jnp.int32, (8, LANES), 0)
    return convolve(padded_ref, weight, bias, relative, start_ref[0:8, :])


def states_kernel(
    b_ref, halo_ref, taps_ref, taps_bias_ref, start_ref, b_early_ref, weighted_ref, factor_ref,
    pieces_ref, b_conv_ref, padded_ref,
):
    state, features = b_ref.shape[1], weighted_ref.shape[1]
    members, rows, _ = pieces_ref.shape
    first = first_rows(
        b_ref, halo_ref[:, 0:state], taps_ref[:, 0:state], taps_bias_ref[:, 0:state], start_ref,
        padded_ref,
    )
    b_conv = jnp.concatenate([first.astype(jnp.float32), b_early_ref[8:, :]], axis=0)
    b_conv_ref[...] = b_conv.astype(jnp.bfloat16)
    b_rows = b_conv.T.astype(jnp.bfloat16)
    for j in range(features // 256):
        tile = slice(j * 256, (j + 1) * 256)
        end_state = jnp.dot(b_rows, weighted_ref[:, tile], preferred_element_type=jnp.float32)
        for m in range(members):
            pieces_ref[m, :, tile] = end_state[m * rows : (m + 1) * rows, :]
    spread = jnp.broadcast_to(factor_ref[...], (rows, LANES))
    for m in range(members):
        pieces_ref[m, :, features:] = spread


def prefix_kernel(
    heads, pieces_ref, before_ref, factors_ref, total_a_ref, total_b_ref, total_c_ref, single_ref,
    wide_ref,
):
    members, rows, padded = pieces_ref.shape
    features = padded - LANES
    for m in range(members):
        single_ref[m : m + 1, :] = pieces_ref[m, 0:1, features:]
    spread_rows(single_ref[...], features, heads, wide_ref)
    product = jnp.ones((1, LANES), jnp.float32)
    for m in range(members):
        factors_ref[m : m + 1, :] = product
        product = product * single_ref[m : m + 1, :]
    total = jnp.zeros((rows, features), jnp.float32)
    for m in range(members):
        before_ref[m] = total
        total = wide_ref[m : m + 1, :] * total + pieces_ref[m, :, 0:features]
    for total_ref in (total_a_ref, total_b_ref, total_c_ref):
        total_ref[:, 0:features] = total
        total_ref[:, features:] = jnp.broadcast_to(product, (rows, LANES))


def wide_factor(pair_ref, features, width):
    factor = pair_ref[0:1, features:]
    return jnp.concatenate(
        [tile_of_heads(factor, j, width) for j in range(features // LANES)], axis=1
    )


def states_in_kernel(heads, *refs):
    *near_refs, far_ref, before_ref, wide_ref, state_ref, near_ref = refs
    members, _, features = before_ref.shape
    near_ref[...] = sum(ref[...] for ref in near_refs)
    factor = wide_factor(near_ref, features, features // heads)
    entering = factor * far_ref[:, 0:features] + near_ref[:, 0:features]
    for m in range(members):
        state_ref[m] = (wide_ref[m : m + 1, :] * entering + before_ref[m]).astype(jnp.bfloat16)


def products_of(
    c_ref, halo_ref, taps_ref, taps_bias_ref, start_ref, b_conv_ref, c_conv_ref, products_ref,
    padded_ref,
):
    tokens, state = c_ref.shape
    padded_ref[0:8, :] = halo_ref[:, state:].astype(jnp.float32)
    padded_ref[8:, :] = c_ref[...].astype(jnp.float32)
    relative = lax.broadcasted_iota(jnp.int32, (tokens, LANES), 0)
    c_conv = convolve(
        padded_ref, taps_ref[:, state:], taps_bias_ref[:, state:], relative, start_ref[...]
    )
    c_conv_ref[...] = c_conv
    products = lax.dot_general(
        c_conv, b_conv_ref[...], (((1,), (1,)), ((), ())), preferred_element_type=jnp.float32
    )
    row = lax.broadcasted_iota(jnp.int32, (tokens, tokens), 0)
    col = lax.broadcasted_iota(jnp.int32, (tokens, tokens), 1)
    starts = jnp.concatenate([start_ref[...]] * (tokens // LANES), axis=1)
    products_ref[...] = jnp.where((col <= row) & (col >= starts), products, 0.0)


def diagonal_of(
    start_ref, columns_ref, cum_rows_ref, step_rows_ref, x_ref, gate_ref, products_ref, gated_ref,
    scale_ref,
):
    tokens, features = x_ref.shape
    width, half = features // cum_rows_ref.shape[0], tokens // 2
    columns = columns_ref[...]
    carried = jnp.where(start_ref[...] < 0, jnp.exp(columns), 0.0)
    lane = lax.broadcasted_iota(jnp.int32, (tokens, LANES), 1)
    per = LANES // width
    for j in range(features // LANES):
        tile = slice(j * LANES, (j + 1) * LANES)
        diagonal = None
        for k in range(per):
            h = j * per + k
            column = jnp.broadcast_to(columns[:, h : h + 1], (tokens, LANES))
            cum_row, step_row = cum_rows_ref[h : h + 1, :], step_rows_ref[h : h + 1, :]
            upper = (
                products_ref[0:half, 0:half] * jnp.exp(column[0:half] - cum_row[:, 0:half])
            ) * step_row[:, 0:half]
            lower_left = (
                products_ref[half:, 0:half] * jnp.exp(column[half:] - cum_row[:, 0:half])
            ) * step_row[:, 0:half]
            lower_right = (
                products_ref[half:, half:] * jnp.exp(column[half:] - cum_row[:, half:])
            ) * step_row[:, half:]
            lower = jnp.concatenate([lower_left, lower_right], axis=1).astype(jnp.bfloat16)
            part = jnp.concatenate(
                [
                    jnp.dot(upper.astype(jnp.bfloat16), x_ref[0:half, tile],
                            preferred_element_type=jnp.float32),
                    jnp.dot(lower, x_ref[:, tile], preferred_element_type=jnp.float32),
                ],
                axis=0,
            )
            diagonal = part if diagonal is None else jnp.where(lane < k * width, diagonal, part)
        gate = gate_ref[:, tile].astype(jnp.float32)
        gate = gate * jax.nn.sigmoid(gate)
        gated_ref[:, tile] = diagonal * gate
        scale_ref[:, tile] = tile_of_heads(carried, j, width) * gate


def diagonal_kernel(turn, *refs):
    (*sources, columns_ref, cum_rows_ref, step_rows_ref, x_ref, gate_ref, factors_ref) = refs[:12]
    wide_ref, c_conv_ref, gated_ref, scale_ref, products_ref, padded_ref = refs[-6:]
    place = lax.axis_index(OUTER)
    early = (place == 0) & (lax.axis_index("tp") < lax.axis_size("tp") // 2)

    @pl.when((early, jnp.logical_not(early))[turn])
    def _():
        spread_rows(factors_ref[...], x_ref.shape[1], cum_rows_ref.shape[0], wide_ref)
        products_of(*sources, c_conv_ref, products_ref, padded_ref)
        diagonal_of(
            sources[4], columns_ref, cum_rows_ref, step_rows_ref, x_ref, gate_ref, products_ref,
            gated_ref, scale_ref,
        )


def gate_kernel(state_ref, c_conv_ref, diagonal_ref, scale_ref, gated_ref, squares_ref):
    members, rows, features = state_ref.shape
    c_conv = c_conv_ref[...]
    squares = jnp.zeros((c_conv.shape[0], LANES), jnp.float32)
    for j in range(features // LANES):
        tile = slice(j * LANES, (j + 1) * LANES)
        state = state_ref[:, :, tile].astype(jnp.float32).reshape(members * rows, LANES)
        carried = jnp.dot(c_conv, state.astype(jnp.bfloat16), preferred_element_type=jnp.float32)
        gated = diagonal_ref[:, tile] + scale_ref[:, tile] * carried
        gated_ref[:, tile] = gated
        squares = squares + gated * gated
    ones = jnp.ones((8, LANES), jnp.bfloat16)
    squares_ref[...] = sum(
        lax.dot_general(ones, part, (((1,), (1,)), ((), ())), preferred_element_type=jnp.float32)
        for part in reversed(bf16_parts(squares))
    )[0:1]


def normalize_kernel(features_all, squares_ref, gated_ref, gain_ref, out_ref, rows_ref, sems):
    count = squares_ref.shape[0]
    tokens, features = gated_ref.shape
    total = squares_ref[0]
    for k in range(1, count):
        total = total + squares_ref[k]
    scale = lax.rsqrt(total / features_all + epsilon)
    scale = jnp.broadcast_to(scale, (LANES, tokens)).T
    chunks = sems.shape[0]
    size = tokens // chunks
    copies = []
    for i in range(chunks):
        part = slice(i * size, (i + 1) * size)
        for j in range(features // LANES):
            tile = slice(j * LANES, (j + 1) * LANES)
            rows_ref[part, tile] = (
                gated_ref[part, tile] * scale[part] * gain_ref[j : j + 1, :]
            ).astype(jnp.bfloat16)
        copies.append(
            pltpu.make_async_copy(
                rows_ref.at[pl.ds(i * size, size), :], out_ref.at[pl.ds(i * size, size), :],
                sems.at[i],
            )
        )
        copies[-1].start()
    for copy in copies:
        copy.wait()


def body(
    inputs, gate_input, b_source, c_source, step_raw, step_bias, decay_rate, conv_weight,
    conv_bias, norm_gain, doc_lengths,
):
    tokens, features = inputs.shape
    heads = step_raw.shape[1]
    state = b_source.shape[1]
    members = 1
    for axis in GROUP:
        members *= lax.axis_size(axis)
    outer = lax.axis_size(OUTER)
    rows = state // members
    shards = members * outer
    ahead = lambda n, k: [(i, i + k) for i in range(n - k)]

    bf16 = jnp.bfloat16
    small = [doc_lengths[None, :], step_raw.T, step_bias[None, :], decay_rate[None, :]]
    tails, *small = call(
        tails_kernel,
        [out((8, 2 * state), bf16)] + [out(o.shape, o.dtype) for o in small],
        b_source, c_source, *small,
        hbm=2 + len(small), scratch=[pltpu.SemaphoreType.DMA((2 + len(small),))],
    )
    halo = lax.ppermute(tails, SEQ, ahead(shards, 1))
    operands = [
        inputs, b_source, c_source, conv_weight, conv_bias[None, :],
        norm_gain.reshape(features // LANES, LANES),
    ]
    results = call(
        prepare_kernel,
        [out(o.shape, o.dtype) for o in operands]
        + [
            out((tokens, features), bf16), out((heads, tokens)), out((heads, tokens)),
            out((tokens, LANES)), out((1, LANES)), out((tokens, LANES), jnp.int32),
            out((tokens, state)),
        ],
        *operands, *small, tails,
        hbm=len(operands),
        scratch=[
            pltpu.VMEM((LANES, tokens), jnp.float32),
            pltpu.VMEM((tokens + 8, state), jnp.float32),
            pltpu.SemaphoreType.DMA((len(operands),)),
        ],
    )
    x, b, c, taps, taps_bias, gain = results[0:6]
    weighted, cum_rows, step_rows, columns, factor, start, b_early = results[6:]
    pieces, b_conv = call(
        states_kernel,
        [out((members, rows, features + LANES)), out((tokens, state), bf16)],
        b, halo, taps, taps_bias, start, b_early, weighted, factor,
        scratch=[pltpu.VMEM((16, state), jnp.float32)],
    )
    pieces = lax.all_to_all(pieces, GROUP, 0, 0)
    pair = out((rows, features + LANES))
    before, factors, total_a, total_b, total_c = call(
        functools.partial(prefix_kernel, heads),
        [out((members, rows, features)), out((members, LANES)), pair, pair, pair],
        pieces,
        scratch=[
            pltpu.VMEM((members, LANES), jnp.float32),
            pltpu.VMEM((members, features), jnp.float32),
        ],
    )

    def diagonal_terms(turn, token, *before):
        sources = [
            c, halo, taps, taps_bias, start, b_conv, columns, cum_rows, step_rows, x, gate_input,
            factors,
        ]
        token = [] if token is None else [token]
        count = len(sources)
        return call(
            functools.partial(diagonal_kernel, turn),
            [out(t.shape) for t in token] + [
                out((members, features)), out((tokens, state), bf16), out((tokens, features)),
                out((tokens, features)),
            ],
            *sources, *token, *before, flops=20_000_000_000,
            aliases={count + k: k for k in range(len(token) + len(before))},
            scratch=[
                pltpu.VMEM((tokens, tokens), jnp.float32),
                pltpu.VMEM((tokens + 8, state), jnp.float32),
            ],
        )

    def send(total, *pairs):
        return lax.ppermute(total, OUTER, pairs)

    total_a, *diagonal = diagonal_terms(0, total_a)
    near_a = send(total_a, (0, 1))
    far = send(total_b, (0, 2), (1, 3))
    near_b = send(total_c, (1, 2), (2, 3))
    wide, c_conv, diagonal, scale = diagonal_terms(1, None, *diagonal)
    states_in = call(
        functools.partial(states_in_kernel, heads),
        out((members, rows, features), bf16),
        near_a, near_b, far, before, wide,
        scratch=[pltpu.VMEM(pair.shape, jnp.float32)],
    )
    states_in = lax.all_to_all(states_in, GROUP, 0, 0)
    gated, squares = call(
        gate_kernel,
        [out((tokens, features)), out((1, tokens))],
        states_in, c_conv, diagonal, scale,
    )
    squares = lax.all_gather(squares, "tp")
    return call(
        functools.partial(normalize_kernel, features * lax.axis_size("tp")),
        jax.ShapeDtypeStruct((tokens, features), bf16),
        squares, gated, gain, to_hbm=True,
        scratch=[pltpu.VMEM((tokens, features), bf16), pltpu.SemaphoreType.DMA((4,))],
    )


def solution(mesh):
    finer = Mesh(
        mesh.devices.reshape(4, 2, 4, 4, mesh.shape["tp"]), ("za", "zb", "y", "x", "tp")
    )
    in_specs = (
        P(SEQ, "tp"), P(SEQ, "tp"), P(SEQ, None), P(SEQ, None), P(SEQ, "tp"), P("tp"), P("tp"),
        P(), P(), P("tp"), P(),
    )
    return jax.shard_map(
        body, mesh=finer, in_specs=in_specs, out_specs=P(SEQ, "tp"), check_vma=False
    )
```

```python
import functools

import jax
import jax.numpy as jnp
from jax import lax
from jax.experimental import pallas as pl
from jax.experimental.pallas import tpu as pltpu
from jax.sharding import Mesh
from jax.sharding import PartitionSpec as P

SEQ = ("za", "zb", "y", "x")
GROUP = ("zb", "y", "x")
OUTER = "za"
LANES = 128
epsilon = 1e-05
VMEM = pl.BlockSpec(memory_space=pltpu.VMEM)
HBM = pl.BlockSpec(memory_space=pltpu.HBM)


def call(
    kernel, outs, *args, hbm=0, after=(), scratch=(), flops=1_000_000, aliases=None, to_hbm=False
):
    if after:
        inner, skip = kernel, len(after)
        kernel = lambda *refs: inner(*refs[:len(args)], *refs[len(args) + skip:])
    multiple = isinstance(outs, (list, tuple))
    return pl.pallas_call(
        kernel,
        out_shape=list(outs) if multiple else outs,
        in_specs=[HBM] * hbm + [VMEM] * (len(args) - hbm) + [VMEM] * len(after),
        out_specs=[VMEM] * len(outs) if multiple else HBM if to_hbm else VMEM,
        input_output_aliases=aliases or {},
        scratch_shapes=list(scratch),
        compiler_params=pltpu.CompilerParams(vmem_limit_bytes=24 * 1024 * 1024),
        cost_estimate=pl.CostEstimate(flops=flops, bytes_accessed=1_000_000, transcendentals=0),
    )(*(pltpu.with_memory_space_constraint(a, pltpu.HBM) for a in args[:hbm]), *args[hbm:], *after)


def out(shape, dtype=jnp.float32):
    return pltpu.VMEM(shape, dtype)


def tile_of_heads(columns, tile, width):
    per, rows = LANES // width, columns.shape[0]
    lane = lax.broadcasted_iota(jnp.int32, (rows, LANES), 1)
    h = tile * per
    spread = jnp.broadcast_to(columns[:, h : h + 1], (rows, LANES))
    for k in range(1, per):
        other = jnp.broadcast_to(columns[:, h + k : h + k + 1], (rows, LANES))
        spread = jnp.where(lane < k * width, spread, other)
    return spread


def tails_kernel(b_ref, c_ref, *refs):
    count = (len(refs) - 2) // 2
    sources, tails_ref, targets, sems = refs[:count], refs[count], refs[count + 1 : -1], refs[-1]
    tokens, state = b_ref.shape
    copies = [
        pltpu.make_async_copy(
            r.at[pl.ds(tokens - 8, 8), :], tails_ref.at[:, pl.ds(k * state, state)], sems.at[k]
        )
        for k, r in enumerate((b_ref, c_ref))
    ]
    for k, (source, target) in enumerate(zip(sources, targets)):
        copies.append(pltpu.make_async_copy(source, target, sems.at[k + 2]))
    for copy in copies:
        copy.start()
    for copy in copies:
        copy.wait()


def convolve(padded_ref, weight, bias, relative, start):
    tokens = relative.shape[0]
    taps = weight.shape[0]
    summed = jnp.broadcast_to(bias, (tokens, bias.shape[1]))
    for k in range(taps):
        back = taps - 1 - k
        term = weight[k : k + 1, :] * padded_ref[8 - back : 8 - back + tokens, :]
        summed = summed + jnp.where(relative - back >= start, term, 0.0)
    return (summed * jax.nn.sigmoid(summed)).astype(jnp.bfloat16)


def bf16_parts(value):
    parts = []
    for _ in range(3):
        part = value.astype(jnp.bfloat16)
        parts.append(part)
        value = value - part.astype(jnp.float32)
    return parts


def spread_matrix(first, last, width, at):
    row = lax.broadcasted_iota(jnp.int32, (LANES, last - first), 0)
    head = (first + lax.broadcasted_iota(jnp.int32, (LANES, last - first), 1)) // width
    inside = (row >= at) if at else (row < 32)
    return jnp.where(inside & ((row & 31) == head), 1.0, 0.0).astype(jnp.bfloat16)


def spread_rows(values, features, heads, wide_ref):
    count = values.shape[0]
    parts = jnp.concatenate(bf16_parts(jnp.where(
        lax.broadcasted_iota(jnp.int32, values.shape, 1) < heads, values, 0.0
    )), axis=0)
    for j in range(0, features, 256):
        wide = jnp.dot(
            parts, spread_matrix(j, j + 256, features // heads, 0),
            preferred_element_type=jnp.float32,
        )
        wide_ref[:, j : j + 256] = (
            wide[2 * count :] + wide[count : 2 * count]
        ) + wide[0:count]


def sequence_index():
    index = 0
    for axis in SEQ:
        index = index * lax.axis_size(axis) + lax.axis_index(axis)
    return index


def to_column(row):
    n = row.shape[1]
    same = lax.broadcasted_iota(jnp.int32, (n, n), 0) == lax.broadcasted_iota(jnp.int32, (n, n), 1)
    return jnp.sum(jnp.where(same, jnp.broadcast_to(row, (n, n)), 0.0), axis=1, keepdims=True)


WEIGHTS_AT = 32


def prepare_kernel(*refs):
    count = 6
    sources, (docs_ref, raw_ref, bias_ref, rate_ref, _) = refs[:count], refs[count : count + 5]
    targets = refs[count + 5 : 2 * count + 5]
    (
        weighted_ref, cum_rows_ref, step_rows_ref, columns_ref, factor_ref, start_ref, b_conv_ref,
        stack_ref, padded_ref, sems,
    ) = refs[2 * count + 5 :]
    x_ref, b_ref, _, taps_ref, taps_bias_ref, _ = targets
    copies = [
        pltpu.make_async_copy(source, target, sems.at[k])
        for k, (source, target) in enumerate(zip(sources, targets))
    ]
    for copy in copies:
        copy.start()
    heads, tokens = raw_ref.shape
    state = b_ref.shape[1]
    width = x_ref.shape[1] // heads
    base = sequence_index() * tokens
    relative = lax.broadcasted_iota(jnp.int32, (tokens, LANES), 0)
    start = jnp.zeros((1, 1), jnp.int32) - base
    last_position = jnp.full((1, 1), tokens - 1, jnp.int32)
    chosen = jnp.broadcast_to(start, relative.shape)
    end_start = start
    for i in range(1, docs_ref.shape[1]):
        start = start + docs_ref[0:1, i - 1 : i]
        chosen = jnp.where(start <= relative, start, chosen)
        end_start = jnp.where(start <= last_position, start, end_start)
    start_ref[...] = chosen

    step = jax.nn.softplus(raw_ref[...] + to_column(bias_ref[...]))
    log_decay = -step * to_column(rate_ref[...])
    rows = lax.broadcasted_iota(jnp.int32, (tokens, tokens), 0)
    cols = lax.broadcasted_iota(jnp.int32, (tokens, tokens), 1)
    upper = jnp.where(rows <= cols, 1.0, 0.0).astype(jnp.bfloat16)
    cum = sum(
        jnp.dot(part, upper, preferred_element_type=jnp.float32)
        for part in reversed(bf16_parts(log_decay))
    )
    cum_rows_ref[...] = cum
    step_rows_ref[...] = step
    position = lax.broadcasted_iota(jnp.int32, (heads, tokens), 1)
    weighting = jnp.where(
        position >= end_start, jnp.exp(cum[:, tokens - 1 : tokens] - cum) * step, 0.0
    )
    stack_ref[...] = jnp.zeros_like(stack_ref)
    stack_ref[0:heads, :] = cum
    for k, part in enumerate(bf16_parts(weighting)):
        at = WEIGHTS_AT * (k + 1)
        stack_ref[at : at + heads, :] = part.astype(jnp.float32)
    columns = stack_ref[...].T
    columns_ref[...] = columns
    factor_ref[...] = jnp.where(end_start < 0, jnp.exp(columns[tokens - 1 : tokens, :]), 0.0)
    for copy in copies:
        copy.wait()
    weights = columns.astype(jnp.bfloat16)
    for j in range(0, x_ref.shape[1], 256):
        tile = slice(j, j + 256)
        spread = jnp.dot(
            weights, spread_matrix(j, j + 256, width, WEIGHTS_AT),
            preferred_element_type=jnp.float32,
        )
        weighted_ref[:, tile] = (x_ref[:, tile].astype(jnp.float32) * spread).astype(jnp.bfloat16)
    side = slice(0, state)
    padded_ref[0:8, :] = jnp.zeros((8, state), jnp.float32)
    padded_ref[8:, :] = b_ref[...].astype(jnp.float32)
    b_conv = convolve(padded_ref, taps_ref[:, side], taps_bias_ref[:, side], relative, chosen)
    b_conv_ref[...] = b_conv.astype(jnp.float32)


def first_rows(source_ref, halo, weight, bias, start_ref, padded_ref):
    padded_ref[0:8, :] = halo.astype(jnp.float32)
    padded_ref[8:, :] = source_ref[0:8, :].astype(jnp.float32)
    relative = lax.broadcasted_iota(jnp.int32, (8, LANES), 0)
    return convolve(padded_ref, weight, bias, relative, start_ref[0:8, :])


def states_kernel(
    b_ref, halo_ref, taps_ref, taps_bias_ref, start_ref, b_early_ref, weighted_ref, factor_ref,
    pieces_ref, b_conv_ref, padded_ref,
):
    state, features = b_ref.shape[1], weighted_ref.shape[1]
    members, rows, _ = pieces_ref.shape
    first = first_rows(
        b_ref, halo_ref[:, 0:state], taps_ref[:, 0:state], taps_bias_ref[:, 0:state], start_ref,
        padded_ref,
    )
    b_conv = jnp.concatenate([first.astype(jnp.float32), b_early_ref[8:, :]], axis=0)
    b_conv_ref[...] = b_conv.astype(jnp.bfloat16)
    b_rows = b_conv.T.astype(jnp.bfloat16)
    for j in range(features // 256):
        tile = slice(j * 256, (j + 1) * 256)
        end_state = jnp.dot(b_rows, weighted_ref[:, tile], preferred_element_type=jnp.float32)
        for m in range(members):
            pieces_ref[m, :, tile] = end_state[m * rows : (m + 1) * rows, :]
    spread = jnp.broadcast_to(factor_ref[...], (rows, LANES))
    for m in range(members):
        pieces_ref[m, :, features:] = spread


def prefix_kernel(
    heads, pieces_ref, before_ref, factors_ref, total_a_ref, total_b_ref, total_c_ref, single_ref,
    wide_ref,
):
    members, rows, padded = pieces_ref.shape
    features = padded - LANES
    for m in range(members):
        single_ref[m : m + 1, :] = pieces_ref[m, 0:1, features:]
    spread_rows(single_ref[...], features, heads, wide_ref)
    product = jnp.ones((1, LANES), jnp.float32)
    for m in range(members):
        factors_ref[m : m + 1, :] = product
        product = product * single_ref[m : m + 1, :]
    total = jnp.zeros((rows, features), jnp.float32)
    for m in range(members):
        before_ref[m] = total
        total = wide_ref[m : m + 1, :] * total + pieces_ref[m, :, 0:features]
    for total_ref in (total_a_ref, total_b_ref, total_c_ref):
        total_ref[:, 0:features] = total
        total_ref[:, features:] = jnp.broadcast_to(product, (rows, LANES))


def wide_factor(pair_ref, features, width):
    factor = pair_ref[0:1, features:]
    return jnp.concatenate(
        [tile_of_heads(factor, j, width) for j in range(features // LANES)], axis=1
    )


def states_in_kernel(heads, *refs):
    *near_refs, far_ref, before_ref, wide_ref, state_ref, near_ref = refs
    members, _, features = before_ref.shape
    near_ref[...] = sum(ref[...] for ref in near_refs)
    factor = wide_factor(near_ref, features, features // heads)
    entering = factor * far_ref[:, 0:features] + near_ref[:, 0:features]
    for m in range(members):
        state_ref[m] = (wide_ref[m : m + 1, :] * entering + before_ref[m]).astype(jnp.bfloat16)


def products_of(
    c_ref, halo_ref, taps_ref, taps_bias_ref, start_ref, b_conv_ref, c_conv_ref, products_ref,
    padded_ref,
):
    tokens, state = c_ref.shape
    padded_ref[0:8, :] = halo_ref[:, state:].astype(jnp.float32)
    padded_ref[8:, :] = c_ref[...].astype(jnp.float32)
    relative = lax.broadcasted_iota(jnp.int32, (tokens, LANES), 0)
    c_conv = convolve(
        padded_ref, taps_ref[:, state:], taps_bias_ref[:, state:], relative, start_ref[...]
    )
    c_conv_ref[...] = c_conv
    products = lax.dot_general(
        c_conv, b_conv_ref[...], (((1,), (1,)), ((), ())), preferred_element_type=jnp.float32
    )
    row = lax.broadcasted_iota(jnp.int32, (tokens, tokens), 0)
    col = lax.broadcasted_iota(jnp.int32, (tokens, tokens), 1)
    starts = jnp.concatenate([start_ref[...]] * (tokens // LANES), axis=1)
    products_ref[...] = jnp.where((col <= row) & (col >= starts), products, 0.0)


def diagonal_of(
    start_ref, columns_ref, cum_rows_ref, step_rows_ref, x_ref, gate_ref, products_ref, gated_ref,
    scale_ref,
):
    tokens, features = x_ref.shape
    width, half = features // cum_rows_ref.shape[0], tokens // 2
    columns = columns_ref[...]
    carried = jnp.where(start_ref[...] < 0, jnp.exp(columns), 0.0)
    lane = lax.broadcasted_iota(jnp.int32, (tokens, LANES), 1)
    per = LANES // width
    for j in range(features // LANES):
        tile = slice(j * LANES, (j + 1) * LANES)
        diagonal = None
        for k in range(per):
            h = j * per + k
            column = jnp.broadcast_to(columns[:, h : h + 1], (tokens, LANES))
            cum_row, step_row = cum_rows_ref[h : h + 1, :], step_rows_ref[h : h + 1, :]
            upper = (
                products_ref[0:half, 0:half] * jnp.exp(column[0:half] - cum_row[:, 0:half])
            ) * step_row[:, 0:half]
            lower_left = (
                products_ref[half:, 0:half] * jnp.exp(column[half:] - cum_row[:, 0:half])
            ) * step_row[:, 0:half]
            lower_right = (
                products_ref[half:, half:] * jnp.exp(column[half:] - cum_row[:, half:])
            ) * step_row[:, half:]
            lower = jnp.concatenate([lower_left, lower_right], axis=1).astype(jnp.bfloat16)
            part = jnp.concatenate(
                [
                    jnp.dot(upper.astype(jnp.bfloat16), x_ref[0:half, tile],
                            preferred_element_type=jnp.float32),
                    jnp.dot(lower, x_ref[:, tile], preferred_element_type=jnp.float32),
                ],
                axis=0,
            )
            diagonal = part if diagonal is None else jnp.where(lane < k * width, diagonal, part)
        gate = gate_ref[:, tile].astype(jnp.float32)
        gate = gate * jax.nn.sigmoid(gate)
        gated_ref[:, tile] = diagonal * gate
        scale_ref[:, tile] = tile_of_heads(carried, j, width) * gate


def diagonal_kernel(turn, *refs):
    (*sources, columns_ref, cum_rows_ref, step_rows_ref, x_ref, gate_ref, factors_ref) = refs[:12]
    wide_ref, c_conv_ref, gated_ref, scale_ref, products_ref, padded_ref = refs[-6:]
    place = lax.axis_index(OUTER)

    @pl.when((place == 0, place == 1, place >= 2)[turn])
    def _():
        spread_rows(factors_ref[...], x_ref.shape[1], cum_rows_ref.shape[0], wide_ref)
        products_of(*sources, c_conv_ref, products_ref, padded_ref)
        diagonal_of(
            sources[4], columns_ref, cum_rows_ref, step_rows_ref, x_ref, gate_ref, products_ref,
            gated_ref, scale_ref,
        )


def gate_kernel(state_ref, c_conv_ref, diagonal_ref, scale_ref, gated_ref, squares_ref):
    members, rows, features = state_ref.shape
    c_conv = c_conv_ref[...]
    squares = jnp.zeros((c_conv.shape[0], LANES), jnp.float32)
    for j in range(features // LANES):
        tile = slice(j * LANES, (j + 1) * LANES)
        state = state_ref[:, :, tile].astype(jnp.float32).reshape(members * rows, LANES)
        carried = jnp.dot(c_conv, state.astype(jnp.bfloat16), preferred_element_type=jnp.float32)
        gated = diagonal_ref[:, tile] + scale_ref[:, tile] * carried
        gated_ref[:, tile] = gated
        squares = squares + gated * gated
    ones = jnp.ones((8, LANES), jnp.bfloat16)
    squares_ref[...] = sum(
        lax.dot_general(ones, part, (((1,), (1,)), ((), ())), preferred_element_type=jnp.float32)
        for part in reversed(bf16_parts(squares))
    )[0:1]


def normalize_kernel(features_all, squares_ref, gated_ref, gain_ref, out_ref, rows_ref, sems):
    count = squares_ref.shape[0]
    tokens, features = gated_ref.shape
    total = squares_ref[0]
    for k in range(1, count):
        total = total + squares_ref[k]
    scale = lax.rsqrt(total / features_all + epsilon)
    scale = jnp.broadcast_to(scale, (LANES, tokens)).T
    chunks = sems.shape[0]
    size = tokens // chunks
    copies = []
    for i in range(chunks):
        part = slice(i * size, (i + 1) * size)
        for j in range(features // LANES):
            tile = slice(j * LANES, (j + 1) * LANES)
            rows_ref[part, tile] = (
                gated_ref[part, tile] * scale[part] * gain_ref[j : j + 1, :]
            ).astype(jnp.bfloat16)
        copies.append(
            pltpu.make_async_copy(
                rows_ref.at[pl.ds(i * size, size), :], out_ref.at[pl.ds(i * size, size), :],
                sems.at[i],
            )
        )
        copies[-1].start()
    for copy in copies:
        copy.wait()


def body(
    inputs, gate_input, b_source, c_source, step_raw, step_bias, decay_rate, conv_weight,
    conv_bias, norm_gain, doc_lengths,
):
    tokens, features = inputs.shape
    heads = step_raw.shape[1]
    state = b_source.shape[1]
    members = 1
    for axis in GROUP:
        members *= lax.axis_size(axis)
    outer = lax.axis_size(OUTER)
    rows = state // members
    shards = members * outer
    ahead = lambda n, k: [(i, i + k) for i in range(n - k)]

    bf16 = jnp.bfloat16
    small = [doc_lengths[None, :], step_raw.T, step_bias[None, :], decay_rate[None, :]]
    tails, *small = call(
        tails_kernel,
        [out((8, 2 * state), bf16)] + [out(o.shape, o.dtype) for o in small],
        b_source, c_source, *small,
        hbm=2 + len(small), scratch=[pltpu.SemaphoreType.DMA((2 + len(small),))],
    )
    halo = lax.ppermute(tails, SEQ, ahead(shards, 1))
    operands = [
        inputs, b_source, c_source, conv_weight, conv_bias[None, :],
        norm_gain.reshape(features // LANES, LANES),
    ]
    results = call(
        prepare_kernel,
        [out(o.shape, o.dtype) for o in operands]
        + [
            out((tokens, features), bf16), out((heads, tokens)), out((heads, tokens)),
            out((tokens, LANES)), out((1, LANES)), out((tokens, LANES), jnp.int32),
            out((tokens, state)),
        ],
        *operands, *small, tails,
        hbm=len(operands),
        scratch=[
            pltpu.VMEM((LANES, tokens), jnp.float32),
            pltpu.VMEM((tokens + 8, state), jnp.float32),
            pltpu.SemaphoreType.DMA((len(operands),)),
        ],
    )
    x, b, c, taps, taps_bias, gain = results[0:6]
    weighted, cum_rows, step_rows, columns, factor, start, b_early = results[6:]
    pieces, b_conv = call(
        states_kernel,
        [out((members, rows, features + LANES)), out((tokens, state), bf16)],
        b, halo, taps, taps_bias, start, b_early, weighted, factor,
        scratch=[pltpu.VMEM((16, state), jnp.float32)],
    )
    pieces = lax.all_to_all(pieces, GROUP, 0, 0)
    pair = out((rows, features + LANES))
    before, factors, total_a, total_b, total_c = call(
        functools.partial(prefix_kernel, heads),
        [out((members, rows, features)), out((members, LANES)), pair, pair, pair],
        pieces,
        scratch=[
            pltpu.VMEM((members, LANES), jnp.float32),
            pltpu.VMEM((members, features), jnp.float32),
        ],
    )

    def diagonal_terms(turn, token, *before):
        sources = [
            c, halo, taps, taps_bias, start, b_conv, columns, cum_rows, step_rows, x, gate_input,
            factors,
        ]
        token = [] if token is None else [token]
        count = len(sources)
        return call(
            functools.partial(diagonal_kernel, turn),
            [out(t.shape) for t in token] + [
                out((members, features)), out((tokens, state), bf16), out((tokens, features)),
                out((tokens, features)),
            ],
            *sources, *token, *before, flops=20_000_000_000,
            aliases={count + k: k for k in range(len(token) + len(before))},
            scratch=[
                pltpu.VMEM((tokens, tokens), jnp.float32),
                pltpu.VMEM((tokens + 8, state), jnp.float32),
            ],
        )

    def send(total, *pairs):
        return lax.ppermute(total, OUTER, pairs)

    total_a, *diagonal = diagonal_terms(0, total_a)
    near_a = send(total_a, (0, 1))
    total_b, *diagonal = diagonal_terms(1, total_b, *diagonal)
    far = send(total_b, (0, 2), (1, 3))
    near_b = send(total_c, (1, 2), (2, 3))
    wide, c_conv, diagonal, scale = diagonal_terms(2, None, *diagonal)
    states_in = call(
        functools.partial(states_in_kernel, heads),
        out((members, rows, features), bf16),
        near_a, near_b, far, before, wide,
        scratch=[pltpu.VMEM(pair.shape, jnp.float32)],
    )
    states_in = lax.all_to_all(states_in, GROUP, 0, 0)
    gated, squares = call(
        gate_kernel,
        [out((tokens, features)), out((1, tokens))],
        states_in, c_conv, diagonal, scale,
    )
    squares = lax.all_gather(squares, "tp")
    return call(
        functools.partial(normalize_kernel, features * lax.axis_size("tp")),
        jax.ShapeDtypeStruct((tokens, features), bf16),
        squares, gated, gain, to_hbm=True,
        scratch=[pltpu.VMEM((tokens, features), bf16), pltpu.SemaphoreType.DMA((4,))],
    )


def solution(mesh):
    finer = Mesh(
        mesh.devices.reshape(4, 2, 4, 4, mesh.shape["tp"]), ("za", "zb", "y", "x", "tp")
    )
    in_specs = (
        P(SEQ, "tp"), P(SEQ, "tp"), P(SEQ, None), P(SEQ, None), P(SEQ, "tp"), P("tp"), P("tp"),
        P(), P(), P("tp"), P(),
    )
    return jax.shard_map(
        body, mesh=finer, in_specs=in_specs, out_specs=P(SEQ, "tp"), check_vma=False
    )
```

```python
import functools

import jax
import jax.numpy as jnp
from jax import lax
from jax.experimental import pallas as pl
from jax.experimental.pallas import tpu as pltpu
from jax.sharding import Mesh
from jax.sharding import PartitionSpec as P

SEQ = ("za", "zb", "y", "x")
GROUP = ("zb", "y", "x")
OUTER = "za"
LANES = 128
epsilon = 1e-05
VMEM = pl.BlockSpec(memory_space=pltpu.VMEM)
HBM = pl.BlockSpec(memory_space=pltpu.HBM)


def call(
    kernel, outs, *args, hbm=0, after=(), scratch=(), flops=1_000_000, aliases=None, to_hbm=False
):
    if after:
        inner, skip = kernel, len(after)
        kernel = lambda *refs: inner(*refs[:len(args)], *refs[len(args) + skip:])
    multiple = isinstance(outs, (list, tuple))
    return pl.pallas_call(
        kernel,
        out_shape=list(outs) if multiple else outs,
        in_specs=[HBM] * hbm + [VMEM] * (len(args) - hbm) + [VMEM] * len(after),
        out_specs=[VMEM] * len(outs) if multiple else HBM if to_hbm else VMEM,
        input_output_aliases=aliases or {},
        scratch_shapes=list(scratch),
        compiler_params=pltpu.CompilerParams(vmem_limit_bytes=24 * 1024 * 1024),
        cost_estimate=pl.CostEstimate(flops=flops, bytes_accessed=1_000_000, transcendentals=0),
    )(*(pltpu.with_memory_space_constraint(a, pltpu.HBM) for a in args[:hbm]), *args[hbm:], *after)


def out(shape, dtype=jnp.float32):
    return pltpu.VMEM(shape, dtype)


def tile_of_heads(columns, tile, width):
    per, rows = LANES // width, columns.shape[0]
    lane = lax.broadcasted_iota(jnp.int32, (rows, LANES), 1)
    h = tile * per
    spread = jnp.broadcast_to(columns[:, h : h + 1], (rows, LANES))
    for k in range(1, per):
        other = jnp.broadcast_to(columns[:, h + k : h + k + 1], (rows, LANES))
        spread = jnp.where(lane < k * width, spread, other)
    return spread


def tails_kernel(b_ref, c_ref, tails_ref, sems):
    tokens, state = b_ref.shape
    copies = [
        pltpu.make_async_copy(
            r.at[pl.ds(tokens - 8, 8), :], tails_ref.at[:, pl.ds(k * state, state)], sems.at[k]
        )
        for k, r in enumerate((b_ref, c_ref))
    ]
    for copy in copies:
        copy.start()
    for copy in copies:
        copy.wait()


def convolve(padded_ref, weight, bias, relative, start):
    tokens = relative.shape[0]
    taps = weight.shape[0]
    summed = jnp.broadcast_to(bias, (tokens, bias.shape[1]))
    for k in range(taps):
        back = taps - 1 - k
        term = weight[k : k + 1, :] * padded_ref[8 - back : 8 - back + tokens, :]
        summed = summed + jnp.where(relative - back >= start, term, 0.0)
    return (summed * jax.nn.sigmoid(summed)).astype(jnp.bfloat16)


def bf16_parts(value):
    parts = []
    for _ in range(3):
        part = value.astype(jnp.bfloat16)
        parts.append(part)
        value = value - part.astype(jnp.float32)
    return parts


def spread_matrix(first, last, width, at):
    row = lax.broadcasted_iota(jnp.int32, (LANES, last - first), 0)
    head = (first + lax.broadcasted_iota(jnp.int32, (LANES, last - first), 1)) // width
    inside = (row >= at) if at else (row < 32)
    return jnp.where(inside & ((row & 31) == head), 1.0, 0.0).astype(jnp.bfloat16)


def spread_rows(values, features, heads, wide_ref):
    count = values.shape[0]
    parts = jnp.concatenate(bf16_parts(jnp.where(
        lax.broadcasted_iota(jnp.int32, values.shape, 1) < heads, values, 0.0
    )), axis=0)
    for j in range(0, features, 256):
        wide = jnp.dot(
            parts, spread_matrix(j, j + 256, features // heads, 0),
            preferred_element_type=jnp.float32,
        )
        wide_ref[:, j : j + 256] = (
            wide[2 * count :] + wide[count : 2 * count]
        ) + wide[0:count]


def sequence_index():
    index = 0
    for axis in SEQ:
        index = index * lax.axis_size(axis) + lax.axis_index(axis)
    return index


def to_column(row):
    n = row.shape[1]
    same = lax.broadcasted_iota(jnp.int32, (n, n), 0) == lax.broadcasted_iota(jnp.int32, (n, n), 1)
    return jnp.sum(jnp.where(same, jnp.broadcast_to(row, (n, n)), 0.0), axis=1, keepdims=True)


WEIGHTS_AT = 32


def prepare_kernel(*refs):
    count, held = 10, 4
    sources, kept = refs[:count], refs[count + 1 : 2 * count + 1 - held]
    (
        weighted_ref, cum_rows_ref, step_rows_ref, columns_ref, factor_ref, start_ref, b_conv_ref,
        stack_ref, padded_ref, sems, docs_ref, raw_ref, bias_ref, rate_ref,
    ) = refs[2 * count + 1 - held :]
    b_ref, taps_ref, taps_bias_ref, x_ref, _, _ = kept
    copies = [
        pltpu.make_async_copy(source, target, sems.at[k])
        for k, (source, target) in enumerate(
            zip(sources, (docs_ref, raw_ref, bias_ref, rate_ref, *kept))
        )
    ]
    for copy in copies:
        copy.start()
    for copy in copies[:4]:
        copy.wait()
    heads, tokens = raw_ref.shape
    state = b_ref.shape[1]
    width = x_ref.shape[1] // heads
    base = sequence_index() * tokens
    relative = lax.broadcasted_iota(jnp.int32, (tokens, LANES), 0)
    start = jnp.zeros((1, 1), jnp.int32) - base
    last_position = jnp.full((1, 1), tokens - 1, jnp.int32)
    chosen = jnp.broadcast_to(start, relative.shape)
    end_start = start
    for i in range(1, docs_ref.shape[1]):
        start = start + docs_ref[0:1, i - 1 : i]
        chosen = jnp.where(start <= relative, start, chosen)
        end_start = jnp.where(start <= last_position, start, end_start)
    start_ref[...] = chosen

    step = jax.nn.softplus(raw_ref[...] + to_column(bias_ref[...]))
    log_decay = -step * to_column(rate_ref[...])
    rows = lax.broadcasted_iota(jnp.int32, (tokens, tokens), 0)
    cols = lax.broadcasted_iota(jnp.int32, (tokens, tokens), 1)
    upper = jnp.where(rows <= cols, 1.0, 0.0).astype(jnp.bfloat16)
    cum = sum(
        jnp.dot(part, upper, preferred_element_type=jnp.float32)
        for part in reversed(bf16_parts(log_decay))
    )
    cum_rows_ref[...] = cum
    step_rows_ref[...] = step
    position = lax.broadcasted_iota(jnp.int32, (heads, tokens), 1)
    weighting = jnp.where(
        position >= end_start, jnp.exp(cum[:, tokens - 1 : tokens] - cum) * step, 0.0
    )
    stack_ref[...] = jnp.zeros_like(stack_ref)
    stack_ref[0:heads, :] = cum
    for k, part in enumerate(bf16_parts(weighting)):
        at = WEIGHTS_AT * (k + 1)
        stack_ref[at : at + heads, :] = part.astype(jnp.float32)
    columns = stack_ref[...].T
    columns_ref[...] = columns
    factor_ref[...] = jnp.where(end_start < 0, jnp.exp(columns[tokens - 1 : tokens, :]), 0.0)
    for copy in copies[4:7]:
        copy.wait()
    side = slice(0, state)
    padded_ref[0:8, :] = jnp.zeros((8, state), jnp.float32)
    padded_ref[8:, :] = b_ref[...].astype(jnp.float32)
    b_conv = convolve(padded_ref, taps_ref[:, side], taps_bias_ref[:, side], relative, chosen)
    b_conv_ref[...] = b_conv.astype(jnp.float32)
    for copy in copies[7:]:
        copy.wait()
    weights = columns.astype(jnp.bfloat16)
    for j in range(0, x_ref.shape[1], 256):
        tile = slice(j, j + 256)
        spread = jnp.dot(
            weights, spread_matrix(j, j + 256, width, WEIGHTS_AT),
            preferred_element_type=jnp.float32,
        )
        weighted_ref[:, tile] = (x_ref[:, tile].astype(jnp.float32) * spread).astype(jnp.bfloat16)


def first_rows(source_ref, halo, weight, bias, start_ref, padded_ref):
    padded_ref[0:8, :] = halo.astype(jnp.float32)
    padded_ref[8:, :] = source_ref[0:8, :].astype(jnp.float32)
    relative = lax.broadcasted_iota(jnp.int32, (8, LANES), 0)
    return convolve(padded_ref, weight, bias, relative, start_ref[0:8, :])


def states_kernel(
    b_ref, halo_ref, taps_ref, taps_bias_ref, start_ref, b_early_ref, weighted_ref, factor_ref,
    pieces_ref, b_conv_ref, padded_ref,
):
    state, features = b_ref.shape[1], weighted_ref.shape[1]
    members, rows, _ = pieces_ref.shape
    first = first_rows(
        b_ref, halo_ref[:, 0:state], taps_ref[:, 0:state], taps_bias_ref[:, 0:state], start_ref,
        padded_ref,
    )
    b_conv = jnp.concatenate([first.astype(jnp.float32), b_early_ref[8:, :]], axis=0)
    b_conv_ref[...] = b_conv.astype(jnp.bfloat16)
    b_rows = b_conv.T.astype(jnp.bfloat16)
    for j in range(features // 256):
        tile = slice(j * 256, (j + 1) * 256)
        end_state = jnp.dot(b_rows, weighted_ref[:, tile], preferred_element_type=jnp.float32)
        for m in range(members):
            pieces_ref[m, :, tile] = end_state[m * rows : (m + 1) * rows, :]
    spread = jnp.broadcast_to(factor_ref[...], (rows, LANES))
    for m in range(members):
        pieces_ref[m, :, features:] = spread


def prefix_kernel(
    heads, pieces_ref, before_ref, factors_ref, total_a_ref, total_b_ref, total_c_ref, single_ref,
    wide_ref,
):
    members, rows, padded = pieces_ref.shape
    features = padded - LANES
    for m in range(members):
        single_ref[m : m + 1, :] = pieces_ref[m, 0:1, features:]
    spread_rows(single_ref[...], features, heads, wide_ref)
    product = jnp.ones((1, LANES), jnp.float32)
    for m in range(members):
        factors_ref[m : m + 1, :] = product
        product = product * single_ref[m : m + 1, :]
    total = jnp.zeros((rows, features), jnp.float32)
    for m in range(members):
        before_ref[m] = total
        total = wide_ref[m : m + 1, :] * total + pieces_ref[m, :, 0:features]
    for total_ref in (total_a_ref, total_b_ref, total_c_ref):
        total_ref[:, 0:features] = total
        total_ref[:, features:] = jnp.broadcast_to(product, (rows, LANES))


def wide_factor(pair_ref, features, width):
    factor = pair_ref[0:1, features:]
    return jnp.concatenate(
        [tile_of_heads(factor, j, width) for j in range(features // LANES)], axis=1
    )


def states_in_kernel(heads, *refs):
    *near_refs, far_a_ref, far_b_ref, before_ref, wide_ref, state_ref, near_ref = refs
    members, _, features = before_ref.shape
    near_ref[...] = sum(ref[...] for ref in near_refs)
    factor = wide_factor(near_ref, features, features // heads)
    far = far_a_ref[:, 0:features] + far_b_ref[:, 0:features]
    entering = factor * far + near_ref[:, 0:features]
    for m in range(members):
        state_ref[m] = (wide_ref[m : m + 1, :] * entering + before_ref[m]).astype(jnp.bfloat16)


def products_of(
    c_ref, halo_ref, taps_ref, taps_bias_ref, start_ref, b_conv_ref, c_conv_ref, products_ref,
    padded_ref,
):
    tokens, state = c_ref.shape
    padded_ref[0:8, :] = halo_ref[:, state:].astype(jnp.float32)
    padded_ref[8:, :] = c_ref[...].astype(jnp.float32)
    relative = lax.broadcasted_iota(jnp.int32, (tokens, LANES), 0)
    c_conv = convolve(
        padded_ref, taps_ref[:, state:], taps_bias_ref[:, state:], relative, start_ref[...]
    )
    c_conv_ref[...] = c_conv
    products = lax.dot_general(
        c_conv, b_conv_ref[...], (((1,), (1,)), ((), ())), preferred_element_type=jnp.float32
    )
    row = lax.broadcasted_iota(jnp.int32, (tokens, tokens), 0)
    col = lax.broadcasted_iota(jnp.int32, (tokens, tokens), 1)
    starts = jnp.concatenate([start_ref[...]] * (tokens // LANES), axis=1)
    products_ref[...] = jnp.where((col <= row) & (col >= starts), products, 0.0)


def diagonal_of(
    start_ref, columns_ref, cum_rows_ref, step_rows_ref, x_ref, gate_ref, products_ref, gated_ref,
    scale_ref,
):
    tokens, features = x_ref.shape
    width, half = features // cum_rows_ref.shape[0], tokens // 2
    columns = columns_ref[...]
    carried = jnp.where(start_ref[...] < 0, jnp.exp(columns), 0.0)
    lane = lax.broadcasted_iota(jnp.int32, (tokens, LANES), 1)
    per = LANES // width
    for j in range(features // LANES):
        tile = slice(j * LANES, (j + 1) * LANES)
        diagonal = None
        for k in range(per):
            h = j * per + k
            column = jnp.broadcast_to(columns[:, h : h + 1], (tokens, LANES))
            cum_row, step_row = cum_rows_ref[h : h + 1, :], step_rows_ref[h : h + 1, :]
            upper = (
                products_ref[0:half, 0:half] * jnp.exp(column[0:half] - cum_row[:, 0:half])
            ) * step_row[:, 0:half]
            lower_left = (
                products_ref[half:, 0:half] * jnp.exp(column[half:] - cum_row[:, 0:half])
            ) * step_row[:, 0:half]
            lower_right = (
                products_ref[half:, half:] * jnp.exp(column[half:] - cum_row[:, half:])
            ) * step_row[:, half:]
            lower = jnp.concatenate([lower_left, lower_right], axis=1).astype(jnp.bfloat16)
            part = jnp.concatenate(
                [
                    jnp.dot(upper.astype(jnp.bfloat16), x_ref[0:half, tile],
                            preferred_element_type=jnp.float32),
                    jnp.dot(lower, x_ref[:, tile], preferred_element_type=jnp.float32),
                ],
                axis=0,
            )
            diagonal = part if diagonal is None else jnp.where(lane < k * width, diagonal, part)
        gate = gate_ref[:, tile].astype(jnp.float32)
        gate = gate * jax.nn.sigmoid(gate)
        gated_ref[:, tile] = diagonal * gate
        scale_ref[:, tile] = tile_of_heads(carried, j, width) * gate


def diagonal_kernel(turn, *refs):
    (*sources, columns_ref, cum_rows_ref, step_rows_ref, x_ref, gate_ref, factors_ref) = refs[:12]
    wide_ref, c_conv_ref, gated_ref, scale_ref, products_ref, padded_ref = refs[-6:]
    place = lax.axis_index(OUTER)

    @pl.when((place == 0, place == 1, place >= 2)[turn])
    def _():
        spread_rows(factors_ref[...], x_ref.shape[1], cum_rows_ref.shape[0], wide_ref)
        products_of(*sources, c_conv_ref, products_ref, padded_ref)
        diagonal_of(
            sources[4], columns_ref, cum_rows_ref, step_rows_ref, x_ref, gate_ref, products_ref,
            gated_ref, scale_ref,
        )


def gate_kernel(state_ref, c_conv_ref, diagonal_ref, scale_ref, gated_ref, squares_ref):
    members, rows, features = state_ref.shape
    c_conv = c_conv_ref[...]
    squares = jnp.zeros((c_conv.shape[0], LANES), jnp.float32)
    for j in range(features // LANES):
        tile = slice(j * LANES, (j + 1) * LANES)
        state = state_ref[:, :, tile].astype(jnp.float32).reshape(members * rows, LANES)
        carried = jnp.dot(c_conv, state.astype(jnp.bfloat16), preferred_element_type=jnp.float32)
        gated = diagonal_ref[:, tile] + scale_ref[:, tile] * carried
        gated_ref[:, tile] = gated
        squares = squares + gated * gated
    ones = jnp.ones((8, LANES), jnp.bfloat16)
    squares_ref[...] = sum(
        lax.dot_general(ones, part, (((1,), (1,)), ((), ())), preferred_element_type=jnp.float32)
        for part in reversed(bf16_parts(squares))
    )[0:1]


def normalize_kernel(features_all, squares_ref, gated_ref, gain_ref, out_ref, rows_ref, sems):
    count = squares_ref.shape[0]
    tokens, features = gated_ref.shape
    total = squares_ref[0]
    for k in range(1, count):
        total = total + squares_ref[k]
    scale = lax.rsqrt(total / features_all + epsilon)
    scale = jnp.broadcast_to(scale, (LANES, tokens)).T
    chunks = sems.shape[0]
    size = tokens // chunks
    copies = []
    for i in range(chunks):
        part = slice(i * size, (i + 1) * size)
        for j in range(features // LANES):
            tile = slice(j * LANES, (j + 1) * LANES)
            rows_ref[part, tile] = (
                gated_ref[part, tile] * scale[part] * gain_ref[j : j + 1, :]
            ).astype(jnp.bfloat16)
        copies.append(
            pltpu.make_async_copy(
                rows_ref.at[pl.ds(i * size, size), :], out_ref.at[pl.ds(i * size, size), :],
                sems.at[i],
            )
        )
        copies[-1].start()
    for copy in copies:
        copy.wait()


def body(
    inputs, gate_input, b_source, c_source, step_raw, step_bias, decay_rate, conv_weight,
    conv_bias, norm_gain, doc_lengths,
):
    tokens, features = inputs.shape
    heads = step_raw.shape[1]
    state = b_source.shape[1]
    members = 1
    for axis in GROUP:
        members *= lax.axis_size(axis)
    outer = lax.axis_size(OUTER)
    rows = state // members
    shards = members * outer
    ahead = lambda n, k: [(i, i + k) for i in range(n - k)]

    bf16 = jnp.bfloat16
    tails = call(
        tails_kernel, out((8, 2 * state), bf16), b_source, c_source,
        hbm=2, scratch=[pltpu.SemaphoreType.DMA((2,))],
    )
    halo = lax.ppermute(tails, SEQ, ahead(shards, 1))
    operands = [
        doc_lengths[None, :], step_raw.T, step_bias[None, :], decay_rate[None, :], b_source,
        conv_weight, conv_bias[None, :], inputs, c_source,
        norm_gain.reshape(features // LANES, LANES),
    ]
    results = call(
        prepare_kernel,
        [out(o.shape, o.dtype) for o in operands[4:]]
        + [
            out((tokens, features), bf16), out((heads, tokens)), out((heads, tokens)),
            out((tokens, LANES)), out((1, LANES)), out((tokens, LANES), jnp.int32),
            out((tokens, state)),
        ],
        *operands, tails,
        hbm=len(operands),
        scratch=[
            pltpu.VMEM((LANES, tokens), jnp.float32),
            pltpu.VMEM((tokens + 8, state), jnp.float32),
            pltpu.SemaphoreType.DMA((len(operands),)),
            *(pltpu.VMEM(o.shape, o.dtype) for o in operands[:4]),
        ],
    )
    b, taps, taps_bias, x, c, gain = results[0:6]
    weighted, cum_rows, step_rows, columns, factor, start, b_early = results[6:]
    pieces, b_conv = call(
        states_kernel,
        [out((members, rows, features + LANES)), out((tokens, state), bf16)],
        b, halo, taps, taps_bias, start, b_early, weighted, factor,
        scratch=[pltpu.VMEM((16, state), jnp.float32)],
    )
    pieces = lax.all_to_all(pieces, GROUP, 0, 0)
    pair = out((rows, features + LANES))
    before, factors, total_a, total_b, total_c = call(
        functools.partial(prefix_kernel, heads),
        [out((members, rows, features)), out((members, LANES)), pair, pair, pair],
        pieces,
        scratch=[
            pltpu.VMEM((members, LANES), jnp.float32),
            pltpu.VMEM((members, features), jnp.float32),
        ],
    )

    def diagonal_terms(turn, token, *before):
        sources = [
            c, halo, taps, taps_bias, start, b_conv, columns, cum_rows, step_rows, x, gate_input,
            factors,
        ]
        token = [] if token is None else [token]
        count = len(sources)
        return call(
            functools.partial(diagonal_kernel, turn),
            [out(t.shape) for t in token] + [
                out((members, features)), out((tokens, state), bf16), out((tokens, features)),
                out((tokens, features)),
            ],
            *sources, *token, *before, flops=20_000_000_000,
            aliases={count + k: k for k in range(len(token) + len(before))},
            scratch=[
                pltpu.VMEM((tokens, tokens), jnp.float32),
                pltpu.VMEM((tokens + 8, state), jnp.float32),
            ],
        )

    def send(total, *pairs):
        return lax.ppermute(total, OUTER, pairs)

    total_a, *diagonal = diagonal_terms(0, total_a)
    near_a = send(total_a, (0, 1))
    total_b, *diagonal = diagonal_terms(1, total_b, *diagonal)
    far_a = send(total_b, (0, 2))
    near_b = send(total_c, (1, 2), (2, 3))
    far_b = send(total_b, (1, 3))
    wide, c_conv, diagonal, scale = diagonal_terms(2, None, *diagonal)
    states_in = call(
        functools.partial(states_in_kernel, heads),
        out((members, rows, features), bf16),
        near_a, near_b, far_a, far_b, before, wide,
        scratch=[pltpu.VMEM(pair.shape, jnp.float32)],
    )
    states_in = lax.all_to_all(states_in, GROUP, 0, 0)
    gated, squares = call(
        gate_kernel,
        [out((tokens, features)), out((1, tokens))],
        states_in, c_conv, diagonal, scale,
    )
    squares = lax.all_gather(squares, "tp")
    return call(
        functools.partial(normalize_kernel, features * lax.axis_size("tp")),
        jax.ShapeDtypeStruct((tokens, features), bf16),
        squares, gated, gain, to_hbm=True,
        scratch=[pltpu.VMEM((tokens, features), bf16), pltpu.SemaphoreType.DMA((4,))],
    )


def solution(mesh):
    finer = Mesh(
        mesh.devices.reshape(4, 2, 4, 4, mesh.shape["tp"]), ("za", "zb", "y", "x", "tp")
    )
    in_specs = (
        P(SEQ, "tp"), P(SEQ, "tp"), P(SEQ, None), P(SEQ, None), P(SEQ, "tp"), P("tp"), P("tp"),
        P(), P(), P("tp"), P(),
    )
    return jax.shard_map(
        body, mesh=finer, in_specs=in_specs, out_specs=P(SEQ, "tp"), check_vma=False
    )
```

```python
import functools

import jax
import jax.numpy as jnp
from jax import lax
from jax.experimental import pallas as pl
from jax.experimental.pallas import tpu as pltpu
from jax.sharding import Mesh
from jax.sharding import PartitionSpec as P

SEQ = ("za", "zb", "y", "x")
GROUP = ("zb", "y", "x")
OUTER = "za"
LANES = 128
epsilon = 1e-05
VMEM = pl.BlockSpec(memory_space=pltpu.VMEM)
HBM = pl.BlockSpec(memory_space=pltpu.HBM)


def call(
    kernel, outs, *args, hbm=0, after=(), scratch=(), flops=1_000_000, aliases=None, to_hbm=False
):
    if after:
        inner, skip = kernel, len(after)
        kernel = lambda *refs: inner(*refs[:len(args)], *refs[len(args) + skip:])
    multiple = isinstance(outs, (list, tuple))
    return pl.pallas_call(
        kernel,
        out_shape=list(outs) if multiple else outs,
        in_specs=[HBM] * hbm + [VMEM] * (len(args) - hbm) + [VMEM] * len(after),
        out_specs=[VMEM] * len(outs) if multiple else HBM if to_hbm else VMEM,
        input_output_aliases=aliases or {},
        scratch_shapes=list(scratch),
        compiler_params=pltpu.CompilerParams(vmem_limit_bytes=24 * 1024 * 1024),
        cost_estimate=pl.CostEstimate(flops=flops, bytes_accessed=1_000_000, transcendentals=0),
    )(*(pltpu.with_memory_space_constraint(a, pltpu.HBM) for a in args[:hbm]), *args[hbm:], *after)


def out(shape, dtype=jnp.float32):
    return pltpu.VMEM(shape, dtype)


def tile_of_heads(columns, tile, width):
    per, rows = LANES // width, columns.shape[0]
    lane = lax.broadcasted_iota(jnp.int32, (rows, LANES), 1)
    h = tile * per
    spread = jnp.broadcast_to(columns[:, h : h + 1], (rows, LANES))
    for k in range(1, per):
        other = jnp.broadcast_to(columns[:, h + k : h + k + 1], (rows, LANES))
        spread = jnp.where(lane < k * width, spread, other)
    return spread


def tails_kernel(b_ref, c_ref, tails_ref, sems):
    tokens, state = b_ref.shape
    copies = [
        pltpu.make_async_copy(
            r.at[pl.ds(tokens - 8, 8), :], tails_ref.at[:, pl.ds(k * state, state)], sems.at[k]
        )
        for k, r in enumerate((b_ref, c_ref))
    ]
    for copy in copies:
        copy.start()
    for copy in copies:
        copy.wait()


def convolve(padded_ref, weight, bias, relative, start):
    tokens = relative.shape[0]
    taps = weight.shape[0]
    summed = jnp.broadcast_to(bias, (tokens, bias.shape[1]))
    for k in range(taps):
        back = taps - 1 - k
        term = weight[k : k + 1, :] * padded_ref[8 - back : 8 - back + tokens, :]
        summed = summed + jnp.where(relative - back >= start, term, 0.0)
    return (summed * jax.nn.sigmoid(summed)).astype(jnp.bfloat16)


def bf16_parts(value):
    parts = []
    for _ in range(3):
        part = value.astype(jnp.bfloat16)
        parts.append(part)
        value = value - part.astype(jnp.float32)
    return parts


def spread_matrix(first, last, width, at):
    row = lax.broadcasted_iota(jnp.int32, (LANES, last - first), 0)
    head = (first + lax.broadcasted_iota(jnp.int32, (LANES, last - first), 1)) // width
    inside = (row >= at) if at else (row < 32)
    return jnp.where(inside & ((row & 31) == head), 1.0, 0.0).astype(jnp.bfloat16)


def spread_rows(values, features, heads, wide_ref):
    count = values.shape[0]
    parts = jnp.concatenate(bf16_parts(jnp.where(
        lax.broadcasted_iota(jnp.int32, values.shape, 1) < heads, values, 0.0
    )), axis=0)
    for j in range(0, features, 256):
        wide = jnp.dot(
            parts, spread_matrix(j, j + 256, features // heads, 0),
            preferred_element_type=jnp.float32,
        )
        wide_ref[:, j : j + 256] = (
            wide[2 * count :] + wide[count : 2 * count]
        ) + wide[0:count]


def sequence_index():
    index = 0
    for axis in SEQ:
        index = index * lax.axis_size(axis) + lax.axis_index(axis)
    return index


def to_column(row):
    n = row.shape[1]
    same = lax.broadcasted_iota(jnp.int32, (n, n), 0) == lax.broadcasted_iota(jnp.int32, (n, n), 1)
    return jnp.sum(jnp.where(same, jnp.broadcast_to(row, (n, n)), 0.0), axis=1, keepdims=True)


WEIGHTS_AT = 32


def prepare_kernel(*refs):
    count, held = 9, 4
    sources, x_ref = refs[:count], refs[count]
    kept = refs[count + 2 : 2 * count + 2 - held]
    (
        weighted_ref, cum_rows_ref, step_rows_ref, columns_ref, factor_ref, start_ref, b_conv_ref,
        stack_ref, padded_ref, sems, docs_ref, raw_ref, bias_ref, rate_ref,
    ) = refs[2 * count + 2 - held :]
    b_ref, taps_ref, taps_bias_ref, _, _ = kept
    copies = [
        pltpu.make_async_copy(source, target, sems.at[k])
        for k, (source, target) in enumerate(
            zip(sources, (docs_ref, raw_ref, bias_ref, rate_ref, *kept))
        )
    ]
    for copy in copies:
        copy.start()
    for copy in copies[:4]:
        copy.wait()
    heads, tokens = raw_ref.shape
    state = b_ref.shape[1]
    width = x_ref.shape[1] // heads
    base = sequence_index() * tokens
    relative = lax.broadcasted_iota(jnp.int32, (tokens, LANES), 0)
    start = jnp.zeros((1, 1), jnp.int32) - base
    last_position = jnp.full((1, 1), tokens - 1, jnp.int32)
    chosen = jnp.broadcast_to(start, relative.shape)
    end_start = start
    for i in range(1, docs_ref.shape[1]):
        start = start + docs_ref[0:1, i - 1 : i]
        chosen = jnp.where(start <= relative, start, chosen)
        end_start = jnp.where(start <= last_position, start, end_start)
    start_ref[...] = chosen

    step = jax.nn.softplus(raw_ref[...] + to_column(bias_ref[...]))
    log_decay = -step * to_column(rate_ref[...])
    rows = lax.broadcasted_iota(jnp.int32, (tokens, tokens), 0)
    cols = lax.broadcasted_iota(jnp.int32, (tokens, tokens), 1)
    upper = jnp.where(rows <= cols, 1.0, 0.0).astype(jnp.bfloat16)
    cum = sum(
        jnp.dot(part, upper, preferred_element_type=jnp.float32)
        for part in reversed(bf16_parts(log_decay))
    )
    cum_rows_ref[...] = cum
    step_rows_ref[...] = step
    position = lax.broadcasted_iota(jnp.int32, (heads, tokens), 1)
    weighting = jnp.where(
        position >= end_start, jnp.exp(cum[:, tokens - 1 : tokens] - cum) * step, 0.0
    )
    stack_ref[...] = jnp.zeros_like(stack_ref)
    stack_ref[0:heads, :] = cum
    for k, part in enumerate(bf16_parts(weighting)):
        at = WEIGHTS_AT * (k + 1)
        stack_ref[at : at + heads, :] = part.astype(jnp.float32)
    columns = stack_ref[...].T
    columns_ref[...] = columns
    factor_ref[...] = jnp.where(end_start < 0, jnp.exp(columns[tokens - 1 : tokens, :]), 0.0)
    for copy in copies[4:]:
        copy.wait()
    side = slice(0, state)
    padded_ref[0:8, :] = jnp.zeros((8, state), jnp.float32)
    padded_ref[8:, :] = b_ref[...].astype(jnp.float32)
    b_conv = convolve(padded_ref, taps_ref[:, side], taps_bias_ref[:, side], relative, chosen)
    b_conv_ref[...] = b_conv.astype(jnp.float32)
    weights = columns.astype(jnp.bfloat16)
    for j in range(0, x_ref.shape[1], 256):
        tile = slice(j, j + 256)
        spread = jnp.dot(
            weights, spread_matrix(j, j + 256, width, WEIGHTS_AT),
            preferred_element_type=jnp.float32,
        )
        weighted_ref[:, tile] = (x_ref[:, tile].astype(jnp.float32) * spread).astype(jnp.bfloat16)


def first_rows(source_ref, halo, weight, bias, start_ref, padded_ref):
    padded_ref[0:8, :] = halo.astype(jnp.float32)
    padded_ref[8:, :] = source_ref[0:8, :].astype(jnp.float32)
    relative = lax.broadcasted_iota(jnp.int32, (8, LANES), 0)
    return convolve(padded_ref, weight, bias, relative, start_ref[0:8, :])


def states_kernel(
    b_ref, halo_ref, taps_ref, taps_bias_ref, start_ref, b_early_ref, weighted_ref, factor_ref,
    pieces_ref, b_conv_ref, padded_ref,
):
    state, features = b_ref.shape[1], weighted_ref.shape[1]
    members, rows, _ = pieces_ref.shape
    first = first_rows(
        b_ref, halo_ref[:, 0:state], taps_ref[:, 0:state], taps_bias_ref[:, 0:state], start_ref,
        padded_ref,
    )
    b_conv = jnp.concatenate([first.astype(jnp.float32), b_early_ref[8:, :]], axis=0)
    b_conv_ref[...] = b_conv.astype(jnp.bfloat16)
    b_rows = b_conv.T.astype(jnp.bfloat16)
    for j in range(features // 256):
        tile = slice(j * 256, (j + 1) * 256)
        end_state = jnp.dot(b_rows, weighted_ref[:, tile], preferred_element_type=jnp.float32)
        for m in range(members):
            pieces_ref[m, :, tile] = end_state[m * rows : (m + 1) * rows, :]
    spread = jnp.broadcast_to(factor_ref[...], (rows, LANES))
    for m in range(members):
        pieces_ref[m, :, features:] = spread


def prefix_kernel(
    heads, pieces_ref, before_ref, factors_ref, total_a_ref, total_b_ref, total_c_ref, single_ref,
    wide_ref,
):
    members, rows, padded = pieces_ref.shape
    features = padded - LANES
    for m in range(members):
        single_ref[m : m + 1, :] = pieces_ref[m, 0:1, features:]
    spread_rows(single_ref[...], features, heads, wide_ref)
    product = jnp.ones((1, LANES), jnp.float32)
    for m in range(members):
        factors_ref[m : m + 1, :] = product
        product = product * single_ref[m : m + 1, :]
    total = jnp.zeros((rows, features), jnp.float32)
    for m in range(members):
        before_ref[m] = total
        total = wide_ref[m : m + 1, :] * total + pieces_ref[m, :, 0:features]
    for total_ref in (total_a_ref, total_b_ref, total_c_ref):
        total_ref[:, 0:features] = total
        total_ref[:, features:] = jnp.broadcast_to(product, (rows, LANES))


def wide_factor(pair_ref, features, width):
    factor = pair_ref[0:1, features:]
    return jnp.concatenate(
        [tile_of_heads(factor, j, width) for j in range(features // LANES)], axis=1
    )


def states_in_kernel(heads, *refs):
    *near_refs, far_ref, before_ref, wide_ref, state_ref, near_ref = refs
    members, _, features = before_ref.shape
    near_ref[...] = sum(ref[...] for ref in near_refs)
    factor = wide_factor(near_ref, features, features // heads)
    entering = factor * far_ref[:, 0:features] + near_ref[:, 0:features]
    for m in range(members):
        state_ref[m] = (wide_ref[m : m + 1, :] * entering + before_ref[m]).astype(jnp.bfloat16)


def products_of(
    c_ref, halo_ref, taps_ref, taps_bias_ref, start_ref, b_conv_ref, c_conv_ref, products_ref,
    padded_ref,
):
    tokens, state = c_ref.shape
    padded_ref[0:8, :] = halo_ref[:, state:].astype(jnp.float32)
    padded_ref[8:, :] = c_ref[...].astype(jnp.float32)
    relative = lax.broadcasted_iota(jnp.int32, (tokens, LANES), 0)
    c_conv = convolve(
        padded_ref, taps_ref[:, state:], taps_bias_ref[:, state:], relative, start_ref[...]
    )
    c_conv_ref[...] = c_conv
    products = lax.dot_general(
        c_conv, b_conv_ref[...], (((1,), (1,)), ((), ())), preferred_element_type=jnp.float32
    )
    row = lax.broadcasted_iota(jnp.int32, (tokens, tokens), 0)
    col = lax.broadcasted_iota(jnp.int32, (tokens, tokens), 1)
    starts = jnp.concatenate([start_ref[...]] * (tokens // LANES), axis=1)
    products_ref[...] = jnp.where((col <= row) & (col >= starts), products, 0.0)


def diagonal_of(
    start_ref, columns_ref, cum_rows_ref, step_rows_ref, x_ref, gate_ref, products_ref, gated_ref,
    scale_ref,
):
    tokens, features = x_ref.shape
    width, half = features // cum_rows_ref.shape[0], tokens // 2
    columns = columns_ref[...]
    carried = jnp.where(start_ref[...] < 0, jnp.exp(columns), 0.0)
    lane = lax.broadcasted_iota(jnp.int32, (tokens, LANES), 1)
    per = LANES // width
    for j in range(features // LANES):
        tile = slice(j * LANES, (j + 1) * LANES)
        diagonal = None
        for k in range(per):
            h = j * per + k
            column = jnp.broadcast_to(columns[:, h : h + 1], (tokens, LANES))
            cum_row, step_row = cum_rows_ref[h : h + 1, :], step_rows_ref[h : h + 1, :]
            upper = (
                products_ref[0:half, 0:half] * jnp.exp(column[0:half] - cum_row[:, 0:half])
            ) * step_row[:, 0:half]
            lower_left = (
                products_ref[half:, 0:half] * jnp.exp(column[half:] - cum_row[:, 0:half])
            ) * step_row[:, 0:half]
            lower_right = (
                products_ref[half:, half:] * jnp.exp(column[half:] - cum_row[:, half:])
            ) * step_row[:, half:]
            lower = jnp.concatenate([lower_left, lower_right], axis=1).astype(jnp.bfloat16)
            part = jnp.concatenate(
                [
                    jnp.dot(upper.astype(jnp.bfloat16), x_ref[0:half, tile],
                            preferred_element_type=jnp.float32),
                    jnp.dot(lower, x_ref[:, tile], preferred_element_type=jnp.float32),
                ],
                axis=0,
            )
            diagonal = part if diagonal is None else jnp.where(lane < k * width, diagonal, part)
        gate = gate_ref[:, tile].astype(jnp.float32)
        gate = gate * jax.nn.sigmoid(gate)
        gated_ref[:, tile] = diagonal * gate
        scale_ref[:, tile] = tile_of_heads(carried, j, width) * gate


def diagonal_kernel(turn, *refs):
    (*sources, columns_ref, cum_rows_ref, step_rows_ref, x_ref, gate_ref, factors_ref) = refs[:12]
    wide_ref, c_conv_ref, gated_ref, scale_ref, products_ref, padded_ref = refs[-6:]
    place = lax.axis_index(OUTER)

    @pl.when((place == 0, place == 1, place >= 2)[turn])
    def _():
        spread_rows(factors_ref[...], x_ref.shape[1], cum_rows_ref.shape[0], wide_ref)
        products_of(*sources, c_conv_ref, products_ref, padded_ref)
        diagonal_of(
            sources[4], columns_ref, cum_rows_ref, step_rows_ref, x_ref, gate_ref, products_ref,
            gated_ref, scale_ref,
        )


def gate_kernel(state_ref, c_conv_ref, diagonal_ref, scale_ref, gated_ref, squares_ref):
    members, rows, features = state_ref.shape
    c_conv = c_conv_ref[...]
    squares = jnp.zeros((c_conv.shape[0], LANES), jnp.float32)
    for j in range(features // LANES):
        tile = slice(j * LANES, (j + 1) * LANES)
        state = state_ref[:, :, tile].astype(jnp.float32).reshape(members * rows, LANES)
        carried = jnp.dot(c_conv, state.astype(jnp.bfloat16), preferred_element_type=jnp.float32)
        gated = diagonal_ref[:, tile] + scale_ref[:, tile] * carried
        gated_ref[:, tile] = gated
        squares = squares + gated * gated
    ones = jnp.ones((8, LANES), jnp.bfloat16)
    squares_ref[...] = sum(
        lax.dot_general(ones, part, (((1,), (1,)), ((), ())), preferred_element_type=jnp.float32)
        for part in reversed(bf16_parts(squares))
    )[0:1]


def normalize_kernel(features_all, squares_ref, gated_ref, gain_ref, out_ref, rows_ref, sems):
    count = squares_ref.shape[0]
    tokens, features = gated_ref.shape
    total = squares_ref[0]
    for k in range(1, count):
        total = total + squares_ref[k]
    scale = lax.rsqrt(total / features_all + epsilon)
    scale = jnp.broadcast_to(scale, (LANES, tokens)).T
    chunks = sems.shape[0]
    size = tokens // chunks
    copies = []
    for i in range(chunks):
        part = slice(i * size, (i + 1) * size)
        for j in range(features // LANES):
            tile = slice(j * LANES, (j + 1) * LANES)
            rows_ref[part, tile] = (
                gated_ref[part, tile] * scale[part] * gain_ref[j : j + 1, :]
            ).astype(jnp.bfloat16)
        copies.append(
            pltpu.make_async_copy(
                rows_ref.at[pl.ds(i * size, size), :], out_ref.at[pl.ds(i * size, size), :],
                sems.at[i],
            )
        )
        copies[-1].start()
    for copy in copies:
        copy.wait()


def body(
    inputs, gate_input, b_source, c_source, step_raw, step_bias, decay_rate, conv_weight,
    conv_bias, norm_gain, doc_lengths,
):
    tokens, features = inputs.shape
    heads = step_raw.shape[1]
    state = b_source.shape[1]
    members = 1
    for axis in GROUP:
        members *= lax.axis_size(axis)
    outer = lax.axis_size(OUTER)
    rows = state // members
    shards = members * outer
    ahead = lambda n, k: [(i, i + k) for i in range(n - k)]

    bf16 = jnp.bfloat16
    tails = call(
        tails_kernel, out((8, 2 * state), bf16), b_source, c_source,
        hbm=2, scratch=[pltpu.SemaphoreType.DMA((2,))], flops=20_000_000_000,
    )
    halo = lax.ppermute(tails, SEQ, ahead(shards, 1))
    operands = [
        doc_lengths[None, :], step_raw.T, step_bias[None, :], decay_rate[None, :], b_source,
        conv_weight, conv_bias[None, :], c_source, norm_gain.reshape(features // LANES, LANES),
    ]
    results = call(
        prepare_kernel,
        [out(o.shape, o.dtype) for o in operands[4:]]
        + [
            out((tokens, features), bf16), out((heads, tokens)), out((heads, tokens)),
            out((tokens, LANES)), out((1, LANES)), out((tokens, LANES), jnp.int32),
            out((tokens, state)),
        ],
        *operands, inputs, tails,
        hbm=len(operands),
        scratch=[
            pltpu.VMEM((LANES, tokens), jnp.float32),
            pltpu.VMEM((tokens + 8, state), jnp.float32),
            pltpu.SemaphoreType.DMA((len(operands),)),
            *(pltpu.VMEM(o.shape, o.dtype) for o in operands[:4]),
        ],
    )
    b, taps, taps_bias, c, gain = results[0:5]
    weighted, cum_rows, step_rows, columns, factor, start, b_early = results[5:]
    pieces, b_conv = call(
        states_kernel,
        [out((members, rows, features + LANES)), out((tokens, state), bf16)],
        b, halo, taps, taps_bias, start, b_early, weighted, factor,
        scratch=[pltpu.VMEM((16, state), jnp.float32)],
    )
    pieces = lax.all_to_all(pieces, GROUP, 0, 0)
    pair = out((rows, features + LANES))
    before, factors, total_a, total_b, total_c = call(
        functools.partial(prefix_kernel, heads),
        [out((members, rows, features)), out((members, LANES)), pair, pair, pair],
        pieces,
        scratch=[
            pltpu.VMEM((members, LANES), jnp.float32),
            pltpu.VMEM((members, features), jnp.float32),
        ],
    )

    def diagonal_terms(turn, token, *before):
        sources = [
            c, halo, taps, taps_bias, start, b_conv, columns, cum_rows, step_rows, inputs, gate_input,
            factors,
        ]
        token = [] if token is None else [token]
        count = len(sources)
        return call(
            functools.partial(diagonal_kernel, turn),
            [out(t.shape) for t in token] + [
                out((members, features)), out((tokens, state), bf16), out((tokens, features)),
                out((tokens, features)),
            ],
            *sources, *token, *before, flops=20_000_000_000,
            aliases={count + k: k for k in range(len(token) + len(before))},
            scratch=[
                pltpu.VMEM((tokens, tokens), jnp.float32),
                pltpu.VMEM((tokens + 8, state), jnp.float32),
            ],
        )

    def send(total, *pairs):
        return lax.ppermute(total, OUTER, pairs)

    total_a, *diagonal = diagonal_terms(0, total_a)
    near_a = send(total_a, (0, 1))
    total_b, *diagonal = diagonal_terms(1, total_b, *diagonal)
    far = send(total_b, (0, 2), (1, 3))
    near_b = send(total_c, (1, 2), (2, 3))
    wide, c_conv, diagonal, scale = diagonal_terms(2, None, *diagonal)
    states_in = call(
        functools.partial(states_in_kernel, heads),
        out((members, rows, features), bf16),
        near_a, near_b, far, before, wide,
        scratch=[pltpu.VMEM(pair.shape, jnp.float32)],
    )
    states_in = lax.all_to_all(states_in, GROUP, 0, 0)
    gated, squares = call(
        gate_kernel,
        [out((tokens, features)), out((1, tokens))],
        states_in, c_conv, diagonal, scale,
    )
    squares = lax.all_gather(squares, "tp")
    return call(
        functools.partial(normalize_kernel, features * lax.axis_size("tp")),
        jax.ShapeDtypeStruct((tokens, features), bf16),
        squares, gated, gain, to_hbm=True,
        scratch=[pltpu.VMEM((tokens, features), bf16), pltpu.SemaphoreType.DMA((4,))],
    )


def solution(mesh):
    finer = Mesh(
        mesh.devices.reshape(4, 2, 4, 4, mesh.shape["tp"]), ("za", "zb", "y", "x", "tp")
    )
    in_specs = (
        P(SEQ, "tp"), P(SEQ, "tp"), P(SEQ, None), P(SEQ, None), P(SEQ, "tp"), P("tp"), P("tp"),
        P(), P(), P("tp"), P(),
    )
    return jax.shard_map(
        body, mesh=finer, in_specs=in_specs, out_specs=P(SEQ, "tp"), check_vma=False
    )
```

```python
import functools

import jax
import jax.numpy as jnp
from jax import lax
from jax.experimental import pallas as pl
from jax.experimental.pallas import tpu as pltpu
from jax.sharding import Mesh
from jax.sharding import PartitionSpec as P

SEQ = ("za", "zb", "y", "x")
GROUP = ("zb", "y", "x")
OUTER = "za"
LANES = 128
epsilon = 1e-05
VMEM = pl.BlockSpec(memory_space=pltpu.VMEM)
HBM = pl.BlockSpec(memory_space=pltpu.HBM)


def call(
    kernel, outs, *args, hbm=0, after=(), scratch=(), flops=1_000_000, aliases=None, to_hbm=False
):
    if after:
        inner, skip = kernel, len(after)
        kernel = lambda *refs: inner(*refs[:len(args)], *refs[len(args) + skip:])
    multiple = isinstance(outs, (list, tuple))
    return pl.pallas_call(
        kernel,
        out_shape=list(outs) if multiple else outs,
        in_specs=[HBM] * hbm + [VMEM] * (len(args) - hbm) + [VMEM] * len(after),
        out_specs=[VMEM] * len(outs) if multiple else HBM if to_hbm else VMEM,
        input_output_aliases=aliases or {},
        scratch_shapes=list(scratch),
        compiler_params=pltpu.CompilerParams(vmem_limit_bytes=24 * 1024 * 1024),
        cost_estimate=pl.CostEstimate(flops=flops, bytes_accessed=1_000_000, transcendentals=0),
    )(*(pltpu.with_memory_space_constraint(a, pltpu.HBM) for a in args[:hbm]), *args[hbm:], *after)


def out(shape, dtype=jnp.float32):
    return pltpu.VMEM(shape, dtype)


def tile_of_heads(columns, tile, width):
    per, rows = LANES // width, columns.shape[0]
    lane = lax.broadcasted_iota(jnp.int32, (rows, LANES), 1)
    h = tile * per
    spread = jnp.broadcast_to(columns[:, h : h + 1], (rows, LANES))
    for k in range(1, per):
        other = jnp.broadcast_to(columns[:, h + k : h + k + 1], (rows, LANES))
        spread = jnp.where(lane < k * width, spread, other)
    return spread


def tails_kernel(b_ref, c_ref, *refs):
    count = (len(refs) - 2) // 2
    sources, tails_ref, targets, sems = refs[:count], refs[count], refs[count + 1 : -1], refs[-1]
    tokens, state = b_ref.shape
    copies = [
        pltpu.make_async_copy(
            r.at[pl.ds(tokens - 8, 8), :], tails_ref.at[:, pl.ds(k * state, state)], sems.at[k]
        )
        for k, r in enumerate((b_ref, c_ref))
    ]
    for k, (source, target) in enumerate(zip(sources, targets)):
        copies.append(pltpu.make_async_copy(source, target, sems.at[k + 2]))
    for copy in copies:
        copy.start()
    for copy in copies:
        copy.wait()


def convolve(padded_ref, weight, bias, relative, start):
    tokens = relative.shape[0]
    taps = weight.shape[0]
    summed = jnp.broadcast_to(bias, (tokens, bias.shape[1]))
    for k in range(taps):
        back = taps - 1 - k
        term = weight[k : k + 1, :] * padded_ref[8 - back : 8 - back + tokens, :]
        summed = summed + jnp.where(relative - back >= start, term, 0.0)
    return (summed * jax.nn.sigmoid(summed)).astype(jnp.bfloat16)


def bf16_parts(value):
    parts = []
    for _ in range(3):
        part = value.astype(jnp.bfloat16)
        parts.append(part)
        value = value - part.astype(jnp.float32)
    return parts


def spread_matrix(first, last, width, at):
    row = lax.broadcasted_iota(jnp.int32, (LANES, last - first), 0)
    head = (first + lax.broadcasted_iota(jnp.int32, (LANES, last - first), 1)) // width
    inside = (row >= at) if at else (row < 32)
    return jnp.where(inside & ((row & 31) == head), 1.0, 0.0).astype(jnp.bfloat16)


def spread_rows(values, features, heads, wide_ref):
    count = values.shape[0]
    parts = jnp.concatenate(bf16_parts(jnp.where(
        lax.broadcasted_iota(jnp.int32, values.shape, 1) < heads, values, 0.0
    )), axis=0)
    for j in range(0, features, 256):
        wide = jnp.dot(
            parts, spread_matrix(j, j + 256, features // heads, 0),
            preferred_element_type=jnp.float32,
        )
        wide_ref[:, j : j + 256] = (
            wide[2 * count :] + wide[count : 2 * count]
        ) + wide[0:count]


def sequence_index():
    index = 0
    for axis in SEQ:
        index = index * lax.axis_size(axis) + lax.axis_index(axis)
    return index


def to_column(row):
    n = row.shape[1]
    same = lax.broadcasted_iota(jnp.int32, (n, n), 0) == lax.broadcasted_iota(jnp.int32, (n, n), 1)
    return jnp.sum(jnp.where(same, jnp.broadcast_to(row, (n, n)), 0.0), axis=1, keepdims=True)


WEIGHTS_AT = 32


def prepare_kernel(*refs):
    count, given = 2, 9
    sources, targets = refs[:count], refs[count + given : 2 * count + given]
    (
        x_ref, docs_ref, raw_ref, bias_ref, rate_ref, b_ref, taps_ref, taps_bias_ref, _,
    ) = refs[count : count + given]
    (
        weighted_ref, cum_rows_ref, step_rows_ref, columns_ref, factor_ref, start_ref, b_conv_ref,
        stack_ref, padded_ref, sems,
    ) = refs[2 * count + given :]
    copies = [
        pltpu.make_async_copy(source, target, sems.at[k])
        for k, (source, target) in enumerate(zip(sources, targets))
    ]
    for copy in copies:
        copy.start()
    heads, tokens = raw_ref.shape
    state = b_ref.shape[1]
    width = x_ref.shape[1] // heads
    base = sequence_index() * tokens
    relative = lax.broadcasted_iota(jnp.int32, (tokens, LANES), 0)
    start = jnp.zeros((1, 1), jnp.int32) - base
    last_position = jnp.full((1, 1), tokens - 1, jnp.int32)
    chosen = jnp.broadcast_to(start, relative.shape)
    end_start = start
    for i in range(1, docs_ref.shape[1]):
        start = start + docs_ref[0:1, i - 1 : i]
        chosen = jnp.where(start <= relative, start, chosen)
        end_start = jnp.where(start <= last_position, start, end_start)
    start_ref[...] = chosen

    step = jax.nn.softplus(raw_ref[...] + to_column(bias_ref[...]))
    log_decay = -step * to_column(rate_ref[...])
    rows = lax.broadcasted_iota(jnp.int32, (tokens, tokens), 0)
    cols = lax.broadcasted_iota(jnp.int32, (tokens, tokens), 1)
    upper = jnp.where(rows <= cols, 1.0, 0.0).astype(jnp.bfloat16)
    cum = sum(
        jnp.dot(part, upper, preferred_element_type=jnp.float32)
        for part in reversed(bf16_parts(log_decay))
    )
    cum_rows_ref[...] = cum
    step_rows_ref[...] = step
    position = lax.broadcasted_iota(jnp.int32, (heads, tokens), 1)
    weighting = jnp.where(
        position >= end_start, jnp.exp(cum[:, tokens - 1 : tokens] - cum) * step, 0.0
    )
    stack_ref[...] = jnp.zeros_like(stack_ref)
    stack_ref[0:heads, :] = cum
    for k, part in enumerate(bf16_parts(weighting)):
        at = WEIGHTS_AT * (k + 1)
        stack_ref[at : at + heads, :] = part.astype(jnp.float32)
    columns = stack_ref[...].T
    columns_ref[...] = columns
    factor_ref[...] = jnp.where(end_start < 0, jnp.exp(columns[tokens - 1 : tokens, :]), 0.0)
    side = slice(0, state)
    padded_ref[0:8, :] = jnp.zeros((8, state), jnp.float32)
    padded_ref[8:, :] = b_ref[...].astype(jnp.float32)
    b_conv = convolve(padded_ref, taps_ref[:, side], taps_bias_ref[:, side], relative, chosen)
    b_conv_ref[...] = b_conv.astype(jnp.float32)
    weights = columns.astype(jnp.bfloat16)
    for j in range(0, x_ref.shape[1], 256):
        tile = slice(j, j + 256)
        spread = jnp.dot(
            weights, spread_matrix(j, j + 256, width, WEIGHTS_AT),
            preferred_element_type=jnp.float32,
        )
        weighted_ref[:, tile] = (x_ref[:, tile].astype(jnp.float32) * spread).astype(jnp.bfloat16)
    for copy in copies:
        copy.wait()


def first_rows(source_ref, halo, weight, bias, start_ref, padded_ref):
    padded_ref[0:8, :] = halo.astype(jnp.float32)
    padded_ref[8:, :] = source_ref[0:8, :].astype(jnp.float32)
    relative = lax.broadcasted_iota(jnp.int32, (8, LANES), 0)
    return convolve(padded_ref, weight, bias, relative, start_ref[0:8, :])


def states_kernel(
    b_ref, halo_ref, taps_ref, taps_bias_ref, start_ref, b_early_ref, weighted_ref, factor_ref,
    pieces_ref, b_conv_ref, padded_ref,
):
    state, features = b_ref.shape[1], weighted_ref.shape[1]
    members, rows, _ = pieces_ref.shape
    first = first_rows(
        b_ref, halo_ref[:, 0:state], taps_ref[:, 0:state], taps_bias_ref[:, 0:state], start_ref,
        padded_ref,
    )
    b_conv = jnp.concatenate([first.astype(jnp.float32), b_early_ref[8:, :]], axis=0)
    b_conv_ref[...] = b_conv.astype(jnp.bfloat16)
    b_rows = b_conv.T.astype(jnp.bfloat16)
    for j in range(features // 256):
        tile = slice(j * 256, (j + 1) * 256)
        end_state = jnp.dot(b_rows, weighted_ref[:, tile], preferred_element_type=jnp.float32)
        for m in range(members):
            pieces_ref[m, :, tile] = end_state[m * rows : (m + 1) * rows, :]
    spread = jnp.broadcast_to(factor_ref[...], (rows, LANES))
    for m in range(members):
        pieces_ref[m, :, features:] = spread


def prefix_kernel(
    heads, pieces_ref, before_ref, factors_ref, total_a_ref, total_b_ref, total_c_ref, single_ref,
    wide_ref,
):
    members, rows, padded = pieces_ref.shape
    features = padded - LANES
    for m in range(members):
        single_ref[m : m + 1, :] = pieces_ref[m, 0:1, features:]
    spread_rows(single_ref[...], features, heads, wide_ref)
    product = jnp.ones((1, LANES), jnp.float32)
    for m in range(members):
        factors_ref[m : m + 1, :] = product
        product = product * single_ref[m : m + 1, :]
    total = jnp.zeros((rows, features), jnp.float32)
    for m in range(members):
        before_ref[m] = total
        total = wide_ref[m : m + 1, :] * total + pieces_ref[m, :, 0:features]
    for total_ref in (total_a_ref, total_b_ref, total_c_ref):
        total_ref[:, 0:features] = total
        total_ref[:, features:] = jnp.broadcast_to(product, (rows, LANES))


def wide_factor(pair_ref, features, width):
    factor = pair_ref[0:1, features:]
    return jnp.concatenate(
        [tile_of_heads(factor, j, width) for j in range(features // LANES)], axis=1
    )


def states_in_kernel(heads, *refs):
    sent_near_ref, sent_far_ref, mixed_ref, before_ref, wide_ref, state_ref, near_ref = refs
    members, _, features = before_ref.shape
    second = lax.axis_index(OUTER) == 1
    mixed = mixed_ref[...]
    near_ref[...] = sent_near_ref[...] + jnp.where(second, mixed, 0.0)
    far = sent_far_ref[:, 0:features] + jnp.where(second, 0.0, mixed[:, 0:features])
    factor = wide_factor(near_ref, features, features // heads)
    entering = factor * far + near_ref[:, 0:features]
    for m in range(members):
        state_ref[m] = (wide_ref[m : m + 1, :] * entering + before_ref[m]).astype(jnp.bfloat16)


def products_of(
    c_ref, halo_ref, taps_ref, taps_bias_ref, start_ref, b_conv_ref, c_conv_ref, products_ref,
    padded_ref,
):
    tokens, state = c_ref.shape
    padded_ref[0:8, :] = halo_ref[:, state:].astype(jnp.float32)
    padded_ref[8:, :] = c_ref[...].astype(jnp.float32)
    relative = lax.broadcasted_iota(jnp.int32, (tokens, LANES), 0)
    c_conv = convolve(
        padded_ref, taps_ref[:, state:], taps_bias_ref[:, state:], relative, start_ref[...]
    )
    c_conv_ref[...] = c_conv
    products = lax.dot_general(
        c_conv, b_conv_ref[...], (((1,), (1,)), ((), ())), preferred_element_type=jnp.float32
    )
    row = lax.broadcasted_iota(jnp.int32, (tokens, tokens), 0)
    col = lax.broadcasted_iota(jnp.int32, (tokens, tokens), 1)
    starts = jnp.concatenate([start_ref[...]] * (tokens // LANES), axis=1)
    products_ref[...] = jnp.where((col <= row) & (col >= starts), products, 0.0)


def diagonal_of(
    start_ref, columns_ref, cum_rows_ref, step_rows_ref, x_ref, gate_ref, products_ref, gated_ref,
    scale_ref,
):
    tokens, features = x_ref.shape
    width, half = features // cum_rows_ref.shape[0], tokens // 2
    columns = columns_ref[...]
    carried = jnp.where(start_ref[...] < 0, jnp.exp(columns), 0.0)
    lane = lax.broadcasted_iota(jnp.int32, (tokens, LANES), 1)
    per = LANES // width
    for j in range(features // LANES):
        tile = slice(j * LANES, (j + 1) * LANES)
        diagonal = None
        for k in range(per):
            h = j * per + k
            column = jnp.broadcast_to(columns[:, h : h + 1], (tokens, LANES))
            cum_row, step_row = cum_rows_ref[h : h + 1, :], step_rows_ref[h : h + 1, :]
            upper = (
                products_ref[0:half, 0:half] * jnp.exp(column[0:half] - cum_row[:, 0:half])
            ) * step_row[:, 0:half]
            lower_left = (
                products_ref[half:, 0:half] * jnp.exp(column[half:] - cum_row[:, 0:half])
            ) * step_row[:, 0:half]
            lower_right = (
                products_ref[half:, half:] * jnp.exp(column[half:] - cum_row[:, half:])
            ) * step_row[:, half:]
            lower = jnp.concatenate([lower_left, lower_right], axis=1).astype(jnp.bfloat16)
            part = jnp.concatenate(
                [
                    jnp.dot(upper.astype(jnp.bfloat16), x_ref[0:half, tile],
                            preferred_element_type=jnp.float32),
                    jnp.dot(lower, x_ref[:, tile], preferred_element_type=jnp.float32),
                ],
                axis=0,
            )
            diagonal = part if diagonal is None else jnp.where(lane < k * width, diagonal, part)
        gate = gate_ref[:, tile].astype(jnp.float32)
        gate = gate * jax.nn.sigmoid(gate)
        gated_ref[:, tile] = diagonal * gate
        scale_ref[:, tile] = tile_of_heads(carried, j, width) * gate


def diagonal_kernel(turn, *refs):
    (*sources, columns_ref, cum_rows_ref, step_rows_ref, x_ref, gate_ref, factors_ref) = refs[:12]
    wide_ref, c_conv_ref, gated_ref, scale_ref, products_ref, padded_ref = refs[-6:]
    place = lax.axis_index(OUTER)

    @pl.when((place == 0, place == 1, place >= 2)[turn])
    def _():
        spread_rows(factors_ref[...], x_ref.shape[1], cum_rows_ref.shape[0], wide_ref)
        products_of(*sources, c_conv_ref, products_ref, padded_ref)
        diagonal_of(
            sources[4], columns_ref, cum_rows_ref, step_rows_ref, x_ref, gate_ref, products_ref,
            gated_ref, scale_ref,
        )


def gate_kernel(state_ref, c_conv_ref, diagonal_ref, scale_ref, gated_ref, squares_ref):
    members, rows, features = state_ref.shape
    c_conv = c_conv_ref[...]
    squares = jnp.zeros((c_conv.shape[0], LANES), jnp.float32)
    for j in range(features // LANES):
        tile = slice(j * LANES, (j + 1) * LANES)
        state = state_ref[:, :, tile].astype(jnp.float32).reshape(members * rows, LANES)
        carried = jnp.dot(c_conv, state.astype(jnp.bfloat16), preferred_element_type=jnp.float32)
        gated = diagonal_ref[:, tile] + scale_ref[:, tile] * carried
        gated_ref[:, tile] = gated
        squares = squares + gated * gated
    ones = jnp.ones((8, LANES), jnp.bfloat16)
    squares_ref[...] = sum(
        lax.dot_general(ones, part, (((1,), (1,)), ((), ())), preferred_element_type=jnp.float32)
        for part in reversed(bf16_parts(squares))
    )[0:1]


def normalize_kernel(features_all, squares_ref, gated_ref, gain_ref, out_ref, rows_ref, sems):
    count = squares_ref.shape[0]
    tokens, features = gated_ref.shape
    total = squares_ref[0]
    for k in range(1, count):
        total = total + squares_ref[k]
    scale = lax.rsqrt(total / features_all + epsilon)
    scale = jnp.broadcast_to(scale, (LANES, tokens)).T
    chunks = sems.shape[0]
    size = tokens // chunks
    copies = []
    for i in range(chunks):
        part = slice(i * size, (i + 1) * size)
        for j in range(features // LANES):
            tile = slice(j * LANES, (j + 1) * LANES)
            rows_ref[part, tile] = (
                gated_ref[part, tile] * scale[part] * gain_ref[j : j + 1, :]
            ).astype(jnp.bfloat16)
        copies.append(
            pltpu.make_async_copy(
                rows_ref.at[pl.ds(i * size, size), :], out_ref.at[pl.ds(i * size, size), :],
                sems.at[i],
            )
        )
        copies[-1].start()
    for copy in copies:
        copy.wait()


def body(
    inputs, gate_input, b_source, c_source, step_raw, step_bias, decay_rate, conv_weight,
    conv_bias, norm_gain, doc_lengths,
):
    tokens, features = inputs.shape
    heads = step_raw.shape[1]
    state = b_source.shape[1]
    members = 1
    for axis in GROUP:
        members *= lax.axis_size(axis)
    outer = lax.axis_size(OUTER)
    rows = state // members
    shards = members * outer
    ahead = lambda n, k: [(i, i + k) for i in range(n - k)]

    bf16 = jnp.bfloat16
    small = [
        doc_lengths[None, :], step_raw.T, step_bias[None, :], decay_rate[None, :], b_source,
        conv_weight, conv_bias[None, :],
    ]
    tails, *small = call(
        tails_kernel,
        [out((8, 2 * state), bf16)] + [out(o.shape, o.dtype) for o in small],
        b_source, c_source, *small,
        hbm=2 + len(small), scratch=[pltpu.SemaphoreType.DMA((2 + len(small),))],
        flops=20_000_000_000,
    )
    halo = lax.ppermute(tails, SEQ, ahead(shards, 1))
    operands = [
        c_source, norm_gain.reshape(features // LANES, LANES),
    ]
    results = call(
        prepare_kernel,
        [out(o.shape, o.dtype) for o in operands]
        + [
            out((tokens, features), bf16), out((heads, tokens)), out((heads, tokens)),
            out((tokens, LANES)), out((1, LANES)), out((tokens, LANES), jnp.int32),
            out((tokens, state)),
        ],
        *operands, inputs, *small, tails,
        hbm=len(operands),
        scratch=[
            pltpu.VMEM((LANES, tokens), jnp.float32),
            pltpu.VMEM((tokens + 8, state), jnp.float32),
            pltpu.SemaphoreType.DMA((len(operands),)),
        ],
    )
    b, taps, taps_bias = small[4:]
    c, gain = results[0:2]
    weighted, cum_rows, step_rows, columns, factor, start, b_early = results[2:]
    pieces, b_conv = call(
        states_kernel,
        [out((members, rows, features + LANES)), out((tokens, state), bf16)],
        b, halo, taps, taps_bias, start, b_early, weighted, factor,
        scratch=[pltpu.VMEM((16, state), jnp.float32)],
    )
    pieces = lax.all_to_all(pieces, GROUP, 0, 0)
    pair = out((rows, features + LANES))
    before, factors, total_a, total_b, total_c = call(
        functools.partial(prefix_kernel, heads),
        [out((members, rows, features)), out((members, LANES)), pair, pair, pair],
        pieces,
        scratch=[
            pltpu.VMEM((members, LANES), jnp.float32),
            pltpu.VMEM((members, features), jnp.float32),
        ],
    )

    def diagonal_terms(turn, token, *before):
        sources = [
            c, halo, taps, taps_bias, start, b_conv, columns, cum_rows, step_rows, inputs, gate_input,
            factors,
        ]
        token = [] if token is None else [token]
        count = len(sources)
        return call(
            functools.partial(diagonal_kernel, turn),
            [out(t.shape) for t in token] + [
                out((members, features)), out((tokens, state), bf16), out((tokens, features)),
                out((tokens, features)),
            ],
            *sources, *token, *before, flops=20_000_000_000,
            aliases={count + k: k for k in range(len(token) + len(before))},
            scratch=[
                pltpu.VMEM((tokens, tokens), jnp.float32),
                pltpu.VMEM((tokens + 8, state), jnp.float32),
            ],
        )

    def send(total, *pairs):
        return lax.ppermute(total, OUTER, pairs)

    total_a, *diagonal = diagonal_terms(0, total_a)
    far = send(total_a, (0, 2))
    total_b, *diagonal = diagonal_terms(1, total_b, *diagonal)
    mixed = send(total_b, (0, 1), (1, 3))
    near = send(total_c, (1, 2), (2, 3))
    wide, c_conv, diagonal, scale = diagonal_terms(2, None, *diagonal)
    states_in = call(
        functools.partial(states_in_kernel, heads),
        out((members, rows, features), bf16),
        near, far, mixed, before, wide,
        scratch=[pltpu.VMEM(pair.shape, jnp.float32)],
    )
    states_in = lax.all_to_all(states_in, GROUP, 0, 0)
    gated, squares = call(
        gate_kernel,
        [out((tokens, features)), out((1, tokens))],
        states_in, c_conv, diagonal, scale,
    )
    squares = lax.all_gather(squares, "tp")
    return call(
        functools.partial(normalize_kernel, features * lax.axis_size("tp")),
        jax.ShapeDtypeStruct((tokens, features), bf16),
        squares, gated, gain, to_hbm=True,
        scratch=[pltpu.VMEM((tokens, features), bf16), pltpu.SemaphoreType.DMA((4,))],
    )


def solution(mesh):
    finer = Mesh(
        mesh.devices.reshape(4, 2, 4, 4, mesh.shape["tp"]), ("za", "zb", "y", "x", "tp")
    )
    in_specs = (
        P(SEQ, "tp"), P(SEQ, "tp"), P(SEQ, None), P(SEQ, None), P(SEQ, "tp"), P("tp"), P("tp"),
        P(), P(), P("tp"), P(),
    )
    return jax.shard_map(
        body, mesh=finer, in_specs=in_specs, out_specs=P(SEQ, "tp"), check_vma=False
    )
```

```python
import functools

import jax
import jax.numpy as jnp
from jax import lax
from jax.experimental import pallas as pl
from jax.experimental.pallas import tpu as pltpu
from jax.sharding import Mesh
from jax.sharding import PartitionSpec as P

SEQ = ("za", "zb", "y", "x")
GROUP = ("zb", "y", "x")
OUTER = "za"
LANES = 128
epsilon = 1e-05
VMEM = pl.BlockSpec(memory_space=pltpu.VMEM)
HBM = pl.BlockSpec(memory_space=pltpu.HBM)


def call(
    kernel, outs, *args, hbm=0, after=(), scratch=(), flops=1_000_000, aliases=None, to_hbm=False
):
    if after:
        inner, skip = kernel, len(after)
        kernel = lambda *refs: inner(*refs[:len(args)], *refs[len(args) + skip:])
    multiple = isinstance(outs, (list, tuple))
    return pl.pallas_call(
        kernel,
        out_shape=list(outs) if multiple else outs,
        in_specs=[HBM] * hbm + [VMEM] * (len(args) - hbm) + [VMEM] * len(after),
        out_specs=[VMEM] * len(outs) if multiple else HBM if to_hbm else VMEM,
        input_output_aliases=aliases or {},
        scratch_shapes=list(scratch),
        compiler_params=pltpu.CompilerParams(vmem_limit_bytes=24 * 1024 * 1024),
        cost_estimate=pl.CostEstimate(flops=flops, bytes_accessed=1_000_000, transcendentals=0),
    )(*(pltpu.with_memory_space_constraint(a, pltpu.HBM) for a in args[:hbm]), *args[hbm:], *after)


def out(shape, dtype=jnp.float32):
    return pltpu.VMEM(shape, dtype)


def tile_of_heads(columns, tile, width):
    per, rows = LANES // width, columns.shape[0]
    lane = lax.broadcasted_iota(jnp.int32, (rows, LANES), 1)
    h = tile * per
    spread = jnp.broadcast_to(columns[:, h : h + 1], (rows, LANES))
    for k in range(1, per):
        other = jnp.broadcast_to(columns[:, h + k : h + k + 1], (rows, LANES))
        spread = jnp.where(lane < k * width, spread, other)
    return spread


def tails_kernel(b_ref, c_ref, *refs):
    count = (len(refs) - 2) // 2
    sources, tails_ref, targets, sems = refs[:count], refs[count], refs[count + 1 : -1], refs[-1]
    tokens, state = b_ref.shape
    copies = [
        pltpu.make_async_copy(
            r.at[pl.ds(tokens - 8, 8), :], tails_ref.at[:, pl.ds(k * state, state)], sems.at[k]
        )
        for k, r in enumerate((b_ref, c_ref))
    ]
    for k, (source, target) in enumerate(zip(sources, targets)):
        copies.append(pltpu.make_async_copy(source, target, sems.at[k + 2]))
    for k, copy in enumerate(copies):
        copy.start(priority=1 if k < 2 else 0)
    for copy in copies:
        copy.wait()


def convolve(padded_ref, weight, bias, relative, start):
    tokens = relative.shape[0]
    taps = weight.shape[0]
    summed = jnp.broadcast_to(bias, (tokens, bias.shape[1]))
    for k in range(taps):
        back = taps - 1 - k
        term = weight[k : k + 1, :] * padded_ref[8 - back : 8 - back + tokens, :]
        summed = summed + jnp.where(relative - back >= start, term, 0.0)
    return (summed * jax.nn.sigmoid(summed)).astype(jnp.bfloat16)


def bf16_parts(value):
    parts = []
    for _ in range(3):
        part = value.astype(jnp.bfloat16)
        parts.append(part)
        value = value - part.astype(jnp.float32)
    return parts


def spread_matrix(first, last, width, at):
    row = lax.broadcasted_iota(jnp.int32, (LANES, last - first), 0)
    head = (first + lax.broadcasted_iota(jnp.int32, (LANES, last - first), 1)) // width
    inside = (row >= at) if at else (row < 32)
    return jnp.where(inside & ((row & 31) == head), 1.0, 0.0).astype(jnp.bfloat16)


def spread_rows(values, features, heads, wide_ref):
    count = values.shape[0]
    parts = jnp.concatenate(bf16_parts(jnp.where(
        lax.broadcasted_iota(jnp.int32, values.shape, 1) < heads, values, 0.0
    )), axis=0)
    for j in range(0, features, 256):
        wide = jnp.dot(
            parts, spread_matrix(j, j + 256, features // heads, 0),
            preferred_element_type=jnp.float32,
        )
        wide_ref[:, j : j + 256] = (
            wide[2 * count :] + wide[count : 2 * count]
        ) + wide[0:count]


def sequence_index():
    index = 0
    for axis in SEQ:
        index = index * lax.axis_size(axis) + lax.axis_index(axis)
    return index


def to_column(row):
    n = row.shape[1]
    same = lax.broadcasted_iota(jnp.int32, (n, n), 0) == lax.broadcasted_iota(jnp.int32, (n, n), 1)
    return jnp.sum(jnp.where(same, jnp.broadcast_to(row, (n, n)), 0.0), axis=1, keepdims=True)


WEIGHTS_AT = 32


def prepare_kernel(*refs):
    count, given = 2, 9
    sources, targets = refs[:count], refs[count + given : 2 * count + given]
    (
        x_ref, docs_ref, raw_ref, bias_ref, rate_ref, b_ref, taps_ref, taps_bias_ref, _,
    ) = refs[count : count + given]
    (
        weighted_ref, cum_rows_ref, step_rows_ref, columns_ref, factor_ref, start_ref, b_conv_ref,
        stack_ref, padded_ref, sems,
    ) = refs[2 * count + given :]
    copies = [
        pltpu.make_async_copy(source, target, sems.at[k])
        for k, (source, target) in enumerate(zip(sources, targets))
    ]
    for copy in copies:
        copy.start()
    heads, tokens = raw_ref.shape
    state = b_ref.shape[1]
    width = x_ref.shape[1] // heads
    base = sequence_index() * tokens
    relative = lax.broadcasted_iota(jnp.int32, (tokens, LANES), 0)
    start = jnp.zeros((1, 1), jnp.int32) - base
    last_position = jnp.full((1, 1), tokens - 1, jnp.int32)
    chosen = jnp.broadcast_to(start, relative.shape)
    end_start = start
    for i in range(1, docs_ref.shape[1]):
        start = start + docs_ref[0:1, i - 1 : i]
        chosen = jnp.where(start <= relative, start, chosen)
        end_start = jnp.where(start <= last_position, start, end_start)
    start_ref[...] = chosen

    step = jax.nn.softplus(raw_ref[...] + to_column(bias_ref[...]))
    log_decay = -step * to_column(rate_ref[...])
    rows = lax.broadcasted_iota(jnp.int32, (tokens, tokens), 0)
    cols = lax.broadcasted_iota(jnp.int32, (tokens, tokens), 1)
    upper = jnp.where(rows <= cols, 1.0, 0.0).astype(jnp.bfloat16)
    cum = sum(
        jnp.dot(part, upper, preferred_element_type=jnp.float32)
        for part in reversed(bf16_parts(log_decay))
    )
    cum_rows_ref[...] = cum
    step_rows_ref[...] = step
    position = lax.broadcasted_iota(jnp.int32, (heads, tokens), 1)
    weighting = jnp.where(
        position >= end_start, jnp.exp(cum[:, tokens - 1 : tokens] - cum) * step, 0.0
    )
    stack_ref[...] = jnp.zeros_like(stack_ref)
    stack_ref[0:heads, :] = cum
    for k, part in enumerate(bf16_parts(weighting)):
        at = WEIGHTS_AT * (k + 1)
        stack_ref[at : at + heads, :] = part.astype(jnp.float32)
    columns = stack_ref[...].T
    columns_ref[...] = columns
    factor_ref[...] = jnp.where(end_start < 0, jnp.exp(columns[tokens - 1 : tokens, :]), 0.0)
    side = slice(0, state)
    padded_ref[0:8, :] = jnp.zeros((8, state), jnp.float32)
    padded_ref[8:, :] = b_ref[...].astype(jnp.float32)
    b_conv = convolve(padded_ref, taps_ref[:, side], taps_bias_ref[:, side], relative, chosen)
    b_conv_ref[...] = b_conv.astype(jnp.float32)
    weights = columns.astype(jnp.bfloat16)
    for j in range(0, x_ref.shape[1], 256):
        tile = slice(j, j + 256)
        spread = jnp.dot(
            weights, spread_matrix(j, j + 256, width, WEIGHTS_AT),
            preferred_element_type=jnp.float32,
        )
        weighted_ref[:, tile] = (x_ref[:, tile].astype(jnp.float32) * spread).astype(jnp.bfloat16)
    for copy in copies:
        copy.wait()


def first_rows(source_ref, halo, weight, bias, start_ref, padded_ref):
    padded_ref[0:8, :] = halo.astype(jnp.float32)
    padded_ref[8:, :] = source_ref[0:8, :].astype(jnp.float32)
    relative = lax.broadcasted_iota(jnp.int32, (8, LANES), 0)
    return convolve(padded_ref, weight, bias, relative, start_ref[0:8, :])


def states_kernel(
    b_ref, halo_ref, taps_ref, taps_bias_ref, start_ref, b_early_ref, weighted_ref, factor_ref,
    pieces_ref, b_conv_ref, padded_ref,
):
    state, features = b_ref.shape[1], weighted_ref.shape[1]
    members, rows, _ = pieces_ref.shape
    first = first_rows(
        b_ref, halo_ref[:, 0:state], taps_ref[:, 0:state], taps_bias_ref[:, 0:state], start_ref,
        padded_ref,
    )
    b_conv = jnp.concatenate([first.astype(jnp.float32), b_early_ref[8:, :]], axis=0)
    b_conv_ref[...] = b_conv.astype(jnp.bfloat16)
    b_rows = b_conv.T.astype(jnp.bfloat16)
    for j in range(features // 256):
        tile = slice(j * 256, (j + 1) * 256)
        end_state = jnp.dot(b_rows, weighted_ref[:, tile], preferred_element_type=jnp.float32)
        for m in range(members):
            pieces_ref[m, :, tile] = end_state[m * rows : (m + 1) * rows, :]
    spread = jnp.broadcast_to(factor_ref[...], (rows, LANES))
    for m in range(members):
        pieces_ref[m, :, features:] = spread


def prefix_kernel(
    heads, pieces_ref, before_ref, factors_ref, total_a_ref, total_b_ref, total_c_ref, single_ref,
    wide_ref,
):
    members, rows, padded = pieces_ref.shape
    features = padded - LANES
    for m in range(members):
        single_ref[m : m + 1, :] = pieces_ref[m, 0:1, features:]
    spread_rows(single_ref[...], features, heads, wide_ref)
    product = jnp.ones((1, LANES), jnp.float32)
    for m in range(members):
        factors_ref[m : m + 1, :] = product
        product = product * single_ref[m : m + 1, :]
    total = jnp.zeros((rows, features), jnp.float32)
    for m in range(members):
        before_ref[m] = total
        total = wide_ref[m : m + 1, :] * total + pieces_ref[m, :, 0:features]
    for total_ref in (total_a_ref, total_b_ref, total_c_ref):
        total_ref[:, 0:features] = total
        total_ref[:, features:] = jnp.broadcast_to(product, (rows, LANES))


def wide_factor(pair_ref, features, width):
    factor = pair_ref[0:1, features:]
    return jnp.concatenate(
        [tile_of_heads(factor, j, width) for j in range(features // LANES)], axis=1
    )


def states_in_kernel(heads, *refs):
    *near_refs, far_ref, before_ref, wide_ref, state_ref, near_ref = refs
    members, _, features = before_ref.shape
    near_ref[...] = sum(ref[...] for ref in near_refs)
    factor = wide_factor(near_ref, features, features // heads)
    entering = factor * far_ref[:, 0:features] + near_ref[:, 0:features]
    for m in range(members):
        state_ref[m] = (wide_ref[m : m + 1, :] * entering + before_ref[m]).astype(jnp.bfloat16)


def products_of(
    c_ref, halo_ref, taps_ref, taps_bias_ref, start_ref, b_conv_ref, c_conv_ref, products_ref,
    padded_ref,
):
    tokens, state = c_ref.shape
    padded_ref[0:8, :] = halo_ref[:, state:].astype(jnp.float32)
    padded_ref[8:, :] = c_ref[...].astype(jnp.float32)
    relative = lax.broadcasted_iota(jnp.int32, (tokens, LANES), 0)
    c_conv = convolve(
        padded_ref, taps_ref[:, state:], taps_bias_ref[:, state:], relative, start_ref[...]
    )
    c_conv_ref[...] = c_conv
    products = lax.dot_general(
        c_conv, b_conv_ref[...], (((1,), (1,)), ((), ())), preferred_element_type=jnp.float32
    )
    row = lax.broadcasted_iota(jnp.int32, (tokens, tokens), 0)
    col = lax.broadcasted_iota(jnp.int32, (tokens, tokens), 1)
    starts = jnp.concatenate([start_ref[...]] * (tokens // LANES), axis=1)
    products_ref[...] = jnp.where((col <= row) & (col >= starts), products, 0.0)


def diagonal_of(
    start_ref, columns_ref, cum_rows_ref, step_rows_ref, x_ref, gate_ref, products_ref, gated_ref,
    scale_ref,
):
    tokens, features = x_ref.shape
    width, half = features // cum_rows_ref.shape[0], tokens // 2
    columns = columns_ref[...]
    carried = jnp.where(start_ref[...] < 0, jnp.exp(columns), 0.0)
    lane = lax.broadcasted_iota(jnp.int32, (tokens, LANES), 1)
    per = LANES // width
    for j in range(features // LANES):
        tile = slice(j * LANES, (j + 1) * LANES)
        diagonal = None
        for k in range(per):
            h = j * per + k
            column = jnp.broadcast_to(columns[:, h : h + 1], (tokens, LANES))
            cum_row, step_row = cum_rows_ref[h : h + 1, :], step_rows_ref[h : h + 1, :]
            upper = (
                products_ref[0:half, 0:half] * jnp.exp(column[0:half] - cum_row[:, 0:half])
            ) * step_row[:, 0:half]
            lower_left = (
                products_ref[half:, 0:half] * jnp.exp(column[half:] - cum_row[:, 0:half])
            ) * step_row[:, 0:half]
            lower_right = (
                products_ref[half:, half:] * jnp.exp(column[half:] - cum_row[:, half:])
            ) * step_row[:, half:]
            lower = jnp.concatenate([lower_left, lower_right], axis=1).astype(jnp.bfloat16)
            part = jnp.concatenate(
                [
                    jnp.dot(upper.astype(jnp.bfloat16), x_ref[0:half, tile],
                            preferred_element_type=jnp.float32),
                    jnp.dot(lower, x_ref[:, tile], preferred_element_type=jnp.float32),
                ],
                axis=0,
            )
            diagonal = part if diagonal is None else jnp.where(lane < k * width, diagonal, part)
        gate = gate_ref[:, tile].astype(jnp.float32)
        gate = gate * jax.nn.sigmoid(gate)
        gated_ref[:, tile] = diagonal * gate
        scale_ref[:, tile] = tile_of_heads(carried, j, width) * gate


def diagonal_kernel(turn, *refs):
    (*sources, columns_ref, cum_rows_ref, step_rows_ref, x_ref, gate_ref, factors_ref) = refs[:12]
    wide_ref, c_conv_ref, gated_ref, scale_ref, products_ref, padded_ref = refs[-6:]
    place = lax.axis_index(OUTER)

    @pl.when((place == 0, place == 1, place >= 2)[turn])
    def _():
        spread_rows(factors_ref[...], x_ref.shape[1], cum_rows_ref.shape[0], wide_ref)
        products_of(*sources, c_conv_ref, products_ref, padded_ref)
        diagonal_of(
            sources[4], columns_ref, cum_rows_ref, step_rows_ref, x_ref, gate_ref, products_ref,
            gated_ref, scale_ref,
        )


def gate_kernel(state_ref, c_conv_ref, diagonal_ref, scale_ref, gated_ref, squares_ref):
    members, rows, features = state_ref.shape
    c_conv = c_conv_ref[...]
    squares = jnp.zeros((c_conv.shape[0], LANES), jnp.float32)
    for j in range(features // LANES):
        tile = slice(j * LANES, (j + 1) * LANES)
        state = state_ref[:, :, tile].astype(jnp.float32).reshape(members * rows, LANES)
        carried = jnp.dot(c_conv, state.astype(jnp.bfloat16), preferred_element_type=jnp.float32)
        gated = diagonal_ref[:, tile] + scale_ref[:, tile] * carried
        gated_ref[:, tile] = gated
        squares = squares + gated * gated
    ones = jnp.ones((8, LANES), jnp.bfloat16)
    squares_ref[...] = sum(
        lax.dot_general(ones, part, (((1,), (1,)), ((), ())), preferred_element_type=jnp.float32)
        for part in reversed(bf16_parts(squares))
    )[0:1]


def normalize_kernel(features_all, squares_ref, gated_ref, gain_ref, out_ref, rows_ref, sems):
    count = squares_ref.shape[0]
    tokens, features = gated_ref.shape
    total = squares_ref[0]
    for k in range(1, count):
        total = total + squares_ref[k]
    scale = lax.rsqrt(total / features_all + epsilon)
    scale = jnp.broadcast_to(scale, (LANES, tokens)).T
    chunks = sems.shape[0]
    size = tokens // chunks
    copies = []
    for i in range(chunks):
        part = slice(i * size, (i + 1) * size)
        for j in range(features // LANES):
            tile = slice(j * LANES, (j + 1) * LANES)
            rows_ref[part, tile] = (
                gated_ref[part, tile] * scale[part] * gain_ref[j : j + 1, :]
            ).astype(jnp.bfloat16)
        copies.append(
            pltpu.make_async_copy(
                rows_ref.at[pl.ds(i * size, size), :], out_ref.at[pl.ds(i * size, size), :],
                sems.at[i],
            )
        )
        copies[-1].start()
    for copy in copies:
        copy.wait()


def body(
    inputs, gate_input, b_source, c_source, step_raw, step_bias, decay_rate, conv_weight,
    conv_bias, norm_gain, doc_lengths,
):
    tokens, features = inputs.shape
    heads = step_raw.shape[1]
    state = b_source.shape[1]
    members = 1
    for axis in GROUP:
        members *= lax.axis_size(axis)
    outer = lax.axis_size(OUTER)
    rows = state // members
    shards = members * outer
    ahead = lambda n, k: [(i, i + k) for i in range(n - k)]

    bf16 = jnp.bfloat16
    small = [
        doc_lengths[None, :], step_raw.T, step_bias[None, :], decay_rate[None, :], b_source,
        conv_weight, conv_bias[None, :],
    ]
    tails, *small = call(
        tails_kernel,
        [out((8, 2 * state), bf16)] + [out(o.shape, o.dtype) for o in small],
        b_source, c_source, *small,
        hbm=2 + len(small), scratch=[pltpu.SemaphoreType.DMA((2 + len(small),))],
        flops=20_000_000_000,
    )
    halo = lax.ppermute(tails, SEQ, ahead(shards, 1))
    operands = [
        c_source, norm_gain.reshape(features // LANES, LANES),
    ]
    results = call(
        prepare_kernel,
        [out(o.shape, o.dtype) for o in operands]
        + [
            out((tokens, features), bf16), out((heads, tokens)), out((heads, tokens)),
            out((tokens, LANES)), out((1, LANES)), out((tokens, LANES), jnp.int32),
            out((tokens, state)),
        ],
        *operands, inputs, *small, tails,
        hbm=len(operands),
        scratch=[
            pltpu.VMEM((LANES, tokens), jnp.float32),
            pltpu.VMEM((tokens + 8, state), jnp.float32),
            pltpu.SemaphoreType.DMA((len(operands),)),
        ],
    )
    b, taps, taps_bias = small[4:]
    c, gain = results[0:2]
    weighted, cum_rows, step_rows, columns, factor, start, b_early = results[2:]
    pieces, b_conv = call(
        states_kernel,
        [out((members, rows, features + LANES)), out((tokens, state), bf16)],
        b, halo, taps, taps_bias, start, b_early, weighted, factor,
        scratch=[pltpu.VMEM((16, state), jnp.float32)],
    )
    pieces = lax.all_to_all(pieces, GROUP, 0, 0)
    pair = out((rows, features + LANES))
    before, factors, total_a, total_b, total_c = call(
        functools.partial(prefix_kernel, heads),
        [out((members, rows, features)), out((members, LANES)), pair, pair, pair],
        pieces,
        scratch=[
            pltpu.VMEM((members, LANES), jnp.float32),
            pltpu.VMEM((members, features), jnp.float32),
        ],
    )

    def diagonal_terms(turn, token, *before):
        sources = [
            c, halo, taps, taps_bias, start, b_conv, columns, cum_rows, step_rows, inputs, gate_input,
            factors,
        ]
        token = [] if token is None else [token]
        count = len(sources)
        return call(
            functools.partial(diagonal_kernel, turn),
            [out(t.shape) for t in token] + [
                out((members, features)), out((tokens, state), bf16), out((tokens, features)),
                out((tokens, features)),
            ],
            *sources, *token, *before, flops=20_000_000_000,
            aliases={count + k: k for k in range(len(token) + len(before))},
            scratch=[
                pltpu.VMEM((tokens, tokens), jnp.float32),
                pltpu.VMEM((tokens + 8, state), jnp.float32),
            ],
        )

    def send(total, *pairs):
        return lax.ppermute(total, OUTER, pairs)

    total_a, *diagonal = diagonal_terms(0, total_a)
    near_a = send(total_a, (0, 1))
    total_b, *diagonal = diagonal_terms(1, total_b, *diagonal)
    far = send(total_b, (0, 2), (1, 3))
    near_b = send(total_c, (1, 2), (2, 3))
    wide, c_conv, diagonal, scale = diagonal_terms(2, None, *diagonal)
    states_in = call(
        functools.partial(states_in_kernel, heads),
        out((members, rows, features), bf16),
        near_a, near_b, far, before, wide,
        scratch=[pltpu.VMEM(pair.shape, jnp.float32)],
    )
    states_in = lax.all_to_all(states_in, GROUP, 0, 0)
    gated, squares = call(
        gate_kernel,
        [out((tokens, features)), out((1, tokens))],
        states_in, c_conv, diagonal, scale,
    )
    squares = lax.all_gather(squares, "tp")
    return call(
        functools.partial(normalize_kernel, features * lax.axis_size("tp")),
        jax.ShapeDtypeStruct((tokens, features), bf16),
        squares, gated, gain, to_hbm=True,
        scratch=[pltpu.VMEM((tokens, features), bf16), pltpu.SemaphoreType.DMA((4,))],
    )


def solution(mesh):
    finer = Mesh(
        mesh.devices.reshape(4, 2, 4, 4, mesh.shape["tp"]), ("za", "zb", "y", "x", "tp")
    )
    in_specs = (
        P(SEQ, "tp"), P(SEQ, "tp"), P(SEQ, None), P(SEQ, None), P(SEQ, "tp"), P("tp"), P("tp"),
        P(), P(), P("tp"), P(),
    )
    return jax.shard_map(
        body, mesh=finer, in_specs=in_specs, out_specs=P(SEQ, "tp"), check_vma=False
    )
```

```python
import functools

import jax
import jax.numpy as jnp
from jax import lax
from jax.experimental import pallas as pl
from jax.experimental.pallas import tpu as pltpu
from jax.sharding import Mesh
from jax.sharding import PartitionSpec as P

SEQ = ("za", "zb", "y", "x")
GROUP = ("zb", "y", "x")
OUTER = "za"
LANES = 128
epsilon = 1e-05
VMEM = pl.BlockSpec(memory_space=pltpu.VMEM)
HBM = pl.BlockSpec(memory_space=pltpu.HBM)


def call(
    kernel, outs, *args, hbm=0, after=(), scratch=(), flops=1_000_000, aliases=None, to_hbm=False
):
    if after:
        inner, skip = kernel, len(after)
        kernel = lambda *refs: inner(*refs[:len(args)], *refs[len(args) + skip:])
    multiple = isinstance(outs, (list, tuple))
    return pl.pallas_call(
        kernel,
        out_shape=list(outs) if multiple else outs,
        in_specs=[HBM] * hbm + [VMEM] * (len(args) - hbm) + [VMEM] * len(after),
        out_specs=[VMEM] * len(outs) if multiple else HBM if to_hbm else VMEM,
        input_output_aliases=aliases or {},
        scratch_shapes=list(scratch),
        compiler_params=pltpu.CompilerParams(vmem_limit_bytes=24 * 1024 * 1024),
        cost_estimate=pl.CostEstimate(flops=flops, bytes_accessed=1_000_000, transcendentals=0),
    )(*(pltpu.with_memory_space_constraint(a, pltpu.HBM) for a in args[:hbm]), *args[hbm:], *after)


def out(shape, dtype=jnp.float32):
    return pltpu.VMEM(shape, dtype)


def tile_of_heads(columns, tile, width):
    per, rows = LANES // width, columns.shape[0]
    lane = lax.broadcasted_iota(jnp.int32, (rows, LANES), 1)
    h = tile * per
    spread = jnp.broadcast_to(columns[:, h : h + 1], (rows, LANES))
    for k in range(1, per):
        other = jnp.broadcast_to(columns[:, h + k : h + k + 1], (rows, LANES))
        spread = jnp.where(lane < k * width, spread, other)
    return spread


def tails_kernel(b_ref, c_ref, *refs):
    count = (len(refs) - 2) // 2
    sources, tails_ref, targets, sems = refs[:count], refs[count], refs[count + 1 : -1], refs[-1]
    tokens, state = b_ref.shape
    copies = [
        pltpu.make_async_copy(
            r.at[pl.ds(tokens - 8, 8), :], tails_ref.at[:, pl.ds(k * state, state)], sems.at[k]
        )
        for k, r in enumerate((b_ref, c_ref))
    ]
    for k, (source, target) in enumerate(zip(sources, targets)):
        copies.append(pltpu.make_async_copy(source, target, sems.at[k + 2]))
    for k, copy in enumerate(copies):
        copy.start(priority=1 if k < 2 else 0)
    for copy in copies:
        copy.wait()


def convolve(padded_ref, weight, bias, relative, start):
    tokens = relative.shape[0]
    taps = weight.shape[0]
    summed = jnp.broadcast_to(bias, (tokens, bias.shape[1]))
    for k in range(taps):
        back = taps - 1 - k
        term = weight[k : k + 1, :] * padded_ref[8 - back : 8 - back + tokens, :]
        summed = summed + jnp.where(relative - back >= start, term, 0.0)
    return (summed * jax.nn.sigmoid(summed)).astype(jnp.bfloat16)


def bf16_parts(value):
    parts = []
    for _ in range(3):
        part = value.astype(jnp.bfloat16)
        parts.append(part)
        value = value - part.astype(jnp.float32)
    return parts


def spread_matrix(first, last, width, at):
    row = lax.broadcasted_iota(jnp.int32, (LANES, last - first), 0)
    head = (first + lax.broadcasted_iota(jnp.int32, (LANES, last - first), 1)) // width
    inside = (row >= at) if at else (row < 32)
    return jnp.where(inside & ((row & 31) == head), 1.0, 0.0).astype(jnp.bfloat16)


def spread_rows(values, features, heads, wide_ref):
    count = values.shape[0]
    parts = jnp.concatenate(bf16_parts(jnp.where(
        lax.broadcasted_iota(jnp.int32, values.shape, 1) < heads, values, 0.0
    )), axis=0)
    for j in range(0, features, 256):
        wide = jnp.dot(
            parts, spread_matrix(j, j + 256, features // heads, 0),
            preferred_element_type=jnp.float32,
        )
        wide_ref[:, j : j + 256] = (
            wide[2 * count :] + wide[count : 2 * count]
        ) + wide[0:count]


def sequence_index():
    index = 0
    for axis in SEQ:
        index = index * lax.axis_size(axis) + lax.axis_index(axis)
    return index


def to_column(row):
    n = row.shape[1]
    same = lax.broadcasted_iota(jnp.int32, (n, n), 0) == lax.broadcasted_iota(jnp.int32, (n, n), 1)
    return jnp.sum(jnp.where(same, jnp.broadcast_to(row, (n, n)), 0.0), axis=1, keepdims=True)


WEIGHTS_AT = 32


def prepare_kernel(*refs):
    count, given = 5, 6
    sources, targets = refs[:count], refs[count + given : 2 * count + given]
    x_ref, docs_ref, raw_ref, bias_ref, rate_ref, _ = refs[count : count + given]
    b_ref, taps_ref, taps_bias_ref, _, _ = targets
    (
        weighted_ref, cum_rows_ref, step_rows_ref, columns_ref, factor_ref, start_ref, b_conv_ref,
        stack_ref, padded_ref, sems,
    ) = refs[2 * count + given :]
    copies = [
        pltpu.make_async_copy(source, target, sems.at[k])
        for k, (source, target) in enumerate(zip(sources, targets))
    ]
    for copy in copies:
        copy.start()
    heads, tokens = raw_ref.shape
    state = b_ref.shape[1]
    width = x_ref.shape[1] // heads
    base = sequence_index() * tokens
    relative = lax.broadcasted_iota(jnp.int32, (tokens, LANES), 0)
    start = jnp.zeros((1, 1), jnp.int32) - base
    last_position = jnp.full((1, 1), tokens - 1, jnp.int32)
    chosen = jnp.broadcast_to(start, relative.shape)
    end_start = start
    for i in range(1, docs_ref.shape[1]):
        start = start + docs_ref[0:1, i - 1 : i]
        chosen = jnp.where(start <= relative, start, chosen)
        end_start = jnp.where(start <= last_position, start, end_start)
    start_ref[...] = chosen

    step = jax.nn.softplus(raw_ref[...] + to_column(bias_ref[...]))
    log_decay = -step * to_column(rate_ref[...])
    rows = lax.broadcasted_iota(jnp.int32, (tokens, tokens), 0)
    cols = lax.broadcasted_iota(jnp.int32, (tokens, tokens), 1)
    upper = jnp.where(rows <= cols, 1.0, 0.0).astype(jnp.bfloat16)
    cum = sum(
        jnp.dot(part, upper, preferred_element_type=jnp.float32)
        for part in reversed(bf16_parts(log_decay))
    )
    cum_rows_ref[...] = cum
    step_rows_ref[...] = step
    position = lax.broadcasted_iota(jnp.int32, (heads, tokens), 1)
    weighting = jnp.where(
        position >= end_start, jnp.exp(cum[:, tokens - 1 : tokens] - cum) * step, 0.0
    )
    stack_ref[...] = jnp.zeros_like(stack_ref)
    stack_ref[0:heads, :] = cum
    for k, part in enumerate(bf16_parts(weighting)):
        at = WEIGHTS_AT * (k + 1)
        stack_ref[at : at + heads, :] = part.astype(jnp.float32)
    columns = stack_ref[...].T
    columns_ref[...] = columns
    factor_ref[...] = jnp.where(end_start < 0, jnp.exp(columns[tokens - 1 : tokens, :]), 0.0)
    weights = columns.astype(jnp.bfloat16)
    for j in range(0, x_ref.shape[1], 256):
        tile = slice(j, j + 256)
        spread = jnp.dot(
            weights, spread_matrix(j, j + 256, width, WEIGHTS_AT),
            preferred_element_type=jnp.float32,
        )
        weighted_ref[:, tile] = (x_ref[:, tile].astype(jnp.float32) * spread).astype(jnp.bfloat16)
    for copy in copies:
        copy.wait()
    side = slice(0, state)
    padded_ref[0:8, :] = jnp.zeros((8, state), jnp.float32)
    padded_ref[8:, :] = b_ref[...].astype(jnp.float32)
    b_conv = convolve(padded_ref, taps_ref[:, side], taps_bias_ref[:, side], relative, chosen)
    b_conv_ref[...] = b_conv.astype(jnp.float32)


def first_rows(source_ref, halo, weight, bias, start_ref, padded_ref):
    padded_ref[0:8, :] = halo.astype(jnp.float32)
    padded_ref[8:, :] = source_ref[0:8, :].astype(jnp.float32)
    relative = lax.broadcasted_iota(jnp.int32, (8, LANES), 0)
    return convolve(padded_ref, weight, bias, relative, start_ref[0:8, :])


def states_kernel(
    b_ref, halo_ref, taps_ref, taps_bias_ref, start_ref, b_early_ref, weighted_ref, factor_ref,
    pieces_ref, b_conv_ref, padded_ref,
):
    state, features = b_ref.shape[1], weighted_ref.shape[1]
    members, rows, _ = pieces_ref.shape
    first = first_rows(
        b_ref, halo_ref[:, 0:state], taps_ref[:, 0:state], taps_bias_ref[:, 0:state], start_ref,
        padded_ref,
    )
    b_conv = jnp.concatenate([first.astype(jnp.float32), b_early_ref[8:, :]], axis=0)
    b_conv_ref[...] = b_conv.astype(jnp.bfloat16)
    b_rows = b_conv.T.astype(jnp.bfloat16)
    for j in range(features // 256):
        tile = slice(j * 256, (j + 1) * 256)
        end_state = jnp.dot(b_rows, weighted_ref[:, tile], preferred_element_type=jnp.float32)
        for m in range(members):
            pieces_ref[m, :, tile] = end_state[m * rows : (m + 1) * rows, :]
    spread = jnp.broadcast_to(factor_ref[...], (rows, LANES))
    for m in range(members):
        pieces_ref[m, :, features:] = spread


def prefix_kernel(
    heads, pieces_ref, before_ref, factors_ref, total_a_ref, total_b_ref, total_c_ref, single_ref,
    wide_ref,
):
    members, rows, padded = pieces_ref.shape
    features = padded - LANES
    for m in range(members):
        single_ref[m : m + 1, :] = pieces_ref[m, 0:1, features:]
    spread_rows(single_ref[...], features, heads, wide_ref)
    product = jnp.ones((1, LANES), jnp.float32)
    for m in range(members):
        factors_ref[m : m + 1, :] = product
        product = product * single_ref[m : m + 1, :]
    total = jnp.zeros((rows, features), jnp.float32)
    for m in range(members):
        before_ref[m] = total
        total = wide_ref[m : m + 1, :] * total + pieces_ref[m, :, 0:features]
    for total_ref in (total_a_ref, total_b_ref, total_c_ref):
        total_ref[:, 0:features] = total
        total_ref[:, features:] = jnp.broadcast_to(product, (rows, LANES))


def wide_factor(pair_ref, features, width):
    factor = pair_ref[0:1, features:]
    return jnp.concatenate(
        [tile_of_heads(factor, j, width) for j in range(features // LANES)], axis=1
    )


def states_in_kernel(heads, *refs):
    *near_refs, far_ref, before_ref, wide_ref, state_ref, near_ref = refs
    members, _, features = before_ref.shape
    near_ref[...] = sum(ref[...] for ref in near_refs)
    factor = wide_factor(near_ref, features, features // heads)
    entering = factor * far_ref[:, 0:features] + near_ref[:, 0:features]
    for m in range(members):
        state_ref[m] = (wide_ref[m : m + 1, :] * entering + before_ref[m]).astype(jnp.bfloat16)


def products_of(
    c_ref, halo_ref, taps_ref, taps_bias_ref, start_ref, b_conv_ref, c_conv_ref, products_ref,
    padded_ref,
):
    tokens, state = c_ref.shape
    padded_ref[0:8, :] = halo_ref[:, state:].astype(jnp.float32)
    padded_ref[8:, :] = c_ref[...].astype(jnp.float32)
    relative = lax.broadcasted_iota(jnp.int32, (tokens, LANES), 0)
    c_conv = convolve(
        padded_ref, taps_ref[:, state:], taps_bias_ref[:, state:], relative, start_ref[...]
    )
    c_conv_ref[...] = c_conv
    products = lax.dot_general(
        c_conv, b_conv_ref[...], (((1,), (1,)), ((), ())), preferred_element_type=jnp.float32
    )
    row = lax.broadcasted_iota(jnp.int32, (tokens, tokens), 0)
    col = lax.broadcasted_iota(jnp.int32, (tokens, tokens), 1)
    starts = jnp.concatenate([start_ref[...]] * (tokens // LANES), axis=1)
    products_ref[...] = jnp.where((col <= row) & (col >= starts), products, 0.0)


def diagonal_of(
    start_ref, columns_ref, cum_rows_ref, step_rows_ref, x_ref, gate_ref, products_ref, gated_ref,
    scale_ref,
):
    tokens, features = x_ref.shape
    width, half = features // cum_rows_ref.shape[0], tokens // 2
    columns = columns_ref[...]
    carried = jnp.where(start_ref[...] < 0, jnp.exp(columns), 0.0)
    lane = lax.broadcasted_iota(jnp.int32, (tokens, LANES), 1)
    per = LANES // width
    for j in range(features // LANES):
        tile = slice(j * LANES, (j + 1) * LANES)
        diagonal = None
        for k in range(per):
            h = j * per + k
            column = jnp.broadcast_to(columns[:, h : h + 1], (tokens, LANES))
            cum_row, step_row = cum_rows_ref[h : h + 1, :], step_rows_ref[h : h + 1, :]
            upper = (
                products_ref[0:half, 0:half] * jnp.exp(column[0:half] - cum_row[:, 0:half])
            ) * step_row[:, 0:half]
            lower_left = (
                products_ref[half:, 0:half] * jnp.exp(column[half:] - cum_row[:, 0:half])
            ) * step_row[:, 0:half]
            lower_right = (
                products_ref[half:, half:] * jnp.exp(column[half:] - cum_row[:, half:])
            ) * step_row[:, half:]
            lower = jnp.concatenate([lower_left, lower_right], axis=1).astype(jnp.bfloat16)
            part = jnp.concatenate(
                [
                    jnp.dot(upper.astype(jnp.bfloat16), x_ref[0:half, tile],
                            preferred_element_type=jnp.float32),
                    jnp.dot(lower, x_ref[:, tile], preferred_element_type=jnp.float32),
                ],
                axis=0,
            )
            diagonal = part if diagonal is None else jnp.where(lane < k * width, diagonal, part)
        gate = gate_ref[:, tile].astype(jnp.float32)
        gate = gate * jax.nn.sigmoid(gate)
        gated_ref[:, tile] = diagonal * gate
        scale_ref[:, tile] = tile_of_heads(carried, j, width) * gate


def diagonal_kernel(turn, *refs):
    (*sources, columns_ref, cum_rows_ref, step_rows_ref, x_ref, gate_ref, factors_ref) = refs[:12]
    wide_ref, c_conv_ref, gated_ref, scale_ref, products_ref, padded_ref = refs[-6:]
    place = lax.axis_index(OUTER)

    @pl.when((place == 0, place == 1, place >= 2)[turn])
    def _():
        spread_rows(factors_ref[...], x_ref.shape[1], cum_rows_ref.shape[0], wide_ref)
        products_of(*sources, c_conv_ref, products_ref, padded_ref)
        diagonal_of(
            sources[4], columns_ref, cum_rows_ref, step_rows_ref, x_ref, gate_ref, products_ref,
            gated_ref, scale_ref,
        )


def gate_kernel(state_ref, c_conv_ref, diagonal_ref, scale_ref, gated_ref, squares_ref):
    members, rows, features = state_ref.shape
    c_conv = c_conv_ref[...]
    squares = jnp.zeros((c_conv.shape[0], LANES), jnp.float32)
    for j in range(features // LANES):
        tile = slice(j * LANES, (j + 1) * LANES)
        state = state_ref[:, :, tile].astype(jnp.float32).reshape(members * rows, LANES)
        carried = jnp.dot(c_conv, state.astype(jnp.bfloat16), preferred_element_type=jnp.float32)
        gated = diagonal_ref[:, tile] + scale_ref[:, tile] * carried
        gated_ref[:, tile] = gated
        squares = squares + gated * gated
    ones = jnp.ones((8, LANES), jnp.bfloat16)
    squares_ref[...] = sum(
        lax.dot_general(ones, part, (((1,), (1,)), ((), ())), preferred_element_type=jnp.float32)
        for part in reversed(bf16_parts(squares))
    )[0:1]


def normalize_kernel(features_all, squares_ref, gated_ref, gain_ref, out_ref, rows_ref, sems):
    count = squares_ref.shape[0]
    tokens, features = gated_ref.shape
    total = squares_ref[0]
    for k in range(1, count):
        total = total + squares_ref[k]
    scale = lax.rsqrt(total / features_all + epsilon)
    scale = jnp.broadcast_to(scale, (LANES, tokens)).T
    chunks = sems.shape[0]
    size = tokens // chunks
    copies = []
    for i in range(chunks):
        part = slice(i * size, (i + 1) * size)
        for j in range(features // LANES):
            tile = slice(j * LANES, (j + 1) * LANES)
            rows_ref[part, tile] = (
                gated_ref[part, tile] * scale[part] * gain_ref[j : j + 1, :]
            ).astype(jnp.bfloat16)
        copies.append(
            pltpu.make_async_copy(
                rows_ref.at[pl.ds(i * size, size), :], out_ref.at[pl.ds(i * size, size), :],
                sems.at[i],
            )
        )
        copies[-1].start()
    for copy in copies:
        copy.wait()


def body(
    inputs, gate_input, b_source, c_source, step_raw, step_bias, decay_rate, conv_weight,
    conv_bias, norm_gain, doc_lengths,
):
    tokens, features = inputs.shape
    heads = step_raw.shape[1]
    state = b_source.shape[1]
    members = 1
    for axis in GROUP:
        members *= lax.axis_size(axis)
    outer = lax.axis_size(OUTER)
    rows = state // members
    shards = members * outer
    ahead = lambda n, k: [(i, i + k) for i in range(n - k)]

    bf16 = jnp.bfloat16
    small = [doc_lengths[None, :], step_raw.T, step_bias[None, :], decay_rate[None, :]]
    tails, *small = call(
        tails_kernel,
        [out((8, 2 * state), bf16)] + [out(o.shape, o.dtype) for o in small],
        b_source, c_source, *small,
        hbm=2 + len(small), scratch=[pltpu.SemaphoreType.DMA((2 + len(small),))],
        flops=20_000_000_000,
    )
    halo = lax.ppermute(tails, SEQ, ahead(shards, 1))
    operands = [
        b_source, conv_weight, conv_bias[None, :], c_source,
        norm_gain.reshape(features // LANES, LANES),
    ]
    results = call(
        prepare_kernel,
        [out(o.shape, o.dtype) for o in operands]
        + [
            out((tokens, features), bf16), out((heads, tokens)), out((heads, tokens)),
            out((tokens, LANES)), out((1, LANES)), out((tokens, LANES), jnp.int32),
            out((tokens, state)),
        ],
        *operands, inputs, *small, tails,
        hbm=len(operands),
        scratch=[
            pltpu.VMEM((LANES, tokens), jnp.float32),
            pltpu.VMEM((tokens + 8, state), jnp.float32),
            pltpu.SemaphoreType.DMA((len(operands),)),
        ],
    )
    b, taps, taps_bias, c, gain = results[0:5]
    weighted, cum_rows, step_rows, columns, factor, start, b_early = results[5:]
    pieces, b_conv = call(
        states_kernel,
        [out((members, rows, features + LANES)), out((tokens, state), bf16)],
        b, halo, taps, taps_bias, start, b_early, weighted, factor,
        scratch=[pltpu.VMEM((16, state), jnp.float32)],
    )
    pieces = lax.all_to_all(pieces, GROUP, 0, 0)
    pair = out((rows, features + LANES))
    before, factors, total_a, total_b, total_c = call(
        functools.partial(prefix_kernel, heads),
        [out((members, rows, features)), out((members, LANES)), pair, pair, pair],
        pieces,
        scratch=[
            pltpu.VMEM((members, LANES), jnp.float32),
            pltpu.VMEM((members, features), jnp.float32),
        ],
    )

    def diagonal_terms(turn, token, *before):
        sources = [
            c, halo, taps, taps_bias, start, b_conv, columns, cum_rows, step_rows, inputs, gate_input,
            factors,
        ]
        token = [] if token is None else [token]
        count = len(sources)
        return call(
            functools.partial(diagonal_kernel, turn),
            [out(t.shape) for t in token] + [
                out((members, features)), out((tokens, state), bf16), out((tokens, features)),
                out((tokens, features)),
            ],
            *sources, *token, *before, flops=20_000_000_000,
            aliases={count + k: k for k in range(len(token) + len(before))},
            scratch=[
                pltpu.VMEM((tokens, tokens), jnp.float32),
                pltpu.VMEM((tokens + 8, state), jnp.float32),
            ],
        )

    def send(total, *pairs):
        return lax.ppermute(total, OUTER, pairs)

    total_a, *diagonal = diagonal_terms(0, total_a)
    near_a = send(total_a, (0, 1))
    total_b, *diagonal = diagonal_terms(1, total_b, *diagonal)
    far = send(total_b, (0, 2), (1, 3))
    near_b = send(total_c, (1, 2), (2, 3))
    wide, c_conv, diagonal, scale = diagonal_terms(2, None, *diagonal)
    states_in = call(
        functools.partial(states_in_kernel, heads),
        out((members, rows, features), bf16),
        near_a, near_b, far, before, wide,
        scratch=[pltpu.VMEM(pair.shape, jnp.float32)],
    )
    states_in = lax.all_to_all(states_in, GROUP, 0, 0)
    gated, squares = call(
        gate_kernel,
        [out((tokens, features)), out((1, tokens))],
        states_in, c_conv, diagonal, scale,
    )
    squares = lax.all_gather(squares, "tp")
    return call(
        functools.partial(normalize_kernel, features * lax.axis_size("tp")),
        jax.ShapeDtypeStruct((tokens, features), bf16),
        squares, gated, gain, to_hbm=True,
        scratch=[pltpu.VMEM((tokens, features), bf16), pltpu.SemaphoreType.DMA((4,))],
    )


def solution(mesh):
    finer = Mesh(
        mesh.devices.reshape(4, 2, 4, 4, mesh.shape["tp"]), ("za", "zb", "y", "x", "tp")
    )
    in_specs = (
        P(SEQ, "tp"), P(SEQ, "tp"), P(SEQ, None), P(SEQ, None), P(SEQ, "tp"), P("tp"), P("tp"),
        P(), P(), P("tp"), P(),
    )
    return jax.shard_map(
        body, mesh=finer, in_specs=in_specs, out_specs=P(SEQ, "tp"), check_vma=False
    )
```
